8 devices in a mesh: dp: 1 (over z), pool: 2 (over y), ep: 4 (over x, core).
Axes of the slice: x: 2, y: 2, z: 1, core: 2. Of those that a mesh axis runs over, the one named last changes fastest.
Arguments:
- hidden_in: bfloat16 [512, 1024], P(('dp', 'ep'))
- k_cache: bfloat16 [2, 512, 128, 8, 128], P(None, ('dp', 'ep'), 'pool')
- v_cache: bfloat16 [2, 512, 128, 8, 128], P(None, ('dp', 'ep'), 'pool')
- cache_len: int32 [512], P(('dp', 'ep'))
- w_q: bfloat16 [2, 1024, 1024], replicated
- w_k: bfloat16 [2, 1024, 1024], replicated
- w_v: bfloat16 [2, 1024, 1024], replicated
- w_o: bfloat16 [2, 1024, 1024], replicated
- w_router: float32 [2, 1024, 64], replicated
- expert_ids: int32 [2, 512, 6], P(None, ('dp', 'ep'))
- w_one: bfloat16 [2, 64, 1024, 704], P(None, 'ep', None, 'pool')
- w_three: bfloat16 [2, 64, 1024, 704], P(None, 'ep', None, 'pool')
- w_two: bfloat16 [2, 64, 704, 1024], P(None, 'ep', 'pool')
Outputs:
- output: bfloat16 [512, 1024], P(('dp', 'ep'))
All inputs are finite; a program needn't handle non-finite values.
Results may differ from the reference program's by a relative error of at most 0.02.
Values are sent between devices in bfloat16 or wider.
A program may use at most 1 GiB of HBM per device.

```python
import jax
import jax.numpy as jnp
from jax import lax

D_MODEL = 1024
N_HEADS = 8
KV_HEADS = 8
HEAD_DIM = 128
N_EXPERTS = 64
TOP_K = 6
FF_DIM = 704
NUM_LAYERS = 2
EP_GROUP = 4
BATCH_TOK = 512
SEQ_LEN = 128

GROUP_SIZE = N_HEADS // KV_HEADS
LOCAL_EXP = N_EXPERTS // EP_GROUP
TOK_SHARD = BATCH_TOK // EP_GROUP


def draw_ids(rkey):
    k_shift, k_first, k_second = jax.random.split(rkey, 3)
    shift_dev = jax.random.randint(k_shift, (NUM_LAYERS, EP_GROUP, 1, 1), 0, EP_GROUP)
    pair_idx = jnp.arange(TOK_SHARD)[:, None] * TOP_K + jnp.arange(TOP_K)[None, :]
    dest_dev = (pair_idx[None, None] + shift_dev) % EP_GROUP
    first_draw = jax.random.randint(k_first, (NUM_LAYERS, EP_GROUP, TOK_SHARD, 1), 0, LOCAL_EXP)
    second_draw = jax.random.randint(k_second, (NUM_LAYERS, EP_GROUP, TOK_SHARD, 1), 0, LOCAL_EXP)
    start_exp = (first_draw * second_draw) // LOCAL_EXP
    local_id = (start_exp + jnp.arange(TOP_K)[None, None, None, :] // EP_GROUP) % LOCAL_EXP
    chosen = dest_dev * LOCAL_EXP + local_id
    return chosen.reshape(NUM_LAYERS, BATCH_TOK, TOP_K).astype(jnp.int32)


def draw_lens(lkey):
    lens_drawn = jax.random.randint(lkey, (BATCH_TOK,), 1, SEQ_LEN + 1)
    return lens_drawn.at[0].set(SEQ_LEN).astype(jnp.int32)


def setup_inputs(seed: int = 0, part: int = 0) -> dict:
    base_key = jax.random.key(seed)
    part_key = jax.random.fold_in(base_key, part)
    share_keys = jax.random.split(base_key, 8)
    part_keys = jax.random.split(part_key, 5)
    attn_in = N_HEADS * HEAD_DIM
    kv_in = KV_HEADS * HEAD_DIM
    cache_shape = (NUM_LAYERS, BATCH_TOK, SEQ_LEN, KV_HEADS, HEAD_DIM)
    hidden_in = jax.random.normal(part_keys[0], (BATCH_TOK, D_MODEL), jnp.float32).astype(jnp.bfloat16)
    k_cache = jax.random.normal(part_keys[1], cache_shape, jnp.float32).astype(jnp.bfloat16)
    v_cache = jax.random.normal(part_keys[2], cache_shape, jnp.float32).astype(jnp.bfloat16)
    cache_len = draw_lens(part_keys[3])
    expert_ids = draw_ids(part_keys[4])
    w_q = (jax.random.normal(share_keys[0], (NUM_LAYERS, D_MODEL, attn_in), jnp.float32) * (2.0 * D_MODEL ** -0.5)).astype(jnp.bfloat16)
    w_k = (jax.random.normal(share_keys[1], (NUM_LAYERS, D_MODEL, kv_in), jnp.float32) * D_MODEL ** -0.5).astype(jnp.bfloat16)
    w_v = (jax.random.normal(share_keys[2], (NUM_LAYERS, D_MODEL, kv_in), jnp.float32) * D_MODEL ** -0.5).astype(jnp.bfloat16)
    w_o = (jax.random.normal(share_keys[3], (NUM_LAYERS, attn_in, D_MODEL), jnp.float32) * (2.0 * attn_in ** -0.5)).astype(jnp.bfloat16)
    w_router = jax.random.normal(share_keys[4], (NUM_LAYERS, D_MODEL, N_EXPERTS), jnp.float32) * (1.5 * D_MODEL ** -0.5)
    w_one = (jax.random.normal(share_keys[5], (NUM_LAYERS, N_EXPERTS, D_MODEL, FF_DIM), jnp.float32) * D_MODEL ** -0.5).astype(jnp.bfloat16)
    w_three = (jax.random.normal(share_keys[6], (NUM_LAYERS, N_EXPERTS, D_MODEL, FF_DIM), jnp.float32) * D_MODEL ** -0.5).astype(jnp.bfloat16)
    w_two = (jax.random.normal(share_keys[7], (NUM_LAYERS, N_EXPERTS, FF_DIM, D_MODEL), jnp.float32) * (2.0 * FF_DIM ** -0.5)).astype(jnp.bfloat16)
    return dict(hidden_in=hidden_in, k_cache=k_cache, v_cache=v_cache, cache_len=cache_len, w_q=w_q, w_k=w_k, w_v=w_v, w_o=w_o, w_router=w_router, expert_ids=expert_ids, w_one=w_one, w_three=w_three, w_two=w_two)


def rms_norm(in_vals):
    in_vals = in_vals.astype(jnp.float32)
    return in_vals * lax.rsqrt(jnp.mean(in_vals * in_vals, axis=-1, keepdims=True) + 1e-6)


def attend_token(packed):
    q_tok, k_new, v_new, k_rows, v_rows, valid_len = packed
    att_scale = HEAD_DIM ** -0.5
    q_grp = q_tok.reshape(KV_HEADS, GROUP_SIZE, HEAD_DIM).astype(jnp.float32)
    score_vals = jnp.einsum('gqd,sgd->gqs', q_grp, k_rows.astype(jnp.float32)) * att_scale
    pos_mask = jnp.arange(SEQ_LEN) < valid_len
    score_vals = jnp.where(pos_mask[None, None, :], score_vals, -1e30)
    new_score = jnp.einsum('gqd,gd->gq', q_grp, k_new.astype(jnp.float32)) * att_scale
    top_score = jnp.maximum(jnp.max(score_vals, axis=-1), new_score)
    prob_vals = jnp.exp(score_vals - top_score[..., None])
    new_prob = jnp.exp(new_score - top_score)
    denom_sum = jnp.sum(prob_vals, axis=-1) + new_prob
    numer_sum = jnp.einsum('gqs,sgd->gqd', prob_vals.astype(jnp.bfloat16).astype(jnp.float32), v_rows.astype(jnp.float32))
    numer_sum = numer_sum + new_prob[..., None] * v_new.astype(jnp.float32)[:, None, :]
    return (numer_sum / denom_sum[..., None]).reshape(N_HEADS * HEAD_DIM)


def moe_experts(u_rows, ids_layer, w_one, w_three, w_two):
    flat_ids = ids_layer.reshape(-1)
    sort_order = jnp.argsort(flat_ids, stable=True)
    tok_rows = u_rows[sort_order // TOP_K].astype(jnp.float32)
    group_sizes = jnp.bincount(flat_ids, length=N_EXPERTS).astype(jnp.int32)
    h_one = lax.ragged_dot(tok_rows, w_one.astype(jnp.float32), group_sizes)
    h_three = lax.ragged_dot(tok_rows, w_three.astype(jnp.float32), group_sizes)
    act_rows = (jax.nn.silu(h_one) * h_three).astype(jnp.bfloat16).astype(jnp.float32)
    out_rows = lax.ragged_dot(act_rows, w_two.astype(jnp.float32), group_sizes).astype(jnp.bfloat16)
    back_order = jnp.argsort(sort_order)
    return out_rows[back_order].reshape(BATCH_TOK, TOP_K, D_MODEL)


def reference(hidden_in, k_cache, v_cache, cache_len, w_q, w_k, w_v, w_o, w_router, expert_ids, w_one, w_three, w_two):
    def layer_step(hidden, layer_in):
        kc_l, vc_l, wq_l, wk_l, wv_l, wo_l, wr_l, ids_l, w1_l, w3_l, w2_l = layer_in
        normed = rms_norm(hidden).astype(jnp.bfloat16)
        q_rows = jnp.dot(normed, wq_l, preferred_element_type=jnp.float32).astype(jnp.bfloat16)
        k_new = jnp.dot(normed, wk_l, preferred_element_type=jnp.float32).astype(jnp.bfloat16).reshape(BATCH_TOK, KV_HEADS, HEAD_DIM)
        v_new = jnp.dot(normed, wv_l, preferred_element_type=jnp.float32).astype(jnp.bfloat16).reshape(BATCH_TOK, KV_HEADS, HEAD_DIM)
        attn_out = lax.map(attend_token, (q_rows, k_new, v_new, kc_l, vc_l, cache_len)).astype(jnp.bfloat16)
        resid_rows = (hidden.astype(jnp.float32) + jnp.dot(attn_out, wo_l, preferred_element_type=jnp.float32)).astype(jnp.bfloat16)
        u_rows = rms_norm(resid_rows).astype(jnp.bfloat16)
        logits = jnp.dot(u_rows.astype(jnp.float32), wr_l)
        gate_vals = jax.nn.softmax(jnp.take_along_axis(logits, ids_l, axis=1), axis=-1)
        pair_rows = moe_experts(u_rows, ids_l, w1_l, w3_l, w2_l)
        mixed_sum = jnp.sum(gate_vals[..., None] * pair_rows.astype(jnp.float32), axis=1)
        return (resid_rows.astype(jnp.float32) + mixed_sum).astype(jnp.bfloat16), None
    hidden_out, unused_ys = lax.scan(layer_step, hidden_in, (k_cache, v_cache, w_q, w_k, w_v, w_o, w_router, expert_ids, w_one, w_three, w_two))
    return hidden_out
```

```python
import functools

import jax
import jax.numpy as jnp
from jax import lax
from jax.experimental import pallas as pl
from jax.experimental.pallas import tpu as pltpu
from jax.sharding import PartitionSpec as P

MESH = pl.DeviceIdType.MESH
F32 = jnp.float32
BF16 = jnp.bfloat16
I32 = jnp.int32
EPS = 1e-6
NEG = -1e30
TB = 8
SLOTS = 4
TILE_M = 128


def _nn(a, b):
    return lax.dot_general(a, b, (((1,), (0,)), ((), ())), preferred_element_type=F32)


def _nt(a, b, precision=None):
    return lax.dot_general(a, b, (((1,), (1,)), ((), ())), preferred_element_type=F32, precision=precision)


def _rms(v):
    return v * lax.rsqrt(jnp.mean(v * v, axis=-1, keepdims=True) + EPS)


def _where_am_i():
    p = lax.axis_index("pool")
    b = lax.axis_index("ep")
    x, c = b // 2, b % 2
    to_y = {"pool": 1 - p}
    to_x = {"ep": (1 - x) * 2 + c}
    to_c = {"ep": x * 2 + (1 - c)}
    return p, b, x, c, to_y, to_x, to_c


def _greet(peers):
    sem = pltpu.get_barrier_semaphore()
    for peer in peers:
        pl.semaphore_signal(sem, inc=1, device_id=peer, device_id_type=MESH)
    pl.semaphore_wait(sem, len(peers))


def _rcopy(src, dst, send, recv, peer):
    return pltpu.make_async_remote_copy(src_ref=src, dst_ref=dst, send_sem=send, recv_sem=recv, device_id=peer, device_id_type=MESH)


def attn_kernel(layer, x_ref, len_ref, k_hbm, v_hbm, wq_hbm, wk_hbm, wv_hbm, wo_hbm, u_out, a_out,
                kbuf, vbuf, wq, wk, wv, wo, q3, o3, o3r, k3, v3, mls, mlr, o2, u_all, a_own, a_half,
                ksem, vsem, wsem, osend, orecv, gsend, grecv, lsem):
    p, b, x, c, to_y, to_x, to_c = _where_am_i()
    half = x_ref.shape[0] // 2
    heads, dim = q3.shape[1], q3.shape[2]
    cols = heads * dim
    rows = kbuf.shape[2]
    n_half = half // TB
    n_blocks = 2 * n_half
    scale = dim ** -0.5

    def tok_of(n):
        return ((1 - p) + (n // n_half) * (2 * p - 1)) * half + (n % n_half) * TB

    def kv_copies(n):
        slot = n % SLOTS
        src = pl.ds(tok_of(n), TB)
        return (pltpu.make_async_copy(k_hbm.at[layer, src], kbuf.at[slot], ksem.at[slot]),
                pltpu.make_async_copy(v_hbm.at[layer, src], vbuf.at[slot], vsem.at[slot]))

    w_copies = [pltpu.make_async_copy(src.at[layer], dst, wsem.at[i])
                for i, (src, dst) in enumerate(((wq_hbm, wq), (wk_hbm, wk), (wv_hbm, wv), (wo_hbm, wo)))]
    w_copies[0].start()
    for n in range(SLOTS):
        for cp in kv_copies(n):
            cp.start()
    for cp in w_copies[1:]:
        cp.start()

    _greet((to_y, to_x, to_c))

    normed = _rms(x_ref[...].astype(F32)).astype(BF16)
    w_copies[0].wait()
    for h in range(0, heads, 2):
        part = _nn(normed, wq[:, h * dim:(h + 2) * dim]).astype(BF16).astype(F32)
        q3[:, h, :] = part[:, :dim]
        q3[:, h + 1, :] = part[:, dim:]

    row_i = lax.broadcasted_iota(I32, (heads, rows), 0)
    lane_i = lax.broadcasted_iota(I32, (heads, rows), 1)
    posl = jnp.where(lane_i % heads == row_i, lane_i // heads + p * (rows // heads), 1 << 20)
    lane = lax.broadcasted_iota(I32, (heads, 128), 1)

    def block(n, acc):
        slot = n % SLOTS
        for cp in kv_copies(n):
            cp.wait()
        t0 = tok_of(n)
        for j in range(TB):
            q = q3[t0 + j].astype(BF16)
            s = _nt(q, kbuf[slot, j])
            s = jnp.where(posl < len_ref[t0 + j], s * scale, NEG)
            m = jnp.max(s, axis=1, keepdims=True)
            pr = jnp.exp(s - m)
            l = jnp.sum(pr, axis=1, keepdims=True)
            o3[t0 + j] = _nn(pr.astype(BF16), vbuf[slot, j])
            at = (n % n_half) * TB + j
            acc = jnp.where(lane == at, m, acc)
            acc = jnp.where(lane == half + at, l, acc)

        @pl.when(n + SLOTS < n_blocks)
        def _():
            for cp in kv_copies(n + SLOTS):
                cp.start()

        return acc

    theirs = (1 - p) * half
    mine = p * half

    def o_copy(i):
        return _rcopy(o3.at[pl.ds(theirs + i * TB, TB)], o3r.at[pl.ds(i * TB, TB)], osend.at[i], orecv.at[i], to_y)

    def first(n, acc):
        acc = block(n, acc)
        o_copy(n).start()
        return acc

    zero = jnp.zeros((heads, 128), F32)
    mls[...] = lax.fori_loop(0, n_half, first, zero)
    ml_copy = _rcopy(mls, mlr, osend.at[n_half], orecv.at[n_half], to_y)
    ml_copy.start()
    ml_own = lax.fori_loop(n_half, n_blocks, block, zero)

    normed = _rms(x_ref[pl.ds(mine, half), :].astype(F32)).astype(BF16)
    for i, (w, dst) in enumerate(((wk, k3), (wv, v3))):
        w_copies[1 + i].wait()
        for h in range(0, heads, 2):
            part = _nn(normed, w[:, h * dim:(h + 2) * dim]).astype(BF16).astype(F32)
            dst[:, h, :] = part[:, :dim]
            dst[:, h + 1, :] = part[:, dim:]

    sn = zero
    for j in range(half):
        sn = jnp.where(lane == j, jnp.sum(q3[mine + j] * k3[j], axis=1, keepdims=True) * scale, sn)

    for i in range(n_half):
        o_copy(i).wait()
    ml_copy.wait()
    ml_their = mlr[...]
    top = jnp.maximum(jnp.maximum(ml_own, ml_their), sn)
    w_own, w_their, w_new = jnp.exp(ml_own - top), jnp.exp(ml_their - top), jnp.exp(sn - top)
    den = pltpu.roll(ml_own, half, 1) * w_own + pltpu.roll(ml_their, half, 1) * w_their + w_new
    w_own, w_their, w_new = w_own / den, w_their / den, w_new / den
    for j in range(half):
        o3r[j] = (o3[mine + j] * w_own[:, j:j + 1] + o3r[j] * w_their[:, j:j + 1] + v3[j] * w_new[:, j:j + 1])
    for h in range(heads):
        o2[:, h * dim:(h + 1) * dim] = o3r[:, h, :].astype(BF16)
    w_copies[3].wait()
    d_model = x_ref.shape[1]
    a = (x_ref[pl.ds(mine, half), :].astype(F32) + _nn(o2[...], wo[...])).astype(BF16)
    a_own[...] = a
    me = b * 2 + p
    u_all[me] = _rms(a.astype(F32)).astype(BF16)

    y_blk, x_blk = b * 2 + (1 - p), ((1 - x) * 2 + c) * 2 + p
    d_blk = ((1 - x) * 2 + c) * 2 + (1 - p)
    lo, hi = pl.ds(0, half // 2), pl.ds(half // 2, half // 2)

    def u_copy(i, src, peer, part=None):
        ref = u_all.at[src] if part is None else u_all.at[src, part]
        return _rcopy(ref, ref, gsend.at[i], grecv.at[i], peer)

    to_y_own = u_copy(0, me, to_y)
    to_x_own = u_copy(1, me, to_x)
    to_c_own = u_copy(2, me, to_c)
    to_y_own.start()
    to_x_own.start()
    to_c_own.start()
    cw = d_model // 2
    my_cols = pl.ds(pl.multiple_of(p * cw, 128), cw)
    their_cols = pl.ds(pl.multiple_of((1 - p) * cw, 128), cw)
    a_copy = _rcopy(a_own.at[:, their_cols], a_half.at[pl.ds(mine, half)], gsend.at[8], grecv.at[8], to_y)
    a_copy.start()
    a_half[pl.ds(mine, half), :] = a_own[:, my_cols]

    to_y_own.wait_recv()
    fwd_x = u_copy(3, y_blk, to_x, lo)
    fwd_x.start()
    c_y = u_copy(4, y_blk, to_c)
    c_y.start()
    to_x_own.wait_recv()
    fwd_y = u_copy(5, x_blk, to_y, hi)
    fwd_y.start()
    c_x = u_copy(6, x_blk, to_c)
    c_x.start()
    fwd_x.wait_recv()
    fwd_y.wait_recv()
    c_d = u_copy(7, d_blk, to_c)
    c_d.start()
    for cp in (to_c_own, c_y, c_x, c_d, a_copy):
        cp.wait_recv()
    out_u = pltpu.make_async_copy(u_all, u_out, lsem.at[0])
    out_a = pltpu.make_async_copy(a_half, a_out, lsem.at[1])
    out_u.start()
    out_a.start()
    for cp in (to_y_own, to_x_own, to_c_own, fwd_x, c_y, fwd_y, c_x, c_d, a_copy):
        cp.wait_send()
    out_u.wait()
    out_a.wait()


def attention(layer, x, lens, kc, vc, wq, wk, wv, wo):
    tokens, d_model = x.shape
    rows, dim = kc.shape[2], kc.shape[3]
    heads = wq.shape[2] // dim
    half = tokens // 2
    hbm = pl.BlockSpec(memory_space=pl.ANY)
    vmem = pl.BlockSpec(memory_space=pltpu.VMEM)
    scratch = [
        pltpu.VMEM((SLOTS, TB, rows, dim), BF16), pltpu.VMEM((SLOTS, TB, rows, dim), BF16),
        pltpu.VMEM(wq.shape[1:], BF16), pltpu.VMEM(wk.shape[1:], BF16), pltpu.VMEM(wv.shape[1:], BF16), pltpu.VMEM(wo.shape[1:], BF16),
        pltpu.VMEM((tokens, heads, dim), F32), pltpu.VMEM((tokens, heads, dim), F32), pltpu.VMEM((half, heads, dim), F32),
        pltpu.VMEM((half, heads, dim), F32), pltpu.VMEM((half, heads, dim), F32),
        pltpu.VMEM((heads, 128), F32), pltpu.VMEM((heads, 128), F32), pltpu.VMEM((half, heads * dim), BF16),
        pltpu.VMEM((8, half, d_model), BF16), pltpu.VMEM((half, d_model), BF16), pltpu.VMEM((tokens, d_model // 2), BF16),
        pltpu.SemaphoreType.DMA((SLOTS,)), pltpu.SemaphoreType.DMA((SLOTS,)), pltpu.SemaphoreType.DMA((4,)),
        pltpu.SemaphoreType.DMA((half // TB + 1,)), pltpu.SemaphoreType.DMA((half // TB + 1,)),
        pltpu.SemaphoreType.DMA((9,)), pltpu.SemaphoreType.DMA((9,)), pltpu.SemaphoreType.DMA((2,)),
    ]
    u, a = pl.pallas_call(
        functools.partial(attn_kernel, layer),
        out_shape=[jax.ShapeDtypeStruct((8, half, d_model), BF16), jax.ShapeDtypeStruct((tokens, d_model // 2), BF16)],
        in_specs=[vmem, pl.BlockSpec(memory_space=pltpu.SMEM)] + [hbm] * 6,
        out_specs=[hbm, hbm],
        scratch_shapes=scratch,
        compiler_params=pltpu.CompilerParams(collective_id=layer, has_side_effects=True, vmem_limit_bytes=48 << 20),
        name=f"attn{layer}",
    )(x, lens, kc, vc, wq, wk, wv, wo)
    return u.reshape(8 * half, d_model), a


def expert_kernel(off_ref, u_ref, pos_ref, w1_ref, w3_ref, w2_ref, y_ref, x_buf):
    e = pl.program_id(0)
    n_tok = u_ref.shape[0]
    n_rows = x_buf.shape[0] - TILE_M

    @pl.when(e == 0)
    def _():
        step = 128
        for r in range(n_rows // step):
            rid = lax.broadcasted_iota(I32, (step, n_tok), 0) + r * step
            hit = rid == pos_ref[0:1, :]
            for k in range(1, 6):
                hit = hit | (rid == pos_ref[k:k + 1, :])
            pick = jnp.where(hit, 1.0, 0.0).astype(BF16)
            x_buf[r * step:(r + 1) * step, :] = _nn(pick, u_ref[...]).astype(BF16)
        x_buf[n_rows:, :] = jnp.zeros((TILE_M, x_buf.shape[1]), BF16)

    lo, hi = off_ref[e], off_ref[e + 1]
    base = lo // 16 * 16

    def tile(i, carry):
        at = pl.multiple_of(base + i * TILE_M, 16)
        rows = x_buf[pl.ds(at, TILE_M), :]
        h1 = _nt(rows, w1_ref[0, 0])
        h3 = _nt(rows, w3_ref[0, 0])
        act = (h1 * jax.nn.sigmoid(h1) * h3).astype(BF16)
        y = _nn(act, w2_ref[0, 0])
        rid = lax.broadcasted_iota(I32, y.shape, 0) + at
        mask = (rid >= lo) & (rid < hi)
        y_ref[pl.ds(at, TILE_M), :] = jnp.where(mask, y, y_ref[pl.ds(at, TILE_M), :])
        return carry

    lax.fori_loop(0, pl.cdiv(hi - base, TILE_M), tile, 0)


def experts(layer, off, u, pos_t, w1, w3, w2, n_rows):
    n_local, width, d_model = w1.shape[1:]
    wspec = lambda: pl.BlockSpec((1, 1, width, d_model), lambda e, off: (layer, e, 0, 0))
    full = lambda shape: pl.BlockSpec(shape, lambda e, off: (0,) * len(shape))
    return pl.pallas_call(
        expert_kernel,
        out_shape=jax.ShapeDtypeStruct((n_rows + TILE_M, d_model), F32),
        grid_spec=pltpu.PrefetchScalarGridSpec(
            num_scalar_prefetch=1, grid=(n_local,),
            in_specs=[full(u.shape), full(pos_t.shape), wspec(), wspec(), wspec()],
            out_specs=full((n_rows + TILE_M, d_model)),
            scratch_shapes=[pltpu.VMEM((n_rows + TILE_M, d_model), BF16)],
        ),
        compiler_params=pltpu.CompilerParams(dimension_semantics=("arbitrary",), vmem_limit_bytes=40 << 20),
        name=f"experts{layer}",
    )(off, u, pos_t, w1, w3, w2)


N_CH = 4


def combine_kernel(y_ref, u_ref, wr_ref, ids_ref, pos_ref, a_ref, x_out,
                   yr, gm, tb, tcr, txs, txr, xo, ysend, yrecv, csend, crecv, xsend, xrecv, fsend, frecv, lsem):
    p, b, x, c, to_y, to_x, to_c = _where_am_i()
    n_rows, cw = yr.shape[1], yr.shape[2]
    n_tok, top_k = u_ref.shape[0], 6
    tokens = a_ref.shape[0]
    mine, theirs = p * N_CH, (1 - p) * N_CH
    _greet((to_y, to_x, to_c))

    def cols(i):
        return pl.ds(pl.multiple_of(i * cw, 128), cw)

    y_copies = [_rcopy(y_ref.at[pl.ds(0, n_rows), cols(theirs + j)], yr.at[j], ysend.at[j], yrecv.at[j], to_y) for j in range(N_CH)]
    for cp in y_copies:
        cp.start()

    step = 128
    n_exp = wr_ref.shape[1]

    def gates(i, carry):
        at = pl.ds(pl.multiple_of(i * step, step), step)
        logits = _nt(u_ref[at, :].astype(F32), wr_ref[0], precision=lax.Precision.HIGHEST)
        lane = lax.broadcasted_iota(I32, (step, n_exp), 1)
        ids = ids_ref[at, :]
        pos = pos_ref[at, :]
        g = [jnp.sum(jnp.where(lane == ids[:, k:k + 1], logits, 0.0), axis=1, keepdims=True) for k in range(top_k)]
        top = functools.reduce(jnp.maximum, g)
        g = [jnp.exp(v - top) for v in g]
        den = functools.reduce(jnp.add, g)
        g = [v / den for v in g]
        rid = lax.broadcasted_iota(I32, (step, n_rows), 1)
        mat = jnp.zeros((step, n_rows), F32)
        for k in range(top_k):
            mat = jnp.where(rid == pos[:, k:k + 1], g[k], mat)
        g1 = mat.astype(BF16)
        rest = mat - g1.astype(F32)
        g2 = rest.astype(BF16)
        gm[0, at, :] = g1
        gm[1, at, :] = g2
        gm[2, at, :] = (rest - g2.astype(F32)).astype(BF16)
        return carry

    lax.fori_loop(0, n_tok // step, gates, 0)

    f_copies = []
    for j in range(N_CH):
        y_copies[j].wait_recv()
        ys = (y_ref[pl.ds(0, n_rows), cols(mine + j)] + yr[j]).astype(BF16)
        t = _nn(gm[0], ys) + (_nn(gm[1], ys) + _nn(gm[2], ys))
        tb[j] = t.reshape(n_tok // tokens, tokens, cw)
        c_copies = [_rcopy(tb.at[j, i * 2 + (1 - c)], tcr.at[j, i], csend.at[j, i], crecv.at[j, i], to_c) for i in range(2)]
        for cp in c_copies:
            cp.start()
        for cp in c_copies:
            cp.wait_recv()
        txs[j] = tb[j, (1 - x) * 2 + c] + tcr[j, 1 - x]
        x_copy = _rcopy(txs.at[j], txr.at[j], xsend.at[j], xrecv.at[j], to_x)
        x_copy.start()
        own = tb[j, x * 2 + c] + tcr[j, x]
        x_copy.wait_recv()
        new = (a_ref[:, j * cw:(j + 1) * cw].astype(F32) + (own + txr[j])).astype(BF16)
        xo[:, cols(mine + j)] = new
        f_copy = _rcopy(xo.at[:, cols(mine + j)], xo.at[:, cols(mine + j)], fsend.at[j], frecv.at[j], to_y)
        f_copy.start()
        f_copies.append((c_copies, x_copy, f_copy))
    for _, _, f_copy in f_copies:
        f_copy.wait_recv()
    out = pltpu.make_async_copy(xo, x_out, lsem)
    out.start()
    for cp in y_copies:
        cp.wait_send()
    for c_copies, x_copy, f_copy in f_copies:
        for cp in c_copies:
            cp.wait_send()
        x_copy.wait_send()
        f_copy.wait_send()
    out.wait()


def combine(layer, y, u, wr, ids, pos, a, n_rows):
    tokens, half_cols = a.shape
    n_tok, d_model = u.shape
    cw = half_cols // N_CH
    vmem = pl.BlockSpec(memory_space=pltpu.VMEM)
    blocks = n_tok // tokens
    dma = pltpu.SemaphoreType.DMA
    return pl.pallas_call(
        combine_kernel,
        grid=(1,),
        out_shape=jax.ShapeDtypeStruct((tokens, d_model), BF16),
        in_specs=[vmem, vmem, pl.BlockSpec((1,) + wr.shape[1:], lambda i: (layer, 0, 0)), vmem, vmem, vmem],
        out_specs=pl.BlockSpec(memory_space=pl.ANY),
        scratch_shapes=[
            pltpu.VMEM((N_CH, n_rows, cw), F32), pltpu.VMEM((3, n_tok, n_rows), BF16), pltpu.VMEM((N_CH, blocks, tokens, cw), F32),
            pltpu.VMEM((N_CH, 2, tokens, cw), F32), pltpu.VMEM((N_CH, tokens, cw), F32), pltpu.VMEM((N_CH, tokens, cw), F32),
            pltpu.VMEM((tokens, d_model), BF16),
            dma((N_CH,)), dma((N_CH,)), dma((N_CH, 2)), dma((N_CH, 2)), dma((N_CH,)), dma((N_CH,)), dma((N_CH,)), dma((N_CH,)), dma,
        ],
        compiler_params=pltpu.CompilerParams(collective_id=2 + layer, has_side_effects=True, vmem_limit_bytes=48 << 20),
        name=f"combine{layer}",
    )(y, u, wr, ids, pos, a)


def routing(ids, n_local):
    n_tok, top_k = ids.shape[1:]
    local = ids - lax.axis_index("ep") * n_local
    hot = (local[..., None] == jnp.arange(n_local)).astype(F32)
    member = jnp.sum(hot, axis=2)
    tri = (jnp.arange(n_tok)[:, None] >= jnp.arange(n_tok)[None, :]).astype(F32)
    cum = jnp.einsum("ts,lse->lte", tri, member)
    count = cum[:, -1, :]
    ends = jnp.einsum("ef,lf->le", jnp.tril(jnp.ones((n_local, n_local), F32)), count, precision=lax.Precision.HIGHEST)
    first = ends - count
    place = jnp.sum(hot * (first[:, None, None, :] + cum[:, :, None, :] - 1.0), axis=-1)
    inside = (local >= 0) & (local < n_local)
    pos = jnp.where(inside, place, -1.0).astype(I32)
    off = jnp.concatenate([first, ends[:, -1:]], axis=1).astype(I32)
    return pos, off


def solution(mesh):
    tok_spec = P(("dp", "ep"), None)
    cache_spec = P(None, ("dp", "ep"), "pool", None, None)
    up_spec = P(None, "ep", None, "pool")
    down_spec = P(None, "ep", "pool", None)
    in_specs = (tok_spec, cache_spec, cache_spec, P(("dp", "ep")), P(), P(), P(), P(), P(), P(None, ("dp", "ep"), None), up_spec, up_spec, down_spec)
    n_ep = mesh.shape["ep"]

    def body(hidden, kc, vc, lens, wq, wk, wv, wo, wr, ids, w1, w3, w2):
        layers, tokens, seq, heads, dim = kc.shape
        n_local = w1.shape[1]
        top_k = ids.shape[2]
        kc = kc.reshape(layers, tokens, seq * heads, dim)
        vc = vc.reshape(layers, tokens, seq * heads, dim)
        w1 = jnp.swapaxes(w1, 2, 3)
        w3 = jnp.swapaxes(w3, 2, 3)
        wr = jnp.swapaxes(wr, 1, 2)
        ids = lax.all_gather(ids, "ep", axis=1, tiled=True)
        n_rows = tokens * top_k // n_ep * n_ep
        pos, off = routing(ids, n_local)
        wide = ((0, 0), (0, 0), (0, 8 - top_k))
        pos = jnp.pad(pos, wide, constant_values=-1)
        ids = jnp.pad(ids, wide)
        pos_t = jnp.swapaxes(pos, 1, 2)
        for layer in range(layers):
            u, a = attention(layer, hidden, lens, kc, vc, wq, wk, wv, wo)
            y = experts(layer, off[layer], u, pos_t[layer], w1, w3, w2, n_rows)
            hidden = combine(layer, y, u, wr, ids[layer], pos[layer], a, n_rows)
        return hidden

    return jax.shard_map(body, mesh=mesh, in_specs=in_specs, out_specs=tok_spec, check_vma=False)
```

```python
import functools

import jax
import jax.numpy as jnp
from jax import lax
from jax.experimental import pallas as pl
from jax.experimental.pallas import tpu as pltpu
from jax.sharding import PartitionSpec as P

MESH = pl.DeviceIdType.MESH
F32 = jnp.float32
BF16 = jnp.bfloat16
I32 = jnp.int32
EPS = 1e-6
NEG = -1e30
TB = 8
SLOTS = 4
TILE_M = 128


def _nn(a, b):
    return lax.dot_general(a, b, (((1,), (0,)), ((), ())), preferred_element_type=F32)


def _nt(a, b, precision=None):
    return lax.dot_general(a, b, (((1,), (1,)), ((), ())), preferred_element_type=F32, precision=precision)


def _rms(v):
    return v * lax.rsqrt(jnp.mean(v * v, axis=-1, keepdims=True) + EPS)


def _where_am_i():
    p = lax.axis_index("pool")
    b = lax.axis_index("ep")
    x, c = b // 2, b % 2
    to_y = {"pool": 1 - p}
    to_x = {"ep": (1 - x) * 2 + c}
    to_c = {"ep": x * 2 + (1 - c)}
    return p, b, x, c, to_y, to_x, to_c


def _greet(peers):
    sem = pltpu.get_barrier_semaphore()
    for peer in peers:
        pl.semaphore_signal(sem, inc=1, device_id=peer, device_id_type=MESH)
    pl.semaphore_wait(sem, len(peers))


def _rcopy(src, dst, send, recv, peer):
    return pltpu.make_async_remote_copy(src_ref=src, dst_ref=dst, send_sem=send, recv_sem=recv, device_id=peer, device_id_type=MESH)


def _route(b, idg, pos_out, ids_out, off_out):
    n_local, top_k = off_out.shape[1], 6
    n_tok = pos_out.shape[2]
    er = lax.broadcasted_iota(I32, (n_local, n_tok), 0)
    tri = (lax.broadcasted_iota(I32, (n_tok, n_tok), 0) <= lax.broadcasted_iota(I32, (n_tok, n_tok), 1)).astype(F32).astype(BF16)
    before = (lax.broadcasted_iota(I32, (n_local, n_local), 0) > lax.broadcasted_iota(I32, (n_local, n_local), 1)).astype(F32).astype(BF16)
    row = lax.broadcasted_iota(I32, (8, n_tok), 0)
    for layer in range(pos_out.shape[0]):
        ids = jnp.concatenate([idg[i, layer] for i in range(idg.shape[0])], axis=1)
        local = ids - b * n_local
        member = jnp.zeros((n_local, n_tok), F32)
        for k in range(top_k):
            member = member + jnp.where(er == local[k:k + 1, :], 1.0, 0.0)
        member = member.astype(BF16)
        cum = _nn(member, tri)
        first = jnp.sum(_nn(before, member), axis=1, keepdims=True)
        place = first + cum - 1.0
        pos = jnp.full((8, n_tok), -1.0, F32)
        for k in range(top_k):
            lk = local[k:k + 1, :]
            at = jnp.sum(jnp.where(er == lk, place, 0.0), axis=0, keepdims=True)
            at = jnp.where((lk >= 0) & (lk < n_local), at, -1.0)
            pos = jnp.where(row == k, at, pos)
        pos_out[layer] = pos.astype(I32)
        ids_out[layer] = ids
        off_out[layer] = jnp.broadcast_to(first, (n_local, 128)).astype(I32)


def attn_kernel(layer, routed, x_ref, len_ref, k_hbm, v_hbm, wq_hbm, wk_hbm, wv_hbm, wo_hbm, *refs):
    if routed:
        ids_ref, *refs = refs
    u_out, a_out, *refs = refs
    if routed:
        pos_out, ids_out, off_out, *refs, idg, isend, irecv = refs
    (kbuf, vbuf, pbuf, wq, wk, wv, wo, q3, o3, o3r, k3, v3, mls, mlr, o2, u_all, a_own, a_half,
     ksem, vsem, wsem, osend, orecv, gsend, grecv, lsem) = refs
    p, b, x, c, to_y, to_x, to_c = _where_am_i()
    half = x_ref.shape[0] // 2
    heads, dim = q3.shape[1], q3.shape[2]
    cols = heads * dim
    rows = kbuf.shape[2]
    n_half = half // TB
    n_blocks = 2 * n_half
    scale = dim ** -0.5

    def tok_of(n):
        return ((1 - p) + (n // n_half) * (2 * p - 1)) * half + (n % n_half) * TB

    def kv_copies(n):
        slot = n % SLOTS
        src = pl.ds(tok_of(n), TB)
        return (pltpu.make_async_copy(k_hbm.at[layer, src], kbuf.at[slot], ksem.at[slot]),
                pltpu.make_async_copy(v_hbm.at[layer, src], vbuf.at[slot], vsem.at[slot]))

    w_copies = [pltpu.make_async_copy(src.at[layer], dst, wsem.at[i])
                for i, (src, dst) in enumerate(((wq_hbm, wq), (wk_hbm, wk), (wv_hbm, wv), (wo_hbm, wo)))]
    w_copies[0].start()
    for n in range(SLOTS):
        for cp in kv_copies(n):
            cp.start()
    for cp in w_copies[1:]:
        cp.start()

    if routed:
        to_d = {"ep": (1 - x) * 2 + (1 - c)}
        _greet((to_y, to_x, to_c, to_d))
        idg[b] = ids_ref[...]
        id_copies = [_rcopy(ids_ref, idg.at[b], isend.at[i], irecv.at[i], peer) for i, peer in enumerate((to_x, to_c, to_d))]
        for cp in id_copies:
            cp.start()
    else:
        _greet((to_y, to_x, to_c))

    normed = _rms(x_ref[...].astype(F32)).astype(BF16)
    w_copies[0].wait()
    for h in range(0, heads, 2):
        part = _nn(normed, wq[:, h * dim:(h + 2) * dim]).astype(BF16).astype(F32)
        q3[:, h, :] = part[:, :dim]
        q3[:, h + 1, :] = part[:, dim:]

    row_i = lax.broadcasted_iota(I32, (heads, rows), 0)
    lane_i = lax.broadcasted_iota(I32, (heads, rows), 1)
    posl = jnp.where(lane_i % heads == row_i, lane_i // heads + p * (rows // heads), 1 << 20)
    lane = lax.broadcasted_iota(I32, (heads, 128), 1)

    def block(n, acc):
        slot = n % SLOTS
        for cp in kv_copies(n):
            cp.wait()
        t0 = tok_of(n)

        def scores(_, acc):
            for j in range(TB):
                q = q3[t0 + j].astype(BF16)
                s = _nt(q, kbuf[slot, j])
                s = jnp.where(posl < len_ref[t0 + j], s * scale, NEG)
                m = jnp.max(s, axis=1, keepdims=True)
                pr = jnp.exp(s - m)
                l = jnp.sum(pr, axis=1, keepdims=True)
                pbuf[j] = pr.astype(BF16)
                at = (n % n_half) * TB + j
                acc = jnp.where(lane == at, m, acc)
                acc = jnp.where(lane == half + at, l, acc)
            return acc

        def values(_, none):
            for j in range(TB):
                o3[t0 + j] = _nn(pbuf[j], vbuf[slot, j])
            return none

        acc = lax.fori_loop(0, 1, scores, acc)
        lax.fori_loop(0, 1, values, 0)

        @pl.when(n + SLOTS < n_blocks)
        def _():
            for cp in kv_copies(n + SLOTS):
                cp.start()

        return acc

    theirs = (1 - p) * half
    mine = p * half

    def o_copy(i):
        return _rcopy(o3.at[pl.ds(theirs + i * TB, TB)], o3r.at[pl.ds(i * TB, TB)], osend.at[i], orecv.at[i], to_y)

    def first(n, acc):
        acc = block(n, acc)
        o_copy(n).start()
        return acc

    zero = jnp.zeros((heads, 128), F32)
    mls[...] = lax.fori_loop(0, n_half, first, zero)
    ml_copy = _rcopy(mls, mlr, osend.at[n_half], orecv.at[n_half], to_y)
    ml_copy.start()
    ml_own = lax.fori_loop(n_half, n_blocks, block, zero)

    normed = _rms(x_ref[pl.ds(mine, half), :].astype(F32)).astype(BF16)
    for i, (w, dst) in enumerate(((wk, k3), (wv, v3))):
        w_copies[1 + i].wait()
        for h in range(0, heads, 2):
            part = _nn(normed, w[:, h * dim:(h + 2) * dim]).astype(BF16).astype(F32)
            dst[:, h, :] = part[:, :dim]
            dst[:, h + 1, :] = part[:, dim:]

    sn = zero
    for j in range(half):
        sn = jnp.where(lane == j, jnp.sum(q3[mine + j] * k3[j], axis=1, keepdims=True) * scale, sn)

    if routed:
        for cp in id_copies:
            cp.wait()
        _route(b, idg, pos_out, ids_out, off_out)

    for i in range(n_half):
        o_copy(i).wait()
    ml_copy.wait()
    ml_their = mlr[...]
    top = jnp.maximum(jnp.maximum(ml_own, ml_their), sn)
    w_own, w_their, w_new = jnp.exp(ml_own - top), jnp.exp(ml_their - top), jnp.exp(sn - top)
    den = pltpu.roll(ml_own, half, 1) * w_own + pltpu.roll(ml_their, half, 1) * w_their + w_new
    w_own, w_their, w_new = w_own / den, w_their / den, w_new / den
    for j in range(half):
        o3r[j] = (o3[mine + j] * w_own[:, j:j + 1] + o3r[j] * w_their[:, j:j + 1] + v3[j] * w_new[:, j:j + 1])
    for h in range(heads):
        o2[:, h * dim:(h + 1) * dim] = o3r[:, h, :].astype(BF16)
    w_copies[3].wait()
    d_model = x_ref.shape[1]
    a = (x_ref[pl.ds(mine, half), :].astype(F32) + _nn(o2[...], wo[...])).astype(BF16)
    a_own[...] = a
    me = b * 2 + p
    u_all[me] = _rms(a.astype(F32)).astype(BF16)

    y_blk, x_blk = b * 2 + (1 - p), ((1 - x) * 2 + c) * 2 + p
    d_blk = ((1 - x) * 2 + c) * 2 + (1 - p)
    lo, hi = pl.ds(0, half // 2), pl.ds(half // 2, half // 2)

    def u_copy(i, src, peer, part=None):
        ref = u_all.at[src] if part is None else u_all.at[src, part]
        return _rcopy(ref, ref, gsend.at[i], grecv.at[i], peer)

    to_y_own = u_copy(0, me, to_y)
    to_x_own = u_copy(1, me, to_x)
    to_c_own = u_copy(2, me, to_c)
    to_y_own.start()
    to_x_own.start()
    to_c_own.start()
    cw = d_model // 2
    my_cols = pl.ds(pl.multiple_of(p * cw, 128), cw)
    their_cols = pl.ds(pl.multiple_of((1 - p) * cw, 128), cw)
    a_copy = _rcopy(a_own.at[:, their_cols], a_half.at[pl.ds(mine, half)], gsend.at[8], grecv.at[8], to_y)
    a_copy.start()
    a_half[pl.ds(mine, half), :] = a_own[:, my_cols]

    to_y_own.wait_recv()
    fwd_x = u_copy(3, y_blk, to_x, lo)
    fwd_x.start()
    c_y = u_copy(4, y_blk, to_c)
    c_y.start()
    to_x_own.wait_recv()
    fwd_y = u_copy(5, x_blk, to_y, hi)
    fwd_y.start()
    c_x = u_copy(6, x_blk, to_c)
    c_x.start()
    fwd_x.wait_recv()
    fwd_y.wait_recv()
    c_d = u_copy(7, d_blk, to_c)
    c_d.start()
    for cp in (to_c_own, c_y, c_x, c_d, a_copy):
        cp.wait_recv()
    out_u = pltpu.make_async_copy(u_all, u_out, lsem.at[0])
    out_a = pltpu.make_async_copy(a_half, a_out, lsem.at[1])
    out_u.start()
    out_a.start()
    for cp in (to_y_own, to_x_own, to_c_own, fwd_x, c_y, fwd_y, c_x, c_d, a_copy):
        cp.wait_send()
    out_u.wait()
    out_a.wait()


def attention(layer, x, lens, kc, vc, wq, wk, wv, wo, ids=None, n_local=0):
    tokens, d_model = x.shape
    rows, dim = kc.shape[2], kc.shape[3]
    heads = wq.shape[2] // dim
    half = tokens // 2
    hbm = pl.BlockSpec(memory_space=pl.ANY)
    vmem = pl.BlockSpec(memory_space=pltpu.VMEM)
    dma = pltpu.SemaphoreType.DMA
    scratch = [
        pltpu.VMEM((SLOTS, TB, rows, dim), BF16), pltpu.VMEM((SLOTS, TB, rows, dim), BF16), pltpu.VMEM((TB, heads, rows), BF16),
        pltpu.VMEM(wq.shape[1:], BF16), pltpu.VMEM(wk.shape[1:], BF16), pltpu.VMEM(wv.shape[1:], BF16), pltpu.VMEM(wo.shape[1:], BF16),
        pltpu.VMEM((tokens, heads, dim), F32), pltpu.VMEM((tokens, heads, dim), F32), pltpu.VMEM((half, heads, dim), F32),
        pltpu.VMEM((half, heads, dim), F32), pltpu.VMEM((half, heads, dim), F32),
        pltpu.VMEM((heads, 128), F32), pltpu.VMEM((heads, 128), F32), pltpu.VMEM((half, heads * dim), BF16),
        pltpu.VMEM((8, half, d_model), BF16), pltpu.VMEM((half, d_model), BF16), pltpu.VMEM((tokens, d_model // 2), BF16),
        dma((SLOTS,)), dma((SLOTS,)), dma((4,)), dma((half // TB + 1,)), dma((half // TB + 1,)), dma((9,)), dma((9,)), dma((2,)),
    ]
    out_shape = [jax.ShapeDtypeStruct((8, half, d_model), BF16), jax.ShapeDtypeStruct((tokens, d_model // 2), BF16)]
    in_specs = [vmem, pl.BlockSpec(memory_space=pltpu.SMEM)] + [hbm] * 6
    out_specs = [hbm, hbm]
    args = [x, lens, kc, vc, wq, wk, wv, wo]
    if ids is not None:
        layers = ids.shape[0]
        args.append(ids)
        in_specs.append(vmem)
        out_shape += [jax.ShapeDtypeStruct((layers, 8, 8 * half), I32)] * 2 + [jax.ShapeDtypeStruct((layers, n_local, 128), I32)]
        out_specs += [vmem] * 3
        scratch += [pltpu.VMEM((4,) + ids.shape, I32), dma((3,)), dma((3,))]
    u, a, *rest = pl.pallas_call(
        functools.partial(attn_kernel, layer, ids is not None),
        out_shape=out_shape, in_specs=in_specs, out_specs=out_specs, scratch_shapes=scratch,
        compiler_params=pltpu.CompilerParams(collective_id=layer, has_side_effects=True, vmem_limit_bytes=60 << 20),
        name=f"attn{layer}",
    )(*args)
    return (u.reshape(8 * half, d_model), a, *rest)


def expert_kernel(layer, off_ref, u_ref, pos_ref, w1_hbm, w3_hbm, w2_hbm, y_ref, x_buf, act, w1, w3, w2, sem):
    n_tok = u_ref.shape[0]
    n_local = w1.shape[0]
    n_rows = x_buf.shape[0] - TILE_M

    def copies(e):
        return [pltpu.make_async_copy(src.at[layer, e], dst.at[e], sem.at[i, e])
                for i, (src, dst) in enumerate(((w1_hbm, w1), (w3_hbm, w3), (w2_hbm, w2)))]

    for e in range(n_local):
        for cp in copies(e):
            cp.start()

    step = 128
    for r in range(n_rows // step):
        rid = lax.broadcasted_iota(I32, (step, n_tok), 0) + r * step
        hit = rid == pos_ref[0, 0:1, :]
        for k in range(1, 6):
            hit = hit | (rid == pos_ref[0, k:k + 1, :])
        pick = jnp.where(hit, 1.0, 0.0).astype(BF16)
        x_buf[r * step:(r + 1) * step, :] = _nn(pick, u_ref[...]).astype(BF16)
    x_buf[n_rows:, :] = jnp.zeros((TILE_M, x_buf.shape[1]), BF16)

    def expert(e, carry):
        lo = off_ref[layer, e, 0]
        hi = jnp.where(e + 1 < n_local, off_ref[layer, jnp.minimum(e + 1, n_local - 1), 0], n_rows)
        base = lo // 16 * 16
        tiles = pl.cdiv(hi - base, TILE_M)
        for cp in copies(e):
            cp.wait()

        def up(i, none):
            rows = x_buf[pl.ds(pl.multiple_of(base + i * TILE_M, 16), TILE_M), :]
            h1 = _nt(rows, w1[e])
            h3 = _nt(rows, w3[e])
            act[pl.ds(pl.multiple_of(i * TILE_M, TILE_M), TILE_M), :] = (h1 * jax.nn.sigmoid(h1) * h3).astype(BF16)
            return none

        def down(i, none):
            at = pl.multiple_of(base + i * TILE_M, 16)
            y = _nn(act[pl.ds(pl.multiple_of(i * TILE_M, TILE_M), TILE_M), :], w2[e])
            rid = lax.broadcasted_iota(I32, y.shape, 0) + at
            mask = (rid >= lo) & (rid < hi)
            y_ref[pl.ds(at, TILE_M), :] = jnp.where(mask, y, y_ref[pl.ds(at, TILE_M), :])
            return none

        lax.fori_loop(0, tiles, up, 0)
        lax.fori_loop(0, tiles, down, 0)
        return carry

    lax.fori_loop(0, n_local, expert, 0)


def experts(layer, off, u, pos_t, w1, w3, w2, n_rows):
    n_local, width, d_model = w1.shape[1:]
    hbm = pl.BlockSpec(memory_space=pl.ANY)
    vmem = pl.BlockSpec(memory_space=pltpu.VMEM)
    weights = pltpu.VMEM((n_local, width, d_model), BF16)
    return pl.pallas_call(
        functools.partial(expert_kernel, layer),
        grid=(1,),
        out_shape=jax.ShapeDtypeStruct((n_rows + TILE_M, d_model), F32),
        in_specs=[pl.BlockSpec(memory_space=pltpu.SMEM), vmem, pl.BlockSpec((1,) + pos_t.shape[1:], lambda i: (layer, 0, 0)), hbm, hbm, hbm],
        out_specs=vmem,
        scratch_shapes=[pltpu.VMEM((n_rows + TILE_M, d_model), BF16), pltpu.VMEM((n_rows + TILE_M, width), BF16),
                        weights, weights, weights, pltpu.SemaphoreType.DMA((3, n_local))],
        compiler_params=pltpu.CompilerParams(vmem_limit_bytes=56 << 20),
        name=f"experts{layer}",
    )(off, u, pos_t, w1, w3, w2)


N_CH = 4


def combine_kernel(y_ref, u_ref, wr_ref, ids_ref, pos_ref, a_ref, x_out,
                   yr, gm, tb, tcr, txs, txr, xo, ysend, yrecv, csend, crecv, xsend, xrecv, fsend, frecv, lsem):
    p, b, x, c, to_y, to_x, to_c = _where_am_i()
    n_rows, cw = yr.shape[1], yr.shape[2]
    n_tok, top_k = u_ref.shape[0], 6
    tokens = a_ref.shape[0]
    mine, theirs = p * N_CH, (1 - p) * N_CH
    _greet((to_y, to_x, to_c))

    def cols(i):
        return pl.ds(pl.multiple_of(i * cw, 128), cw)

    y_copies = [_rcopy(y_ref.at[pl.ds(0, n_rows), cols(theirs + j)], yr.at[j], ysend.at[j], yrecv.at[j], to_y) for j in range(N_CH)]
    for cp in y_copies:
        cp.start()

    step = 128
    n_exp = wr_ref.shape[1]

    def gates(i, carry):
        at = pl.ds(pl.multiple_of(i * step, step), step)
        logits = _nt(u_ref[at, :].astype(F32), wr_ref[0], precision=lax.Precision.HIGHEST)
        lane = lax.broadcasted_iota(I32, (step, n_exp), 1)
        ids = jnp.transpose(ids_ref[0, :, at].astype(F32)).astype(I32)
        pos = jnp.transpose(pos_ref[0, :, at].astype(F32)).astype(I32)
        g = [jnp.sum(jnp.where(lane == ids[:, k:k + 1], logits, 0.0), axis=1, keepdims=True) for k in range(top_k)]
        top = functools.reduce(jnp.maximum, g)
        g = [jnp.exp(v - top) for v in g]
        den = functools.reduce(jnp.add, g)
        g = [v / den for v in g]
        rid = lax.broadcasted_iota(I32, (step, n_rows), 1)
        mat = jnp.zeros((step, n_rows), F32)
        for k in range(top_k):
            mat = jnp.where(rid == pos[:, k:k + 1], g[k], mat)
        g1 = mat.astype(BF16)
        rest = mat - g1.astype(F32)
        g2 = rest.astype(BF16)
        gm[0, at, :] = g1
        gm[1, at, :] = g2
        gm[2, at, :] = (rest - g2.astype(F32)).astype(BF16)
        return carry

    lax.fori_loop(0, n_tok // step, gates, 0)

    f_copies = []
    for j in range(N_CH):
        y_copies[j].wait_recv()
        ys = (y_ref[pl.ds(0, n_rows), cols(mine + j)] + yr[j]).astype(BF16)
        t = _nn(gm[0], ys) + (_nn(gm[1], ys) + _nn(gm[2], ys))
        tb[j] = t.reshape(n_tok // tokens, tokens, cw)
        c_copies = [_rcopy(tb.at[j, i * 2 + (1 - c)], tcr.at[j, i], csend.at[j, i], crecv.at[j, i], to_c) for i in range(2)]
        for cp in c_copies:
            cp.start()
        for cp in c_copies:
            cp.wait_recv()
        txs[j] = tb[j, (1 - x) * 2 + c] + tcr[j, 1 - x]
        x_copy = _rcopy(txs.at[j], txr.at[j], xsend.at[j], xrecv.at[j], to_x)
        x_copy.start()
        own = tb[j, x * 2 + c] + tcr[j, x]
        x_copy.wait_recv()
        new = (a_ref[:, j * cw:(j + 1) * cw].astype(F32) + (own + txr[j])).astype(BF16)
        xo[:, cols(mine + j)] = new
        f_copy = _rcopy(xo.at[:, cols(mine + j)], xo.at[:, cols(mine + j)], fsend.at[j], frecv.at[j], to_y)
        f_copy.start()
        f_copies.append((c_copies, x_copy, f_copy))
    for _, _, f_copy in f_copies:
        f_copy.wait_recv()
    out = pltpu.make_async_copy(xo, x_out, lsem)
    out.start()
    for cp in y_copies:
        cp.wait_send()
    for c_copies, x_copy, f_copy in f_copies:
        for cp in c_copies:
            cp.wait_send()
        x_copy.wait_send()
        f_copy.wait_send()
    out.wait()


def combine(layer, y, u, wr, ids, pos, a, n_rows):
    tokens, half_cols = a.shape
    n_tok, d_model = u.shape
    cw = half_cols // N_CH
    vmem = pl.BlockSpec(memory_space=pltpu.VMEM)
    blocks = n_tok // tokens
    sliced = lambda arr: pl.BlockSpec((1,) + arr.shape[1:], lambda i: (layer, 0, 0))
    dma = pltpu.SemaphoreType.DMA
    return pl.pallas_call(
        combine_kernel,
        grid=(1,),
        out_shape=jax.ShapeDtypeStruct((tokens, d_model), BF16),
        in_specs=[vmem, vmem, sliced(wr), sliced(ids), sliced(pos), vmem],
        out_specs=pl.BlockSpec(memory_space=pl.ANY),
        scratch_shapes=[
            pltpu.VMEM((N_CH, n_rows, cw), F32), pltpu.VMEM((3, n_tok, n_rows), BF16), pltpu.VMEM((N_CH, blocks, tokens, cw), F32),
            pltpu.VMEM((N_CH, 2, tokens, cw), F32), pltpu.VMEM((N_CH, tokens, cw), F32), pltpu.VMEM((N_CH, tokens, cw), F32),
            pltpu.VMEM((tokens, d_model), BF16),
            dma((N_CH,)), dma((N_CH,)), dma((N_CH, 2)), dma((N_CH, 2)), dma((N_CH,)), dma((N_CH,)), dma((N_CH,)), dma((N_CH,)), dma,
        ],
        compiler_params=pltpu.CompilerParams(collective_id=2 + layer, has_side_effects=True, vmem_limit_bytes=48 << 20),
        name=f"combine{layer}",
    )(y, u, wr, ids, pos, a)


def solution(mesh):
    tok_spec = P(("dp", "ep"), None)
    cache_spec = P(None, ("dp", "ep"), "pool", None, None)
    up_spec = P(None, "ep", None, "pool")
    down_spec = P(None, "ep", "pool", None)
    in_specs = (tok_spec, cache_spec, cache_spec, P(("dp", "ep")), P(), P(), P(), P(), P(), P(None, ("dp", "ep"), None), up_spec, up_spec, down_spec)

    def body(hidden, kc, vc, lens, wq, wk, wv, wo, wr, ids, w1, w3, w2):
        layers, tokens, seq, heads, dim = kc.shape
        n_local = w1.shape[1]
        top_k = ids.shape[2]
        kc = kc.reshape(layers, tokens, seq * heads, dim)
        vc = vc.reshape(layers, tokens, seq * heads, dim)
        w1 = jnp.swapaxes(w1, 2, 3)
        w3 = jnp.swapaxes(w3, 2, 3)
        wr = jnp.swapaxes(wr, 1, 2)
        n_rows = tokens * top_k
        ids = jnp.pad(jnp.swapaxes(ids, 1, 2), ((0, 0), (0, 8 - top_k), (0, 0)))
        for layer in range(layers):
            first = layer == 0
            u, a, *tables = attention(layer, hidden, lens, kc, vc, wq, wk, wv, wo, ids if first else None, n_local)
            if first:
                pos, ids_all, off = tables
            y = experts(layer, off, u, pos, w1, w3, w2, n_rows)
            hidden = combine(layer, y, u, wr, ids_all, pos, a, n_rows)
        return hidden

    return jax.shard_map(body, mesh=mesh, in_specs=in_specs, out_specs=tok_spec, check_vma=False)
```

```python
import functools

import jax
import jax.numpy as jnp
from jax import lax
from jax.experimental import pallas as pl
from jax.experimental.pallas import tpu as pltpu
from jax.sharding import PartitionSpec as P

MESH = pl.DeviceIdType.MESH
F32 = jnp.float32
BF16 = jnp.bfloat16
I32 = jnp.int32
EPS = 1e-6
NEG = -1e30
TB = 8
SLOTS = 4
TILE_M = 128
DEPTH = 4


def _nn(a, b):
    return lax.dot_general(a, b, (((1,), (0,)), ((), ())), preferred_element_type=F32)


def _nt(a, b, precision=None):
    return lax.dot_general(a, b, (((1,), (1,)), ((), ())), preferred_element_type=F32, precision=precision)


def _rms(v):
    return v * lax.rsqrt(jnp.mean(v * v, axis=-1, keepdims=True) + EPS)


def _where_am_i():
    p = lax.axis_index("pool")
    b = lax.axis_index("ep")
    x, c = b // 2, b % 2
    to_y = {"pool": 1 - p}
    to_x = {"ep": (1 - x) * 2 + c}
    to_c = {"ep": x * 2 + (1 - c)}
    return p, b, x, c, to_y, to_x, to_c


def _greet(peers):
    sem = pltpu.get_barrier_semaphore()
    for peer in peers:
        pl.semaphore_signal(sem, inc=1, device_id=peer, device_id_type=MESH)
    pl.semaphore_wait(sem, len(peers))


def _rcopy(src, dst, send, recv, peer):
    return pltpu.make_async_remote_copy(src_ref=src, dst_ref=dst, send_sem=send, recv_sem=recv, device_id=peer, device_id_type=MESH)


def _route(b, idg, pos_out, ids_out, off_out):
    n_local, top_k = off_out.shape[1], 6
    n_tok = pos_out.shape[2]
    er = lax.broadcasted_iota(I32, (n_local, n_tok), 0)
    tri = (lax.broadcasted_iota(I32, (n_tok, n_tok), 0) <= lax.broadcasted_iota(I32, (n_tok, n_tok), 1)).astype(F32).astype(BF16)
    before = (lax.broadcasted_iota(I32, (n_local, n_local), 0) > lax.broadcasted_iota(I32, (n_local, n_local), 1)).astype(F32).astype(BF16)
    row = lax.broadcasted_iota(I32, (8, n_tok), 0)
    for layer in range(pos_out.shape[0]):
        ids = jnp.concatenate([idg[i, layer] for i in range(idg.shape[0])], axis=1)
        local = ids - b * n_local
        member = jnp.zeros((n_local, n_tok), F32)
        for k in range(top_k):
            member = member + jnp.where(er == local[k:k + 1, :], 1.0, 0.0)
        member = member.astype(BF16)
        cum = _nn(member, tri)
        first = jnp.sum(_nn(before, member), axis=1, keepdims=True)
        place = first + cum - 1.0
        pos = jnp.full((8, n_tok), -1.0, F32)
        for k in range(top_k):
            lk = local[k:k + 1, :]
            at = jnp.sum(jnp.where(er == lk, place, 0.0), axis=0, keepdims=True)
            at = jnp.where((lk >= 0) & (lk < n_local), at, -1.0)
            pos = jnp.where(row == k, at, pos)
        pos_out[layer] = pos.astype(I32)
        ids_out[layer] = ids
        off_out[layer] = jnp.broadcast_to(first, (n_local, 128)).astype(I32)


def attn_kernel(layer, routed, x_ref, len_ref, k_hbm, v_hbm, wq_hbm, wk_hbm, wv_hbm, wo_hbm, *refs):
    if routed:
        ids_ref, *refs = refs
    u_out, a_out, *refs = refs
    if routed:
        pos_out, ids_out, off_out, *refs, idg, isend, irecv = refs
    (kbuf, vbuf, pbuf, wq, wk, wv, wo, q3, o3, o3r, k3, v3, mls, mlr, o2, u_all, a_own, a_half,
     ksem, vsem, wsem, osend, orecv, gsend, grecv, lsem) = refs
    p, b, x, c, to_y, to_x, to_c = _where_am_i()
    half = x_ref.shape[0] // 2
    heads, dim = q3.shape[1], q3.shape[2]
    cols = heads * dim
    rows = kbuf.shape[2]
    n_half = half // TB
    n_blocks = 2 * n_half
    scale = dim ** -0.5

    def tok_of(n):
        return ((1 - p) + (n // n_half) * (2 * p - 1)) * half + (n % n_half) * TB

    def kv_copies(n):
        slot = n % SLOTS
        src = pl.ds(tok_of(n), TB)
        return (pltpu.make_async_copy(k_hbm.at[layer, src], kbuf.at[slot], ksem.at[slot]),
                pltpu.make_async_copy(v_hbm.at[layer, src], vbuf.at[slot], vsem.at[slot]))

    w_copies = [pltpu.make_async_copy(src.at[layer], dst, wsem.at[i])
                for i, (src, dst) in enumerate(((wq_hbm, wq), (wk_hbm, wk), (wv_hbm, wv), (wo_hbm, wo)))]
    w_copies[0].start()
    for n in range(SLOTS):
        for cp in kv_copies(n):
            cp.start()
    for cp in w_copies[1:]:
        cp.start()

    if routed:
        to_d = {"ep": (1 - x) * 2 + (1 - c)}
        _greet((to_y, to_x, to_c, to_d))
        idg[b] = ids_ref[...]
        id_copies = [_rcopy(ids_ref, idg.at[b], isend.at[i], irecv.at[i], peer) for i, peer in enumerate((to_x, to_c, to_d))]
        for cp in id_copies:
            cp.start()
    else:
        _greet((to_y, to_x, to_c))

    normed = _rms(x_ref[...].astype(F32)).astype(BF16)
    w_copies[0].wait()
    for h in range(0, heads, 2):
        part = _nn(normed, wq[:, h * dim:(h + 2) * dim]).astype(BF16).astype(F32)
        q3[:, h, :] = part[:, :dim]
        q3[:, h + 1, :] = part[:, dim:]

    row_i = lax.broadcasted_iota(I32, (heads, rows), 0)
    lane_i = lax.broadcasted_iota(I32, (heads, rows), 1)
    posl = jnp.where(lane_i % heads == row_i, lane_i // heads + p * (rows // heads), 1 << 20)
    lane = lax.broadcasted_iota(I32, (heads, 128), 1)

    def block(n, acc):
        slot = n % SLOTS
        for cp in kv_copies(n):
            cp.wait()
        t0 = tok_of(n)

        def scores(_, acc):
            for j in range(TB):
                q = q3[t0 + j].astype(BF16)
                s = _nt(q, kbuf[slot, j])
                s = jnp.where(posl < len_ref[t0 + j], s * scale, NEG)
                m = jnp.max(s, axis=1, keepdims=True)
                pr = jnp.exp(s - m)
                l = jnp.sum(pr, axis=1, keepdims=True)
                pbuf[j] = pr.astype(BF16)
                at = (n % n_half) * TB + j
                acc = jnp.where(lane == at, m, acc)
                acc = jnp.where(lane == half + at, l, acc)
            return acc

        def values(_, none):
            for j in range(TB):
                o3[t0 + j] = _nn(pbuf[j], vbuf[slot, j])
            return none

        acc = lax.fori_loop(0, 1, scores, acc)
        lax.fori_loop(0, 1, values, 0)

        @pl.when(n + SLOTS < n_blocks)
        def _():
            for cp in kv_copies(n + SLOTS):
                cp.start()

        return acc

    theirs = (1 - p) * half
    mine = p * half

    def o_copy(i):
        return _rcopy(o3.at[pl.ds(theirs + i * TB, TB)], o3r.at[pl.ds(i * TB, TB)], osend.at[i], orecv.at[i], to_y)

    def first(n, acc):
        acc = block(n, acc)
        o_copy(n).start()
        return acc

    zero = jnp.zeros((heads, 128), F32)
    mls[...] = lax.fori_loop(0, n_half, first, zero)
    ml_copy = _rcopy(mls, mlr, osend.at[n_half], orecv.at[n_half], to_y)
    ml_copy.start()
    ml_own = lax.fori_loop(n_half, n_blocks, block, zero)

    normed = _rms(x_ref[pl.ds(mine, half), :].astype(F32)).astype(BF16)
    for i, (w, dst) in enumerate(((wk, k3), (wv, v3))):
        w_copies[1 + i].wait()
        for h in range(0, heads, 2):
            part = _nn(normed, w[:, h * dim:(h + 2) * dim]).astype(BF16).astype(F32)
            dst[:, h, :] = part[:, :dim]
            dst[:, h + 1, :] = part[:, dim:]

    sn = zero
    for j in range(half):
        sn = jnp.where(lane == j, jnp.sum(q3[mine + j] * k3[j], axis=1, keepdims=True) * scale, sn)

    if routed:
        for cp in id_copies:
            cp.wait()
        _route(b, idg, pos_out, ids_out, off_out)

    for i in range(n_half):
        o_copy(i).wait()
    ml_copy.wait()
    ml_their = mlr[...]
    top = jnp.maximum(jnp.maximum(ml_own, ml_their), sn)
    w_own, w_their, w_new = jnp.exp(ml_own - top), jnp.exp(ml_their - top), jnp.exp(sn - top)
    den = pltpu.roll(ml_own, half, 1) * w_own + pltpu.roll(ml_their, half, 1) * w_their + w_new
    w_own, w_their, w_new = w_own / den, w_their / den, w_new / den
    for j in range(half):
        o3r[j] = (o3[mine + j] * w_own[:, j:j + 1] + o3r[j] * w_their[:, j:j + 1] + v3[j] * w_new[:, j:j + 1])
    for h in range(heads):
        o2[:, h * dim:(h + 1) * dim] = o3r[:, h, :].astype(BF16)
    w_copies[3].wait()
    d_model = x_ref.shape[1]
    a = (x_ref[pl.ds(mine, half), :].astype(F32) + _nn(o2[...], wo[...])).astype(BF16)
    a_own[...] = a
    me = b * 2 + p
    u_all[me] = _rms(a.astype(F32)).astype(BF16)

    y_blk, x_blk = b * 2 + (1 - p), ((1 - x) * 2 + c) * 2 + p
    d_blk = ((1 - x) * 2 + c) * 2 + (1 - p)
    lo, hi = pl.ds(0, half // 2), pl.ds(half // 2, half // 2)

    def u_copy(i, src, peer, part=None):
        ref = u_all.at[src] if part is None else u_all.at[src, part]
        return _rcopy(ref, ref, gsend.at[i], grecv.at[i], peer)

    to_y_own = u_copy(0, me, to_y)
    to_x_own = u_copy(1, me, to_x)
    to_c_own = u_copy(2, me, to_c)
    to_y_own.start()
    to_x_own.start()
    to_c_own.start()
    cw = d_model // 2
    my_cols = pl.ds(pl.multiple_of(p * cw, 128), cw)
    their_cols = pl.ds(pl.multiple_of((1 - p) * cw, 128), cw)
    a_copy = _rcopy(a_own.at[:, their_cols], a_half.at[pl.ds(mine, half)], gsend.at[8], grecv.at[8], to_y)
    a_copy.start()
    a_half[pl.ds(mine, half), :] = a_own[:, my_cols]

    to_y_own.wait_recv()
    fwd_x = u_copy(3, y_blk, to_x, lo)
    fwd_x.start()
    c_y = u_copy(4, y_blk, to_c)
    c_y.start()
    to_x_own.wait_recv()
    fwd_y = u_copy(5, x_blk, to_y, hi)
    fwd_y.start()
    c_x = u_copy(6, x_blk, to_c)
    c_x.start()
    fwd_x.wait_recv()
    fwd_y.wait_recv()
    c_d = u_copy(7, d_blk, to_c)
    c_d.start()
    for cp in (to_c_own, c_y, c_x, c_d, a_copy):
        cp.wait_recv()
    out_u = pltpu.make_async_copy(u_all, u_out, lsem.at[0])
    out_a = pltpu.make_async_copy(a_half, a_out, lsem.at[1])
    out_u.start()
    out_a.start()
    for cp in (to_y_own, to_x_own, to_c_own, fwd_x, c_y, fwd_y, c_x, c_d, a_copy):
        cp.wait_send()
    out_u.wait()
    out_a.wait()


def attention(layer, x, lens, kc, vc, wq, wk, wv, wo, ids=None, n_local=0):
    tokens, d_model = x.shape
    rows, dim = kc.shape[2], kc.shape[3]
    heads = wq.shape[2] // dim
    half = tokens // 2
    hbm = pl.BlockSpec(memory_space=pl.ANY)
    vmem = pl.BlockSpec(memory_space=pltpu.VMEM)
    dma = pltpu.SemaphoreType.DMA
    scratch = [
        pltpu.VMEM((SLOTS, TB, rows, dim), BF16), pltpu.VMEM((SLOTS, TB, rows, dim), BF16), pltpu.VMEM((TB, heads, rows), BF16),
        pltpu.VMEM(wq.shape[1:], BF16), pltpu.VMEM(wk.shape[1:], BF16), pltpu.VMEM(wv.shape[1:], BF16), pltpu.VMEM(wo.shape[1:], BF16),
        pltpu.VMEM((tokens, heads, dim), F32), pltpu.VMEM((tokens, heads, dim), F32), pltpu.VMEM((half, heads, dim), F32),
        pltpu.VMEM((half, heads, dim), F32), pltpu.VMEM((half, heads, dim), F32),
        pltpu.VMEM((heads, 128), F32), pltpu.VMEM((heads, 128), F32), pltpu.VMEM((half, heads * dim), BF16),
        pltpu.VMEM((8, half, d_model), BF16), pltpu.VMEM((half, d_model), BF16), pltpu.VMEM((tokens, d_model // 2), BF16),
        dma((SLOTS,)), dma((SLOTS,)), dma((4,)), dma((half // TB + 1,)), dma((half // TB + 1,)), dma((9,)), dma((9,)), dma((2,)),
    ]
    out_shape = [jax.ShapeDtypeStruct((8, half, d_model), BF16), jax.ShapeDtypeStruct((tokens, d_model // 2), BF16)]
    in_specs = [vmem, pl.BlockSpec(memory_space=pltpu.SMEM)] + [hbm] * 6
    out_specs = [hbm, hbm]
    args = [x, lens, kc, vc, wq, wk, wv, wo]
    if ids is not None:
        layers = ids.shape[0]
        args.append(ids)
        in_specs.append(vmem)
        out_shape += [jax.ShapeDtypeStruct((layers, 8, 8 * half), I32)] * 2 + [jax.ShapeDtypeStruct((layers, n_local, 128), I32)]
        out_specs += [vmem] * 3
        scratch += [pltpu.VMEM((4,) + ids.shape, I32), dma((3,)), dma((3,))]
    u, a, *rest = pl.pallas_call(
        functools.partial(attn_kernel, layer, ids is not None),
        out_shape=out_shape, in_specs=in_specs, out_specs=out_specs, scratch_shapes=scratch,
        compiler_params=pltpu.CompilerParams(collective_id=layer, has_side_effects=True, vmem_limit_bytes=60 << 20),
        name=f"attn{layer}",
    )(*args)
    return (u.reshape(8 * half, d_model), a, *rest)


def expert_kernel(layer, part, off_ref, u_ref, pos_ref, w1_hbm, w3_hbm, w2_hbm, own_out, send_out,
                  xt, act, y_buf, w1, w3, w2, t_exp, t_at, t_new, t_lo, t_hi, live, sem, osem):
    n_tok = u_ref.shape[0]
    n_local = w1.shape[0]
    n_rows = own_out.shape[0]
    start = part * n_rows
    weights = ((w1_hbm, w1), (w3_hbm, w3), (w2_hbm, w2))

    def copies(e):
        return [pltpu.make_async_copy(src.at[layer, e], dst.at[e], sem.at[i, e]) for i, (src, dst) in enumerate(weights)]

    def plan(e, state):
        t, n = state
        end = jnp.where(e + 1 < n_local, off_ref[layer, jnp.minimum(e + 1, n_local - 1), 0], start + n_rows)
        lo = jnp.maximum(off_ref[layer, e, 0] - start, 0)
        hi = jnp.minimum(end - start, n_rows)
        base = lo // 16 * 16
        live[n] = e

        def put(i, t):
            t_exp[t] = e
            t_at[t] = base + i * TILE_M
            t_new[t] = jnp.where(i == 0, n + 1, 0)
            t_lo[t] = lo
            t_hi[t] = hi
            return t + 1

        some = lo < hi
        return lax.fori_loop(0, jnp.where(some, pl.cdiv(hi - base, TILE_M), 0), put, t), jnp.where(some, n + 1, n)

    tiles, n_live = lax.fori_loop(0, n_local, plan, (0, 0))
    t_new[tiles] = 0

    def start_nth(i):
        @pl.when(i < n_live)
        def _():
            for cp in copies(live[i]):
                cp.start()

    for i in range(DEPTH):
        start_nth(i)

    step = 128
    for r in range(n_rows // step):
        rid = lax.broadcasted_iota(I32, (step, n_tok), 0) + (r * step + start)
        hit = rid == pos_ref[0, 0:1, :]
        for k in range(1, 6):
            hit = hit | (rid == pos_ref[0, k:k + 1, :])
        rows = _nn(jnp.where(hit, 1.0, 0.0).astype(BF16), u_ref[...])
        xt[:, r * step:(r + 1) * step] = jnp.transpose(rows).astype(BF16)
    xt[:, n_rows:] = jnp.zeros((xt.shape[0], xt.shape[1] - n_rows), BF16)

    def arrive(k):
        @pl.when(t_new[k] > 0)
        def _():
            for cp in copies(t_exp[k]):
                cp.wait()
            start_nth(t_new[k] - 1 + DEPTH)

    def up(k):
        e, at = t_exp[k], t_at[k]
        cols = xt[:, pl.ds(pl.multiple_of(at // 128 * 128, 128), 2 * TILE_M)]
        h1 = _nn(w1[e], cols)
        h3 = _nn(w3[e], cols)
        return jnp.transpose(h1 * jax.nn.sigmoid(h1) * h3).astype(BF16)

    def down(k):
        at = pl.multiple_of(t_at[k], 16)
        y = _nn(act[k % 2, pl.ds(pl.multiple_of(t_at[k] % 128, 16), TILE_M), :], w2[t_exp[k]])
        rid = lax.broadcasted_iota(I32, y.shape, 0) + at
        mask = (rid >= t_lo[k]) & (rid < t_hi[k])
        y_buf[pl.ds(at, TILE_M), :] = jnp.where(mask, y, y_buf[pl.ds(at, TILE_M), :])

    arrive(0)
    arrive(1)
    act[0] = up(0)

    def both(k, none):
        arrive(k + 1)
        act[k % 2] = up(k)
        down(k - 1)
        return none

    lax.fori_loop(1, tiles, both, 0)
    down(tiles - 1)
    p = lax.axis_index("pool")
    cw = own_out.shape[1]
    outs = [pltpu.make_async_copy(y_buf.at[pl.ds(0, n_rows), pl.ds(pl.multiple_of(q * cw, 128), cw)], dst, osem.at[i])
            for i, (q, dst) in enumerate(((1 - p, send_out), (p, own_out)))]
    for cp in outs:
        cp.start()
    for cp in outs:
        cp.wait()


def experts(layer, part, off, u, pos_t, w1, w3, w2, n_rows):
    n_local, width, d_model = w1.shape[1:]
    hbm = pl.BlockSpec(memory_space=pl.ANY)
    vmem = pl.BlockSpec(memory_space=pltpu.VMEM)
    weights = pltpu.VMEM((n_local, width, d_model), BF16)
    table = pltpu.SMEM((64,), I32)
    return pl.pallas_call(
        functools.partial(expert_kernel, layer, part),
        grid=(1,),
        out_shape=[jax.ShapeDtypeStruct((n_rows, d_model // 2), F32)] * 2,
        in_specs=[pl.BlockSpec(memory_space=pltpu.SMEM), vmem, pl.BlockSpec((1,) + pos_t.shape[1:], lambda i: (layer, 0, 0)), hbm, hbm, hbm],
        out_specs=[hbm, hbm],
        scratch_shapes=[pltpu.VMEM((d_model, n_rows + 2 * TILE_M), BF16), pltpu.VMEM((2, 2 * TILE_M, width), BF16),
                        pltpu.VMEM((n_rows + TILE_M, d_model), F32), weights, weights, weights,
                        table, table, table, table, table, table, pltpu.SemaphoreType.DMA((3, n_local)), pltpu.SemaphoreType.DMA((2,))],
        compiler_params=pltpu.CompilerParams(vmem_limit_bytes=45 << 20),
        cost_estimate=pl.CostEstimate(flops=int(1.2e10), bytes_accessed=18 << 20, transcendentals=0),
        name=f"experts{layer}{part}",
    )(off, u, pos_t, w1, w3, w2)


N_CH = 4


def combine_kernel(own1_ref, got1_ref, own2_ref, send2_ref, u_ref, wr_ref, ids_ref, pos_ref, a_ref, x_out,
                   yr, gm, tb, tcr, txs, txr, xo, ysend, yrecv, csend, crecv, xsend, xrecv, fsend, frecv, lsem):
    p, b, x, c, to_y, to_x, to_c = _where_am_i()
    half_rows, cw = yr.shape[1], yr.shape[2]
    n_rows = 2 * half_rows
    n_tok, top_k = u_ref.shape[0], 6
    tokens = a_ref.shape[0]
    mine = p * N_CH
    _greet((to_y, to_x, to_c))

    def cols(i):
        return pl.ds(pl.multiple_of(i * cw, 128), cw)

    y_copies = [_rcopy(send2_ref.at[:, j * cw:(j + 1) * cw], yr.at[j], ysend.at[j], yrecv.at[j], to_y) for j in range(N_CH)]
    for cp in y_copies:
        cp.start()

    step = 128
    n_exp = wr_ref.shape[1]

    def gates(i, carry):
        at = pl.ds(pl.multiple_of(i * step, step), step)
        logits = _nt(u_ref[at, :].astype(F32), wr_ref[0], precision=lax.Precision.HIGHEST)
        lane = lax.broadcasted_iota(I32, (step, n_exp), 1)
        ids = jnp.transpose(ids_ref[0, :, at].astype(F32)).astype(I32)
        pos = jnp.transpose(pos_ref[0, :, at].astype(F32)).astype(I32)
        g = [jnp.sum(jnp.where(lane == ids[:, k:k + 1], logits, 0.0), axis=1, keepdims=True) for k in range(top_k)]
        top = functools.reduce(jnp.maximum, g)
        g = [jnp.exp(v - top) for v in g]
        den = functools.reduce(jnp.add, g)
        g = [v / den for v in g]
        rid = lax.broadcasted_iota(I32, (step, n_rows), 1)
        mat = jnp.zeros((step, n_rows), F32)
        for k in range(top_k):
            mat = jnp.where(rid == pos[:, k:k + 1], g[k], mat)
        g1 = mat.astype(BF16)
        rest = mat - g1.astype(F32)
        g2 = rest.astype(BF16)
        gm[0, at, :] = g1
        gm[1, at, :] = g2
        gm[2, at, :] = (rest - g2.astype(F32)).astype(BF16)
        return carry

    lax.fori_loop(0, n_tok // step, gates, 0)

    def gated(ys, rows):
        return _nn(gm[0, :, rows], ys) + (_nn(gm[1, :, rows], ys) + _nn(gm[2, :, rows], ys))

    for j in range(N_CH):
        ys = (own1_ref[:, j * cw:(j + 1) * cw] + got1_ref[:, j * cw:(j + 1) * cw]).astype(BF16)
        tb[j] = gated(ys, pl.ds(0, half_rows)).reshape(n_tok // tokens, tokens, cw)

    f_copies = []
    for j in range(N_CH):
        y_copies[j].wait_recv()
        ys = (own2_ref[:, j * cw:(j + 1) * cw] + yr[j]).astype(BF16)
        tb[j] = tb[j] + gated(ys, pl.ds(half_rows, half_rows)).reshape(n_tok // tokens, tokens, cw)
        c_copies = [_rcopy(tb.at[j, i * 2 + (1 - c)], tcr.at[j, i], csend.at[j, i], crecv.at[j, i], to_c) for i in range(2)]
        for cp in c_copies:
            cp.start()
        for cp in c_copies:
            cp.wait_recv()
        txs[j] = tb[j, (1 - x) * 2 + c] + tcr[j, 1 - x]
        x_copy = _rcopy(txs.at[j], txr.at[j], xsend.at[j], xrecv.at[j], to_x)
        x_copy.start()
        own = tb[j, x * 2 + c] + tcr[j, x]
        x_copy.wait_recv()
        new = (a_ref[:, j * cw:(j + 1) * cw].astype(F32) + (own + txr[j])).astype(BF16)
        xo[:, cols(mine + j)] = new
        f_copy = _rcopy(xo.at[:, cols(mine + j)], xo.at[:, cols(mine + j)], fsend.at[j], frecv.at[j], to_y)
        f_copy.start()
        f_copies.append((c_copies, x_copy, f_copy))
    for _, _, f_copy in f_copies:
        f_copy.wait_recv()
    out = pltpu.make_async_copy(xo, x_out, lsem)
    out.start()
    for cp in y_copies:
        cp.wait_send()
    for c_copies, x_copy, f_copy in f_copies:
        for cp in c_copies:
            cp.wait_send()
        x_copy.wait_send()
        f_copy.wait_send()
    out.wait()


def combine(layer, own1, got1, own2, send2, u, wr, ids, pos, a):
    half_rows = own1.shape[0]
    n_rows = 2 * half_rows
    tokens, half_cols = a.shape
    n_tok, d_model = u.shape
    cw = half_cols // N_CH
    vmem = pl.BlockSpec(memory_space=pltpu.VMEM)
    blocks = n_tok // tokens
    sliced = lambda arr: pl.BlockSpec((1,) + arr.shape[1:], lambda i: (layer, 0, 0))
    dma = pltpu.SemaphoreType.DMA
    return pl.pallas_call(
        combine_kernel,
        grid=(1,),
        out_shape=jax.ShapeDtypeStruct((tokens, d_model), BF16),
        in_specs=[vmem] * 5 + [sliced(wr), sliced(ids), sliced(pos), vmem],
        out_specs=pl.BlockSpec(memory_space=pl.ANY),
        scratch_shapes=[
            pltpu.VMEM((N_CH, half_rows, cw), F32), pltpu.VMEM((3, n_tok, n_rows), BF16), pltpu.VMEM((N_CH, blocks, tokens, cw), F32),
            pltpu.VMEM((N_CH, 2, tokens, cw), F32), pltpu.VMEM((N_CH, tokens, cw), F32), pltpu.VMEM((N_CH, tokens, cw), F32),
            pltpu.VMEM((tokens, d_model), BF16),
            dma((N_CH,)), dma((N_CH,)), dma((N_CH, 2)), dma((N_CH, 2)), dma((N_CH,)), dma((N_CH,)), dma((N_CH,)), dma((N_CH,)), dma,
        ],
        compiler_params=pltpu.CompilerParams(collective_id=2 + layer, has_side_effects=True, vmem_limit_bytes=48 << 20),
        name=f"combine{layer}",
    )(own1, got1, own2, send2, u, wr, ids, pos, a)


def solution(mesh):
    tok_spec = P(("dp", "ep"), None)
    cache_spec = P(None, ("dp", "ep"), "pool", None, None)
    up_spec = P(None, "ep", None, "pool")
    down_spec = P(None, "ep", "pool", None)
    in_specs = (tok_spec, cache_spec, cache_spec, P(("dp", "ep")), P(), P(), P(), P(), P(), P(None, ("dp", "ep"), None), up_spec, up_spec, down_spec)

    def body(hidden, kc, vc, lens, wq, wk, wv, wo, wr, ids, w1, w3, w2):
        layers, tokens, seq, heads, dim = kc.shape
        n_local = w1.shape[1]
        top_k = ids.shape[2]
        kc = kc.reshape(layers, tokens, seq * heads, dim)
        vc = vc.reshape(layers, tokens, seq * heads, dim)
        w1 = jnp.swapaxes(w1, 2, 3)
        w3 = jnp.swapaxes(w3, 2, 3)
        wr = jnp.swapaxes(wr, 1, 2)
        n_rows = tokens * top_k
        ids = jnp.pad(jnp.swapaxes(ids, 1, 2), ((0, 0), (0, 8 - top_k), (0, 0)))
        for layer in range(layers):
            first = layer == 0
            u, a, *tables = attention(layer, hidden, lens, kc, vc, wq, wk, wv, wo, ids if first else None, n_local)
            if first:
                pos, ids_all, off = tables
            own1, send1 = experts(layer, 0, off, u, pos, w1, w3, w2, n_rows // 2)
            got1 = lax.ppermute(send1, "pool", [(0, 1), (1, 0)])
            own2, send2 = experts(layer, 1, off, u, pos, w1, w3, w2, n_rows // 2)
            hidden = combine(layer, own1, got1, own2, send2, u, wr, ids_all, pos, a)
        return hidden

    return jax.shard_map(body, mesh=mesh, in_specs=in_specs, out_specs=tok_spec, check_vma=False)
```

```python
import functools

import jax
import jax.numpy as jnp
from jax import lax
from jax.experimental import pallas as pl
from jax.experimental.pallas import tpu as pltpu
from jax.sharding import PartitionSpec as P

MESH = pl.DeviceIdType.MESH
F32 = jnp.float32
BF16 = jnp.bfloat16
I32 = jnp.int32
EPS = 1e-6
NEG = -1e30
TB = 8
SLOTS = 4
TILE_M = 128
DEPTH = 4
VMEM_MIB = (51, 34)


def _nn(a, b):
    return lax.dot_general(a, b, (((1,), (0,)), ((), ())), preferred_element_type=F32)


def _nt(a, b, precision=None):
    return lax.dot_general(a, b, (((1,), (1,)), ((), ())), preferred_element_type=F32, precision=precision)


def _rms(v):
    return v * lax.rsqrt(jnp.mean(v * v, axis=-1, keepdims=True) + EPS)


def _where_am_i():
    p = lax.axis_index("pool")
    b = lax.axis_index("ep")
    x, c = b // 2, b % 2
    to_y = {"pool": 1 - p}
    to_x = {"ep": (1 - x) * 2 + c}
    to_c = {"ep": x * 2 + (1 - c)}
    return p, b, x, c, to_y, to_x, to_c


def _greet(peers):
    sem = pltpu.get_barrier_semaphore()
    for peer in peers:
        pl.semaphore_signal(sem, inc=1, device_id=peer, device_id_type=MESH)
    pl.semaphore_wait(sem, len(peers))


def _rcopy(src, dst, send, recv, peer):
    return pltpu.make_async_remote_copy(src_ref=src, dst_ref=dst, send_sem=send, recv_sem=recv, device_id=peer, device_id_type=MESH)


def _route(b, idg, pos_out, ids_out, off_out):
    n_local, top_k = off_out.shape[1], 6
    n_tok = pos_out.shape[2]
    er = lax.broadcasted_iota(I32, (n_local, n_tok), 0)
    tri = (lax.broadcasted_iota(I32, (n_tok, n_tok), 0) <= lax.broadcasted_iota(I32, (n_tok, n_tok), 1)).astype(F32).astype(BF16)
    before = (lax.broadcasted_iota(I32, (n_local, n_local), 0) > lax.broadcasted_iota(I32, (n_local, n_local), 1)).astype(F32).astype(BF16)
    row = lax.broadcasted_iota(I32, (8, n_tok), 0)
    for layer in range(pos_out.shape[0]):
        ids = jnp.concatenate([idg[i, layer] for i in range(idg.shape[0])], axis=1)
        local = ids - b * n_local
        member = jnp.zeros((n_local, n_tok), F32)
        for k in range(top_k):
            member = member + jnp.where(er == local[k:k + 1, :], 1.0, 0.0)
        member = member.astype(BF16)
        cum = _nn(member, tri)
        first = jnp.sum(_nn(before, member), axis=1, keepdims=True)
        place = first + cum - 1.0
        pos = jnp.full((8, n_tok), -1.0, F32)
        for k in range(top_k):
            lk = local[k:k + 1, :]
            at = jnp.sum(jnp.where(er == lk, place, 0.0), axis=0, keepdims=True)
            at = jnp.where((lk >= 0) & (lk < n_local), at, -1.0)
            pos = jnp.where(row == k, at, pos)
        pos_out[layer] = pos.astype(I32)
        ids_out[layer] = ids
        off_out[layer] = jnp.broadcast_to(first, (n_local, 128)).astype(I32)


def attn_kernel(layer, routed, x_ref, len_ref, k_hbm, v_hbm, wq_hbm, wk_hbm, wv_hbm, wo_hbm, *refs):
    if routed:
        ids_ref, *refs = refs
    u_out, a_out, a_send, *refs = refs
    if routed:
        pos_out, ids_out, off_out, *refs, idg, isend, irecv = refs
    (kbuf, vbuf, pbuf, wq, wk, wv, wo, q3, o3, o3r, k3, v3, mls, mlr, o2, u_all, a_own,
     ksem, vsem, wsem, osend, orecv, gsend, grecv, lsem) = refs
    p, b, x, c, to_y, to_x, to_c = _where_am_i()
    half = x_ref.shape[0] // 2
    heads, dim = q3.shape[1], q3.shape[2]
    cols = heads * dim
    rows = kbuf.shape[2]
    n_half = half // TB
    n_blocks = 2 * n_half
    scale = dim ** -0.5

    def tok_of(n):
        return ((1 - p) + (n // n_half) * (2 * p - 1)) * half + (n % n_half) * TB

    def kv_copies(n):
        slot = n % SLOTS
        src = pl.ds(tok_of(n), TB)
        return (pltpu.make_async_copy(k_hbm.at[layer, src], kbuf.at[slot], ksem.at[slot]),
                pltpu.make_async_copy(v_hbm.at[layer, src], vbuf.at[slot], vsem.at[slot]))

    w_copies = [pltpu.make_async_copy(src.at[layer], dst, wsem.at[i])
                for i, (src, dst) in enumerate(((wq_hbm, wq), (wk_hbm, wk), (wv_hbm, wv), (wo_hbm, wo)))]
    w_copies[0].start()
    for n in range(SLOTS):
        for cp in kv_copies(n):
            cp.start()
    for cp in w_copies[1:]:
        cp.start()

    if routed:
        to_d = {"ep": (1 - x) * 2 + (1 - c)}
        _greet((to_y, to_x, to_c, to_d))
        idg[b] = ids_ref[...]
        id_copies = [_rcopy(ids_ref, idg.at[b], isend.at[i], irecv.at[i], peer) for i, peer in enumerate((to_x, to_c, to_d))]
        for cp in id_copies:
            cp.start()
    else:
        _greet((to_y, to_x, to_c))

    normed = _rms(x_ref[...].astype(F32)).astype(BF16)
    w_copies[0].wait()
    for h in range(0, heads, 2):
        part = _nn(normed, wq[:, h * dim:(h + 2) * dim]).astype(BF16).astype(F32)
        q3[:, h, :] = part[:, :dim]
        q3[:, h + 1, :] = part[:, dim:]

    row_i = lax.broadcasted_iota(I32, (heads, rows), 0)
    lane_i = lax.broadcasted_iota(I32, (heads, rows), 1)
    posl = jnp.where(lane_i % heads == row_i, lane_i // heads + p * (rows // heads), 1 << 20)
    lane = lax.broadcasted_iota(I32, (heads, 128), 1)

    def block(n, acc):
        slot = n % SLOTS
        for cp in kv_copies(n):
            cp.wait()
        t0 = tok_of(n)

        def scores(_, acc):
            for j in range(TB):
                q = q3[t0 + j].astype(BF16)
                s = _nt(q, kbuf[slot, j])
                s = jnp.where(posl < len_ref[t0 + j], s * scale, NEG)
                m = jnp.max(s, axis=1, keepdims=True)
                pr = jnp.exp(s - m)
                l = jnp.sum(pr, axis=1, keepdims=True)
                pbuf[j] = pr.astype(BF16)
                at = (n % n_half) * TB + j
                acc = jnp.where(lane == at, m, acc)
                acc = jnp.where(lane == half + at, l, acc)
            return acc

        def values(_, none):
            for j in range(TB):
                o3[t0 + j] = _nn(pbuf[j], vbuf[slot, j])
            return none

        acc = lax.fori_loop(0, 1, scores, acc)
        lax.fori_loop(0, 1, values, 0)

        @pl.when(n + SLOTS < n_blocks)
        def _():
            for cp in kv_copies(n + SLOTS):
                cp.start()

        return acc

    theirs = (1 - p) * half
    mine = p * half

    def o_copy(i):
        return _rcopy(o3.at[pl.ds(theirs + i * TB, TB)], o3r.at[pl.ds(i * TB, TB)], osend.at[i], orecv.at[i], to_y)

    def first(n, acc):
        acc = block(n, acc)
        o_copy(n).start()
        return acc

    zero = jnp.zeros((heads, 128), F32)
    mls[...] = lax.fori_loop(0, n_half, first, zero)
    ml_copy = _rcopy(mls, mlr, osend.at[n_half], orecv.at[n_half], to_y)
    ml_copy.start()
    normed = _rms(x_ref[pl.ds(mine, half), :].astype(F32)).astype(BF16)
    for i, (w, dst) in enumerate(((wk, k3), (wv, v3))):
        w_copies[1 + i].wait()
        for h in range(0, heads, 2):
            part = _nn(normed, w[:, h * dim:(h + 2) * dim]).astype(BF16).astype(F32)
            dst[:, h, :] = part[:, :dim]
            dst[:, h + 1, :] = part[:, dim:]

    sn = zero
    for j in range(half):
        sn = jnp.where(lane == j, jnp.sum(q3[mine + j] * k3[j], axis=1, keepdims=True) * scale, sn)

    if routed:
        for cp in id_copies:
            cp.wait()
        _route(b, idg, pos_out, ids_out, off_out)

    ml_own = lax.fori_loop(n_half, n_blocks, block, zero)

    for i in range(n_half):
        o_copy(i).wait()
    ml_copy.wait()
    ml_their = mlr[...]
    top = jnp.maximum(jnp.maximum(ml_own, ml_their), sn)
    w_own, w_their, w_new = jnp.exp(ml_own - top), jnp.exp(ml_their - top), jnp.exp(sn - top)
    den = pltpu.roll(ml_own, half, 1) * w_own + pltpu.roll(ml_their, half, 1) * w_their + w_new
    w_own, w_their, w_new = w_own / den, w_their / den, w_new / den
    for j in range(half):
        o3r[j] = (o3[mine + j] * w_own[:, j:j + 1] + o3r[j] * w_their[:, j:j + 1] + v3[j] * w_new[:, j:j + 1])
    for h in range(heads):
        o2[:, h * dim:(h + 1) * dim] = o3r[:, h, :].astype(BF16)
    w_copies[3].wait()
    d_model = x_ref.shape[1]
    a = (x_ref[pl.ds(mine, half), :].astype(F32) + _nn(o2[...], wo[...])).astype(BF16)
    a_own[...] = a
    me = b * 2 + p
    u_all[me] = _rms(a.astype(F32)).astype(BF16)

    y_blk, x_blk = b * 2 + (1 - p), ((1 - x) * 2 + c) * 2 + p
    d_blk = ((1 - x) * 2 + c) * 2 + (1 - p)
    lo, hi = pl.ds(0, half // 2), pl.ds(half // 2, half // 2)

    def u_copy(i, src, peer, part=None):
        ref = u_all.at[src] if part is None else u_all.at[src, part]
        return _rcopy(ref, ref, gsend.at[i], grecv.at[i], peer)

    own_y = [u_copy(0, me, to_y, lo), u_copy(1, me, to_y, hi)]
    own_x = [u_copy(2, me, to_x, hi), u_copy(3, me, to_x, lo)]
    own_c = u_copy(4, me, to_c)
    for cp in (own_y[0], own_x[0], own_y[1], own_x[1], own_c):
        cp.start()
    cw = d_model // 2
    outs = [pltpu.make_async_copy(a_own.at[:, pl.ds(pl.multiple_of(q * cw, 128), cw)], dst, lsem.at[1 + i])
            for i, (q, dst) in enumerate(((1 - p, a_send), (p, a_out)))]
    for cp in outs:
        cp.start()
    own_y[0].wait_recv()
    fwd_x = u_copy(5, y_blk, to_x, lo)
    fwd_x.start()
    own_x[0].wait_recv()
    fwd_y = u_copy(6, x_blk, to_y, hi)
    fwd_y.start()
    own_y[1].wait_recv()
    c_y = u_copy(7, y_blk, to_c)
    c_y.start()
    own_x[1].wait_recv()
    c_x = u_copy(8, x_blk, to_c)
    c_x.start()
    fwd_x.wait_recv()
    fwd_y.wait_recv()
    c_d = u_copy(9, d_blk, to_c)
    c_d.start()
    for cp in (own_c, c_y, c_x, c_d):
        cp.wait_recv()
    out_u = pltpu.make_async_copy(u_all, u_out, lsem.at[0])
    out_u.start()
    for cp in (*own_y, *own_x, own_c, fwd_x, c_y, fwd_y, c_x, c_d):
        cp.wait_send()
    for cp in outs:
        cp.wait()
    out_u.wait()


def attention(layer, x, lens, kc, vc, wq, wk, wv, wo, ids=None, n_local=0):
    tokens, d_model = x.shape
    rows, dim = kc.shape[2], kc.shape[3]
    heads = wq.shape[2] // dim
    half = tokens // 2
    hbm = pl.BlockSpec(memory_space=pltpu.HBM)
    anywhere = pl.BlockSpec(memory_space=pl.ANY)
    vmem = pl.BlockSpec(memory_space=pltpu.VMEM)
    dma = pltpu.SemaphoreType.DMA
    scratch = [
        pltpu.VMEM((SLOTS, TB, rows, dim), BF16), pltpu.VMEM((SLOTS, TB, rows, dim), BF16), pltpu.VMEM((TB, heads, rows), BF16),
        pltpu.VMEM(wq.shape[1:], BF16), pltpu.VMEM(wk.shape[1:], BF16), pltpu.VMEM(wv.shape[1:], BF16), pltpu.VMEM(wo.shape[1:], BF16),
        pltpu.VMEM((tokens, heads, dim), F32), pltpu.VMEM((tokens, heads, dim), F32), pltpu.VMEM((half, heads, dim), F32),
        pltpu.VMEM((half, heads, dim), F32), pltpu.VMEM((half, heads, dim), F32),
        pltpu.VMEM((heads, 128), F32), pltpu.VMEM((heads, 128), F32), pltpu.VMEM((half, heads * dim), BF16),
        pltpu.VMEM((8, half, d_model), BF16), pltpu.VMEM((half, d_model), BF16),
        dma((SLOTS,)), dma((SLOTS,)), dma((4,)), dma((half // TB + 1,)), dma((half // TB + 1,)), dma((10,)), dma((10,)), dma((3,)),
    ]
    out_shape = [jax.ShapeDtypeStruct((8, half, d_model), BF16)] + [jax.ShapeDtypeStruct((half, d_model // 2), BF16)] * 2
    in_specs = [vmem, pl.BlockSpec(memory_space=pltpu.SMEM)] + [hbm] * 6
    out_specs = [anywhere] * 3
    args = [x, lens, kc, vc, wq, wk, wv, wo]
    if ids is not None:
        layers = ids.shape[0]
        args.append(ids)
        in_specs.append(vmem)
        out_shape += [jax.ShapeDtypeStruct((layers, 8, 8 * half), I32)] * 2 + [jax.ShapeDtypeStruct((layers, n_local, 128), I32)]
        out_specs += [vmem] * 3
        scratch += [pltpu.VMEM((4,) + ids.shape, I32), dma((3,)), dma((3,))]
    u, a, a_send, *rest = pl.pallas_call(
        functools.partial(attn_kernel, layer, ids is not None),
        out_shape=out_shape, in_specs=in_specs, out_specs=out_specs, scratch_shapes=scratch,
        compiler_params=pltpu.CompilerParams(collective_id=layer, has_side_effects=True, vmem_limit_bytes=VMEM_MIB[layer] << 20),
        name=f"attn{layer}",
    )(*args)
    return (u.reshape(8 * half, d_model), a, a_send, *rest)


def expert_kernel(layer, part, off_ref, u_ref, pos_ref, w1_hbm, w3_hbm, w2_hbm, own_out, send_out,
                  xt, act, y_buf, w1, w3, w2, t_exp, t_at, t_new, t_lo, t_hi, live, sem, osem):
    n_tok = u_ref.shape[0]
    n_local = w1.shape[0]
    n_rows = own_out.shape[0]
    start = part * n_rows
    weights = ((w1_hbm, w1), (w3_hbm, w3), (w2_hbm, w2))

    def copies(e):
        return [pltpu.make_async_copy(src.at[layer, e], dst.at[e], sem.at[i, e]) for i, (src, dst) in enumerate(weights)]

    def plan(e, state):
        t, n = state
        end = jnp.where(e + 1 < n_local, off_ref[layer, jnp.minimum(e + 1, n_local - 1), 0], start + n_rows)
        lo = jnp.maximum(off_ref[layer, e, 0] - start, 0)
        hi = jnp.minimum(end - start, n_rows)
        base = lo // 16 * 16
        live[n] = e

        def put(i, t):
            t_exp[t] = e
            t_at[t] = base + i * TILE_M
            t_new[t] = jnp.where(i == 0, n + 1, 0)
            t_lo[t] = lo
            t_hi[t] = hi
            return t + 1

        some = lo < hi
        return lax.fori_loop(0, jnp.where(some, pl.cdiv(hi - base, TILE_M), 0), put, t), jnp.where(some, n + 1, n)

    tiles, n_live = lax.fori_loop(0, n_local, plan, (0, 0))
    t_new[tiles] = 0

    def start_nth(i):
        @pl.when(i < n_live)
        def _():
            for cp in copies(live[i]):
                cp.start()

    for i in range(DEPTH):
        start_nth(i)

    step = 128
    for r in range(n_rows // step):
        rid = lax.broadcasted_iota(I32, (step, n_tok), 0) + (r * step + start)
        hit = rid == pos_ref[0, 0:1, :]
        for k in range(1, 6):
            hit = hit | (rid == pos_ref[0, k:k + 1, :])
        rows = _nn(jnp.where(hit, 1.0, 0.0).astype(BF16), u_ref[...])
        xt[:, r * step:(r + 1) * step] = jnp.transpose(rows).astype(BF16)
    xt[:, n_rows:] = jnp.zeros((xt.shape[0], xt.shape[1] - n_rows), BF16)

    def arrive(k):
        @pl.when(t_new[k] > 0)
        def _():
            for cp in copies(t_exp[k]):
                cp.wait()
            start_nth(t_new[k] - 1 + DEPTH)

    def up(k):
        e, at = t_exp[k], t_at[k]
        cols = xt[:, pl.ds(pl.multiple_of(at // 128 * 128, 128), 2 * TILE_M)]
        h1 = _nn(w1[e], cols)
        h3 = _nn(w3[e], cols)
        return jnp.transpose(h1 * jax.nn.sigmoid(h1) * h3).astype(BF16)

    def down(k):
        at = pl.multiple_of(t_at[k], 16)
        y = _nn(act[k % 2, pl.ds(pl.multiple_of(t_at[k] % 128, 16), TILE_M), :], w2[t_exp[k]])
        rid = lax.broadcasted_iota(I32, y.shape, 0) + at
        mask = (rid >= t_lo[k]) & (rid < t_hi[k])
        y_buf[pl.ds(at, TILE_M), :] = jnp.where(mask, y, y_buf[pl.ds(at, TILE_M), :])

    arrive(0)
    arrive(1)
    act[0] = up(0)

    def both(k, none):
        arrive(k + 1)
        act[k % 2] = up(k)
        down(k - 1)
        return none

    lax.fori_loop(1, tiles, both, 0)
    down(tiles - 1)
    p = lax.axis_index("pool")
    cw = own_out.shape[1]
    outs = [pltpu.make_async_copy(y_buf.at[pl.ds(0, n_rows), pl.ds(pl.multiple_of(q * cw, 128), cw)], dst, osem.at[i])
            for i, (q, dst) in enumerate(((1 - p, send_out), (p, own_out)))]
    for cp in outs:
        cp.start()
    for cp in outs:
        cp.wait()


def experts(layer, part, off, u, pos_t, w1, w3, w2, n_rows):
    n_local, width, d_model = w1.shape[1:]
    hbm = pl.BlockSpec(memory_space=pl.ANY)
    vmem = pl.BlockSpec(memory_space=pltpu.VMEM)
    weights = pltpu.VMEM((n_local, width, d_model), BF16)
    table = pltpu.SMEM((64,), I32)
    return pl.pallas_call(
        functools.partial(expert_kernel, layer, part),
        grid=(1,),
        out_shape=[jax.ShapeDtypeStruct((n_rows, d_model // 2), F32)] * 2,
        in_specs=[pl.BlockSpec(memory_space=pltpu.SMEM), vmem, pl.BlockSpec((1,) + pos_t.shape[1:], lambda i: (layer, 0, 0)), hbm, hbm, hbm],
        out_specs=[hbm, hbm],
        scratch_shapes=[pltpu.VMEM((d_model, n_rows + 2 * TILE_M), BF16), pltpu.VMEM((2, 2 * TILE_M, width), BF16),
                        pltpu.VMEM((n_rows + TILE_M, d_model), F32), weights, weights, weights,
                        table, table, table, table, table, table, pltpu.SemaphoreType.DMA((3, n_local)), pltpu.SemaphoreType.DMA((2,))],
        compiler_params=pltpu.CompilerParams(vmem_limit_bytes=45 << 20),
        cost_estimate=pl.CostEstimate(flops=int(1.2e10), bytes_accessed=18 << 20, transcendentals=0),
        name=f"experts{layer}{part}",
    )(off, u, pos_t, w1, w3, w2)


N_CH = 4


def combine_kernel(own1_ref, got1_ref, own2_ref, send2_ref, u_ref, wr_ref, ids_ref, pos_ref, a_ref, a_got_ref, x_out,
                   yr, gm, tb, tcr, txs, txr, xo, a_buf, ysend, yrecv, csend, crecv, xsend, xrecv, fsend, frecv, lsem):
    p, b, x, c, to_y, to_x, to_c = _where_am_i()
    half_rows, cw = yr.shape[1], yr.shape[2]
    n_rows = 2 * half_rows
    n_tok, top_k = u_ref.shape[0], 6
    tokens = 2 * a_ref.shape[0]
    mine = p * N_CH
    _greet((to_y, to_x, to_c))

    def cols(i):
        return pl.ds(pl.multiple_of(i * cw, 128), cw)

    y_copies = [_rcopy(send2_ref.at[:, j * cw:(j + 1) * cw], yr.at[j], ysend.at[j], yrecv.at[j], to_y) for j in range(N_CH)]
    for cp in y_copies:
        cp.start()

    half = a_ref.shape[0]
    a_buf[pl.ds(pl.multiple_of(p * half, half), half), :] = a_ref[...]
    a_buf[pl.ds(pl.multiple_of((1 - p) * half, half), half), :] = a_got_ref[...]
    step = 128
    n_exp = wr_ref.shape[1]
    wr = wr_ref[0]
    wr1 = wr.astype(BF16)
    wr2 = (wr - wr1.astype(F32)).astype(BF16)
    wr3 = (wr - wr1.astype(F32) - wr2.astype(F32)).astype(BF16)

    def gates(i, carry):
        at = pl.ds(pl.multiple_of(i * step, step), step)
        rows = u_ref[at, :]
        logits = _nt(rows, wr1) + (_nt(rows, wr2) + _nt(rows, wr3))
        lane = lax.broadcasted_iota(I32, (step, n_exp), 1)
        ids = jnp.transpose(ids_ref[0, :, at].astype(F32)).astype(I32)
        pos = jnp.transpose(pos_ref[0, :, at].astype(F32)).astype(I32)
        g = [jnp.sum(jnp.where(lane == ids[:, k:k + 1], logits, 0.0), axis=1, keepdims=True) for k in range(top_k)]
        top = functools.reduce(jnp.maximum, g)
        g = [jnp.exp(v - top) for v in g]
        den = functools.reduce(jnp.add, g)
        g = [v / den for v in g]
        rid = lax.broadcasted_iota(I32, (step, n_rows), 1)
        mat = jnp.zeros((step, n_rows), F32)
        for k in range(top_k):
            mat = jnp.where(rid == pos[:, k:k + 1], g[k], mat)
        g1 = mat.astype(BF16)
        rest = mat - g1.astype(F32)
        g2 = rest.astype(BF16)
        gm[0, at, :] = g1
        gm[1, at, :] = g2
        gm[2, at, :] = (rest - g2.astype(F32)).astype(BF16)
        return carry

    lax.fori_loop(0, n_tok // step, gates, 0)

    def gated(ys, rows):
        return _nn(gm[0, :, rows], ys) + (_nn(gm[1, :, rows], ys) + _nn(gm[2, :, rows], ys))

    for j in range(N_CH):
        ys = (own1_ref[:, j * cw:(j + 1) * cw] + got1_ref[:, j * cw:(j + 1) * cw]).astype(BF16)
        tb[j] = gated(ys, pl.ds(0, half_rows)).reshape(n_tok // tokens, tokens, cw)

    f_copies = []

    def finish(j, c_copies, x_copy):
        x_copy.wait_recv()
        own = tb[j, x * 2 + c] + tcr[j, x]
        new = (a_buf[:, j * cw:(j + 1) * cw].astype(F32) + (own + txr[j])).astype(BF16)
        xo[:, cols(mine + j)] = new
        f_copy = _rcopy(xo.at[:, cols(mine + j)], xo.at[:, cols(mine + j)], fsend.at[j], frecv.at[j], to_y)
        f_copy.start()
        f_copies.append((c_copies, x_copy, f_copy))

    last = None
    for j in range(N_CH):
        y_copies[j].wait_recv()
        ys = (own2_ref[:, j * cw:(j + 1) * cw] + yr[j]).astype(BF16)
        tb[j] = tb[j] + gated(ys, pl.ds(half_rows, half_rows)).reshape(n_tok // tokens, tokens, cw)
        c_copies = [_rcopy(tb.at[j, i * 2 + (1 - c)], tcr.at[j, i], csend.at[j, i], crecv.at[j, i], to_c) for i in range(2)]
        for cp in c_copies:
            cp.start()
        if last is not None:
            finish(*last)
        for cp in c_copies:
            cp.wait_recv()
        txs[j] = tb[j, (1 - x) * 2 + c] + tcr[j, 1 - x]
        x_copy = _rcopy(txs.at[j], txr.at[j], xsend.at[j], xrecv.at[j], to_x)
        x_copy.start()
        last = (j, c_copies, x_copy)
    finish(*last)
    for _, _, f_copy in f_copies:
        f_copy.wait_recv()
    out = pltpu.make_async_copy(xo, x_out, lsem)
    out.start()
    for cp in y_copies:
        cp.wait_send()
    for c_copies, x_copy, f_copy in f_copies:
        for cp in c_copies:
            cp.wait_send()
        x_copy.wait_send()
        f_copy.wait_send()
    out.wait()


def combine(layer, own1, got1, own2, send2, u, wr, ids, pos, a, a_got):
    half_rows = own1.shape[0]
    n_rows = 2 * half_rows
    half, half_cols = a.shape
    tokens = 2 * half
    n_tok, d_model = u.shape
    cw = half_cols // N_CH
    vmem = pl.BlockSpec(memory_space=pltpu.VMEM)
    blocks = n_tok // tokens
    sliced = lambda arr: pl.BlockSpec((1,) + arr.shape[1:], lambda i: (layer, 0, 0))
    dma = pltpu.SemaphoreType.DMA
    return pl.pallas_call(
        combine_kernel,
        grid=(1,),
        out_shape=jax.ShapeDtypeStruct((tokens, d_model), BF16),
        in_specs=[vmem] * 5 + [sliced(wr), sliced(ids), sliced(pos), vmem, vmem],
        out_specs=pl.BlockSpec(memory_space=pl.ANY),
        scratch_shapes=[
            pltpu.VMEM((N_CH, half_rows, cw), F32), pltpu.VMEM((3, n_tok, n_rows), BF16), pltpu.VMEM((N_CH, blocks, tokens, cw), F32),
            pltpu.VMEM((N_CH, 2, tokens, cw), F32), pltpu.VMEM((N_CH, tokens, cw), F32), pltpu.VMEM((N_CH, tokens, cw), F32),
            pltpu.VMEM((tokens, d_model), BF16), pltpu.VMEM((tokens, half_cols), BF16),
            dma((N_CH,)), dma((N_CH,)), dma((N_CH, 2)), dma((N_CH, 2)), dma((N_CH,)), dma((N_CH,)), dma((N_CH,)), dma((N_CH,)), dma,
        ],
        compiler_params=pltpu.CompilerParams(collective_id=2 + layer, has_side_effects=True, vmem_limit_bytes=32 << 20),
        name=f"combine{layer}",
    )(own1, got1, own2, send2, u, wr, ids, pos, a, a_got)


def solution(mesh):
    tok_spec = P(("dp", "ep"), None)
    cache_spec = P(None, ("dp", "ep"), "pool", None, None)
    up_spec = P(None, "ep", None, "pool")
    down_spec = P(None, "ep", "pool", None)
    in_specs = (tok_spec, cache_spec, cache_spec, P(("dp", "ep")), P(), P(), P(), P(), P(), P(None, ("dp", "ep"), None), up_spec, up_spec, down_spec)

    def body(hidden, kc, vc, lens, wq, wk, wv, wo, wr, ids, w1, w3, w2):
        layers, tokens, seq, heads, dim = kc.shape
        n_local = w1.shape[1]
        top_k = ids.shape[2]
        kc = kc.reshape(layers, tokens, seq * heads, dim)
        vc = vc.reshape(layers, tokens, seq * heads, dim)
        w1 = jnp.swapaxes(w1, 2, 3)
        w3 = jnp.swapaxes(w3, 2, 3)
        wr = jnp.swapaxes(wr, 1, 2)
        n_rows = tokens * top_k
        ids = jnp.pad(jnp.swapaxes(ids, 1, 2), ((0, 0), (0, 8 - top_k), (0, 0)))
        for layer in range(layers):
            first = layer == 0
            u, a, a_send, *tables = attention(layer, hidden, lens, kc, vc, wq, wk, wv, wo, ids if first else None, n_local)
            if first:
                pos, ids_all, off = tables
            swap = [(0, 1), (1, 0)]
            a_got = lax.ppermute(a_send, "pool", swap)
            own1, send1 = experts(layer, 0, off, u, pos, w1, w3, w2, n_rows // 2)
            got1 = lax.ppermute(send1, "pool", swap)
            own2, send2 = experts(layer, 1, off, u, pos, w1, w3, w2, n_rows // 2)
            hidden = combine(layer, own1, got1, own2, send2, u, wr, ids_all, pos, a, a_got)
        return hidden

    return jax.shard_map(body, mesh=mesh, in_specs=in_specs, out_specs=tok_spec, check_vma=False)
```

```python
import functools

import jax
import jax.numpy as jnp
from jax import lax
from jax.experimental import pallas as pl
from jax.experimental.pallas import tpu as pltpu
from jax.sharding import PartitionSpec as P

MESH = pl.DeviceIdType.MESH
F32 = jnp.float32
BF16 = jnp.bfloat16
I32 = jnp.int32
EPS = 1e-6
NEG = -1e30
TB = 8
SLOTS = 4
TILE_M = 128
DEPTH = 4
VMEM_MIB = (51, 51)


def _nn(a, b):
    return lax.dot_general(a, b, (((1,), (0,)), ((), ())), preferred_element_type=F32)


def _nt(a, b, precision=None):
    return lax.dot_general(a, b, (((1,), (1,)), ((), ())), preferred_element_type=F32, precision=precision)


def _rms(v):
    return v * lax.rsqrt(jnp.mean(v * v, axis=-1, keepdims=True) + EPS)


def _where_am_i():
    p = lax.axis_index("pool")
    b = lax.axis_index("ep")
    x, c = b // 2, b % 2
    to_y = {"pool": 1 - p}
    to_x = {"ep": (1 - x) * 2 + c}
    to_c = {"ep": x * 2 + (1 - c)}
    return p, b, x, c, to_y, to_x, to_c


def _greet(peers):
    sem = pltpu.get_barrier_semaphore()
    for peer in peers:
        pl.semaphore_signal(sem, inc=1, device_id=peer, device_id_type=MESH)
    pl.semaphore_wait(sem, len(peers))


def _rcopy(src, dst, send, recv, peer):
    return pltpu.make_async_remote_copy(src_ref=src, dst_ref=dst, send_sem=send, recv_sem=recv, device_id=peer, device_id_type=MESH)


def _route(b, idg, pos_out, ids_out, off_out):
    n_local, top_k = off_out.shape[1], 6
    n_tok = pos_out.shape[2]
    er = lax.broadcasted_iota(I32, (n_local, n_tok), 0)
    tri = (lax.broadcasted_iota(I32, (n_tok, n_tok), 0) <= lax.broadcasted_iota(I32, (n_tok, n_tok), 1)).astype(F32).astype(BF16)
    before = (lax.broadcasted_iota(I32, (n_local, n_local), 0) > lax.broadcasted_iota(I32, (n_local, n_local), 1)).astype(F32).astype(BF16)
    row = lax.broadcasted_iota(I32, (8, n_tok), 0)
    for layer in range(pos_out.shape[0]):
        ids = jnp.concatenate([idg[i, layer] for i in range(idg.shape[0])], axis=1)
        local = ids - b * n_local
        member = jnp.zeros((n_local, n_tok), F32)
        for k in range(top_k):
            member = member + jnp.where(er == local[k:k + 1, :], 1.0, 0.0)
        member = member.astype(BF16)
        cum = _nn(member, tri)
        first = jnp.sum(_nn(before, member), axis=1, keepdims=True)
        place = first + cum - 1.0
        pos = jnp.full((8, n_tok), -1.0, F32)
        for k in range(top_k):
            lk = local[k:k + 1, :]
            at = jnp.sum(jnp.where(er == lk, place, 0.0), axis=0, keepdims=True)
            at = jnp.where((lk >= 0) & (lk < n_local), at, -1.0)
            pos = jnp.where(row == k, at, pos)
        pos_out[layer] = pos.astype(I32)
        ids_out[layer] = ids
        off_out[layer] = jnp.broadcast_to(first, (n_local, 128)).astype(I32)


def attn_kernel(layer, routed, x_ref, len_ref, k_hbm, v_hbm, wq_hbm, wk_hbm, wv_hbm, wo_hbm, *refs):
    if routed:
        ids_ref, *refs = refs
    u_out, a_out, a_got, *refs = refs
    if routed:
        pos_out, ids_out, off_out, *refs, idg, isend, irecv = refs
    (kbuf, vbuf, pbuf, wq, wk, wv, wo, q3, o3, o3r, k3, v3, mls, mlr, o2, u_all, a_own, a_recv,
     ksem, vsem, wsem, osend, orecv, gsend, grecv, lsem) = refs
    p, b, x, c, to_y, to_x, to_c = _where_am_i()
    half = x_ref.shape[0] // 2
    heads, dim = q3.shape[1], q3.shape[2]
    cols = heads * dim
    rows = kbuf.shape[2]
    n_half = half // TB
    n_blocks = 2 * n_half
    scale = dim ** -0.5

    def tok_of(n):
        return ((1 - p) + (n // n_half) * (2 * p - 1)) * half + (n % n_half) * TB

    def kv_copies(n):
        slot = n % SLOTS
        src = pl.ds(tok_of(n), TB)
        return (pltpu.make_async_copy(k_hbm.at[layer, src], kbuf.at[slot], ksem.at[slot]),
                pltpu.make_async_copy(v_hbm.at[layer, src], vbuf.at[slot], vsem.at[slot]))

    w_copies = [pltpu.make_async_copy(src.at[layer], dst, wsem.at[i])
                for i, (src, dst) in enumerate(((wq_hbm, wq), (wk_hbm, wk), (wv_hbm, wv), (wo_hbm, wo)))]
    w_copies[0].start()
    for n in range(SLOTS):
        for cp in kv_copies(n):
            cp.start()
    for cp in w_copies[1:]:
        cp.start()

    if routed:
        to_d = {"ep": (1 - x) * 2 + (1 - c)}
        _greet((to_y, to_x, to_c, to_d))
        idg[b] = ids_ref[...]
        id_copies = [_rcopy(ids_ref, idg.at[b], isend.at[i], irecv.at[i], peer) for i, peer in enumerate((to_x, to_c, to_d))]
        for cp in id_copies:
            cp.start()
    else:
        _greet((to_y, to_x, to_c))

    normed = _rms(x_ref[...].astype(F32)).astype(BF16)
    w_copies[0].wait()
    for h in range(0, heads, 2):
        part = _nn(normed, wq[:, h * dim:(h + 2) * dim]).astype(BF16).astype(F32)
        q3[:, h, :] = part[:, :dim]
        q3[:, h + 1, :] = part[:, dim:]

    row_i = lax.broadcasted_iota(I32, (heads, rows), 0)
    lane_i = lax.broadcasted_iota(I32, (heads, rows), 1)
    posl = jnp.where(lane_i % heads == row_i, lane_i // heads + p * (rows // heads), 1 << 20)
    lane = lax.broadcasted_iota(I32, (heads, 128), 1)

    def block(n, acc):
        slot = n % SLOTS
        for cp in kv_copies(n):
            cp.wait()
        t0 = tok_of(n)

        def scores(_, acc):
            for j in range(TB):
                q = q3[t0 + j].astype(BF16)
                s = _nt(q, kbuf[slot, j])
                s = jnp.where(posl < len_ref[t0 + j], s * scale, NEG)
                m = jnp.max(s, axis=1, keepdims=True)
                pr = jnp.exp(s - m)
                l = jnp.sum(pr, axis=1, keepdims=True)
                pbuf[j] = pr.astype(BF16)
                at = (n % n_half) * TB + j
                acc = jnp.where(lane == at, m, acc)
                acc = jnp.where(lane == half + at, l, acc)
            return acc

        def values(_, none):
            for j in range(TB):
                o3[t0 + j] = _nn(pbuf[j], vbuf[slot, j])
            return none

        acc = lax.fori_loop(0, 1, scores, acc)
        lax.fori_loop(0, 1, values, 0)

        @pl.when(n + SLOTS < n_blocks)
        def _():
            for cp in kv_copies(n + SLOTS):
                cp.start()

        return acc

    theirs = (1 - p) * half
    mine = p * half

    def o_copy(i):
        return _rcopy(o3.at[pl.ds(theirs + i * TB, TB)], o3r.at[pl.ds(i * TB, TB)], osend.at[i], orecv.at[i], to_y)

    def first(n, acc):
        acc = block(n, acc)
        o_copy(n).start()
        return acc

    zero = jnp.zeros((heads, 128), F32)
    mls[...] = lax.fori_loop(0, n_half, first, zero)
    ml_copy = _rcopy(mls, mlr, osend.at[n_half], orecv.at[n_half], to_y)
    ml_copy.start()
    normed = _rms(x_ref[pl.ds(mine, half), :].astype(F32)).astype(BF16)
    for i, (w, dst) in enumerate(((wk, k3), (wv, v3))):
        w_copies[1 + i].wait()
        for h in range(0, heads, 2):
            part = _nn(normed, w[:, h * dim:(h + 2) * dim]).astype(BF16).astype(F32)
            dst[:, h, :] = part[:, :dim]
            dst[:, h + 1, :] = part[:, dim:]

    sn = zero
    for j in range(half):
        sn = jnp.where(lane == j, jnp.sum(q3[mine + j] * k3[j], axis=1, keepdims=True) * scale, sn)

    if routed:
        for cp in id_copies:
            cp.wait()
        _route(b, idg, pos_out, ids_out, off_out)

    ml_own = lax.fori_loop(n_half, n_blocks, block, zero)

    for i in range(n_half):
        o_copy(i).wait()
    ml_copy.wait()
    ml_their = mlr[...]
    top = jnp.maximum(jnp.maximum(ml_own, ml_their), sn)
    w_own, w_their, w_new = jnp.exp(ml_own - top), jnp.exp(ml_their - top), jnp.exp(sn - top)
    den = pltpu.roll(ml_own, half, 1) * w_own + pltpu.roll(ml_their, half, 1) * w_their + w_new
    w_own, w_their, w_new = w_own / den, w_their / den, w_new / den
    for j in range(half):
        o3r[j] = (o3[mine + j] * w_own[:, j:j + 1] + o3r[j] * w_their[:, j:j + 1] + v3[j] * w_new[:, j:j + 1])
    for h in range(heads):
        o2[:, h * dim:(h + 1) * dim] = o3r[:, h, :].astype(BF16)
    w_copies[3].wait()
    d_model = x_ref.shape[1]
    a = (x_ref[pl.ds(mine, half), :].astype(F32) + _nn(o2[...], wo[...])).astype(BF16)
    a_own[...] = a
    me = b * 2 + p
    u_all[me] = _rms(a.astype(F32)).astype(BF16)

    y_blk, x_blk = b * 2 + (1 - p), ((1 - x) * 2 + c) * 2 + p
    d_blk = ((1 - x) * 2 + c) * 2 + (1 - p)
    lo, hi = pl.ds(0, half // 2), pl.ds(half // 2, half // 2)

    def u_copy(i, src, peer, part=None):
        ref = u_all.at[src] if part is None else u_all.at[src, part]
        return _rcopy(ref, ref, gsend.at[i], grecv.at[i], peer)

    own_y = [u_copy(0, me, to_y, lo), u_copy(1, me, to_y, hi)]
    own_x = [u_copy(2, me, to_x, hi), u_copy(3, me, to_x, lo)]
    own_c = u_copy(4, me, to_c)
    for cp in (own_y[0], own_x[0], own_y[1], own_x[1], own_c):
        cp.start()
    cw = d_model // 2
    mine_a, theirs_a = (a_own.at[:, pl.ds(pl.multiple_of(q * cw, 128), cw)] for q in (p, 1 - p))
    a_copy = _rcopy(theirs_a, a_recv, gsend.at[10], grecv.at[10], to_y)
    out_a = pltpu.make_async_copy(mine_a, a_out, lsem.at[1])
    out_a.start()
    own_y[0].wait_recv()
    fwd_x = u_copy(5, y_blk, to_x, lo)
    fwd_x.start()
    own_x[0].wait_recv()
    fwd_y = u_copy(6, x_blk, to_y, hi)
    fwd_y.start()
    a_copy.start()
    own_y[1].wait_recv()
    c_y = u_copy(7, y_blk, to_c)
    c_y.start()
    own_x[1].wait_recv()
    c_x = u_copy(8, x_blk, to_c)
    c_x.start()
    fwd_x.wait_recv()
    fwd_y.wait_recv()
    c_d = u_copy(9, d_blk, to_c)
    c_d.start()
    for cp in (own_c, c_y, c_x, c_d):
        cp.wait_recv()
    out_u = pltpu.make_async_copy(u_all, u_out, lsem.at[0])
    out_u.start()
    a_copy.wait_recv()
    out_g = pltpu.make_async_copy(a_recv, a_got, lsem.at[2])
    out_g.start()
    for cp in (*own_y, *own_x, own_c, fwd_x, c_y, fwd_y, c_x, c_d, a_copy):
        cp.wait_send()
    out_a.wait()
    out_u.wait()
    out_g.wait()


def attention(layer, x, lens, kc, vc, wq, wk, wv, wo, ids=None, n_local=0):
    tokens, d_model = x.shape
    rows, dim = kc.shape[2], kc.shape[3]
    heads = wq.shape[2] // dim
    half = tokens // 2
    hbm = pl.BlockSpec(memory_space=pltpu.HBM)
    anywhere = pl.BlockSpec(memory_space=pl.ANY)
    vmem = pl.BlockSpec(memory_space=pltpu.VMEM)
    dma = pltpu.SemaphoreType.DMA
    scratch = [
        pltpu.VMEM((SLOTS, TB, rows, dim), BF16), pltpu.VMEM((SLOTS, TB, rows, dim), BF16), pltpu.VMEM((TB, heads, rows), BF16),
        pltpu.VMEM(wq.shape[1:], BF16), pltpu.VMEM(wk.shape[1:], BF16), pltpu.VMEM(wv.shape[1:], BF16), pltpu.VMEM(wo.shape[1:], BF16),
        pltpu.VMEM((tokens, heads, dim), F32), pltpu.VMEM((tokens, heads, dim), F32), pltpu.VMEM((half, heads, dim), F32),
        pltpu.VMEM((half, heads, dim), F32), pltpu.VMEM((half, heads, dim), F32),
        pltpu.VMEM((heads, 128), F32), pltpu.VMEM((heads, 128), F32), pltpu.VMEM((half, heads * dim), BF16),
        pltpu.VMEM((8, half, d_model), BF16), pltpu.VMEM((half, d_model), BF16), pltpu.VMEM((half, d_model // 2), BF16),
        dma((SLOTS,)), dma((SLOTS,)), dma((4,)), dma((half // TB + 1,)), dma((half // TB + 1,)), dma((11,)), dma((11,)), dma((3,)),
    ]
    out_shape = [jax.ShapeDtypeStruct((8, half, d_model), BF16)] + [jax.ShapeDtypeStruct((half, d_model // 2), BF16)] * 2
    in_specs = [vmem, pl.BlockSpec(memory_space=pltpu.SMEM)] + [hbm] * 6
    out_specs = [anywhere] * 3
    args = [x, lens, kc, vc, wq, wk, wv, wo]
    if ids is not None:
        layers = ids.shape[0]
        args.append(ids)
        in_specs.append(vmem)
        out_shape += [jax.ShapeDtypeStruct((layers, 8, 8 * half), I32)] * 2 + [jax.ShapeDtypeStruct((layers, n_local, 128), I32)]
        out_specs += [vmem] * 3
        scratch += [pltpu.VMEM((4,) + ids.shape, I32), dma((3,)), dma((3,))]
    u, a, a_got, *rest = pl.pallas_call(
        functools.partial(attn_kernel, layer, ids is not None),
        out_shape=out_shape, in_specs=in_specs, out_specs=out_specs, scratch_shapes=scratch,
        compiler_params=pltpu.CompilerParams(collective_id=layer, has_side_effects=True, vmem_limit_bytes=VMEM_MIB[layer] << 20),
        name=f"attn{layer}",
    )(*args)
    return (u.reshape(8 * half, d_model), a, a_got, *rest)


def expert_kernel(layer, part, off_ref, u_ref, pos_ref, w1_hbm, w3_hbm, w2_hbm, own_ref, send_ref,
                  xt, act, w1, w3, w2, t_exp, t_at, t_new, t_lo, t_hi, live, sem):
    n_tok = u_ref.shape[0]
    n_local = w1.shape[0]
    n_rows, cw = own_ref.shape
    p = lax.axis_index("pool")
    start = part * n_rows
    weights = ((w1_hbm, w1), (w3_hbm, w3), (w2_hbm, w2))

    def copies(e):
        return [pltpu.make_async_copy(src.at[layer, e], dst.at[e], sem.at[i, e]) for i, (src, dst) in enumerate(weights)]

    def plan(e, state):
        t, n = state
        end = jnp.where(e + 1 < n_local, off_ref[layer, jnp.minimum(e + 1, n_local - 1), 0], start + n_rows)
        lo = jnp.maximum(off_ref[layer, e, 0] - start, 0)
        hi = jnp.minimum(end - start, n_rows)
        base = lo // 16 * 16
        live[n] = e

        def put(i, t):
            t_exp[t] = e
            t_at[t] = jnp.minimum(base + i * TILE_M, n_rows - TILE_M)
            t_new[t] = jnp.where(i == 0, n + 1, 0)
            t_lo[t] = lo
            t_hi[t] = hi
            return t + 1

        some = lo < hi
        return lax.fori_loop(0, jnp.where(some, pl.cdiv(hi - base, TILE_M), 0), put, t), jnp.where(some, n + 1, n)

    tiles, n_live = lax.fori_loop(0, n_local, plan, (0, 0))
    t_new[tiles] = 0

    def start_nth(i):
        @pl.when(i < n_live)
        def _():
            for cp in copies(live[i]):
                cp.start()

    for i in range(DEPTH):
        start_nth(i)

    step = 128
    for r in range(n_rows // step):
        rid = lax.broadcasted_iota(I32, (step, n_tok), 0) + (r * step + start)
        hit = rid == pos_ref[layer, 0:1, :]
        for k in range(1, 6):
            hit = hit | (rid == pos_ref[layer, k:k + 1, :])
        rows = _nn(jnp.where(hit, 1.0, 0.0).astype(BF16), u_ref[...])
        xt[:, r * step:(r + 1) * step] = jnp.transpose(rows).astype(BF16)
    xt[:, n_rows:] = jnp.zeros((xt.shape[0], xt.shape[1] - n_rows), BF16)

    def arrive(k):
        @pl.when(t_new[k] > 0)
        def _():
            for cp in copies(t_exp[k]):
                cp.wait()
            start_nth(t_new[k] - 1 + DEPTH)

    def up(k):
        e, at = t_exp[k], t_at[k]
        cols = xt[:, pl.ds(pl.multiple_of(at // 128 * 128, 128), 2 * TILE_M)]
        h1 = _nn(w1[e], cols)
        h3 = _nn(w3[e], cols)
        return jnp.transpose(h1 * jax.nn.sigmoid(h1) * h3).astype(BF16)

    def down(k):
        at = pl.multiple_of(t_at[k], 16)
        rows = act[k % 2, pl.ds(pl.multiple_of(t_at[k] % 128, 16), TILE_M), :]
        rid = lax.broadcasted_iota(I32, (TILE_M, cw), 0) + at
        mask = (rid >= t_lo[k]) & (rid < t_hi[k])
        for ref, q in ((own_ref, p), (send_ref, 1 - p)):
            y = _nn(rows, w2[t_exp[k], :, pl.ds(pl.multiple_of(q * cw, 128), cw)])
            ref[pl.ds(at, TILE_M), :] = jnp.where(mask, y, ref[pl.ds(at, TILE_M), :])

    arrive(0)
    arrive(1)
    act[0] = up(0)

    def both(k, none):
        arrive(k + 1)
        act[k % 2] = up(k)
        down(k - 1)
        return none

    lax.fori_loop(1, tiles, both, 0)
    down(tiles - 1)


def experts(layer, part, off, u, pos_t, w1, w3, w2, n_rows):
    n_local, width, d_model = w1.shape[1:]
    hbm = pl.BlockSpec(memory_space=pl.ANY)
    vmem = pl.BlockSpec(memory_space=pltpu.VMEM)
    weights = pltpu.VMEM((n_local, width, d_model), BF16)
    table = pltpu.SMEM((64,), I32)
    return pl.pallas_call(
        functools.partial(expert_kernel, layer, part),
        out_shape=[jax.ShapeDtypeStruct((n_rows, d_model // 2), F32)] * 2,
        in_specs=[pl.BlockSpec(memory_space=pltpu.SMEM), vmem, vmem, hbm, hbm, hbm],
        out_specs=[vmem, vmem],
        scratch_shapes=[pltpu.VMEM((d_model, n_rows + 2 * TILE_M), BF16), pltpu.VMEM((2, 2 * TILE_M, width), BF16),
                        weights, weights, weights,
                        table, table, table, table, table, table, pltpu.SemaphoreType.DMA((3, n_local))],
        compiler_params=pltpu.CompilerParams(vmem_limit_bytes=45 << 20),
        cost_estimate=pl.CostEstimate(flops=int(1.2e10), bytes_accessed=18 << 20, transcendentals=0),
        name=f"experts{layer}{part}",
    )(off, u, pos_t, w1, w3, w2)


N_CH = 4


def combine_kernel(layer, own1_ref, got1_ref, own2_ref, send2_ref, u_ref, wr_ref, ids_ref, pos_ref, a_ref, a_got_ref, x_out,
                   yr, gm, tb, tcr, txs, txr, xo, a_buf, ysend, yrecv, csend, crecv, xsend, xrecv, fsend, frecv, lsem):
    p, b, x, c, to_y, to_x, to_c = _where_am_i()
    half_rows, cw = yr.shape[1], yr.shape[2]
    n_rows = 2 * half_rows
    n_tok, top_k = u_ref.shape[0], 6
    tokens = 2 * a_ref.shape[0]
    mine = p * N_CH
    _greet((to_y, to_x, to_c))

    def cols(i):
        return pl.ds(pl.multiple_of(i * cw, 128), cw)

    y_copies = [_rcopy(send2_ref.at[:, j * cw:(j + 1) * cw], yr.at[j], ysend.at[j], yrecv.at[j], to_y) for j in range(N_CH)]
    for cp in y_copies:
        cp.start()

    half = a_ref.shape[0]
    a_buf[pl.ds(pl.multiple_of(p * half, half), half), :] = a_ref[...]
    a_buf[pl.ds(pl.multiple_of((1 - p) * half, half), half), :] = a_got_ref[...]
    step = 128
    n_exp = wr_ref.shape[1]
    wr = wr_ref[layer]
    wr1 = wr.astype(BF16)
    wr2 = (wr - wr1.astype(F32)).astype(BF16)
    wr3 = (wr - wr1.astype(F32) - wr2.astype(F32)).astype(BF16)

    def gates(i, carry):
        at = pl.ds(pl.multiple_of(i * step, step), step)
        rows = u_ref[at, :]
        logits = _nt(rows, wr1) + (_nt(rows, wr2) + _nt(rows, wr3))
        lane = lax.broadcasted_iota(I32, (step, n_exp), 1)
        ids = jnp.transpose(ids_ref[layer, :, at].astype(F32)).astype(I32)
        pos = jnp.transpose(pos_ref[layer, :, at].astype(F32)).astype(I32)
        g = [jnp.sum(jnp.where(lane == ids[:, k:k + 1], logits, 0.0), axis=1, keepdims=True) for k in range(top_k)]
        top = functools.reduce(jnp.maximum, g)
        g = [jnp.exp(v - top) for v in g]
        den = functools.reduce(jnp.add, g)
        g = [v / den for v in g]
        rid = lax.broadcasted_iota(I32, (step, n_rows), 1)
        mat = jnp.zeros((step, n_rows), F32)
        for k in range(top_k):
            mat = jnp.where(rid == pos[:, k:k + 1], g[k], mat)
        g1 = mat.astype(BF16)
        rest = mat - g1.astype(F32)
        g2 = rest.astype(BF16)
        gm[0, at, :] = g1
        gm[1, at, :] = g2
        gm[2, at, :] = (rest - g2.astype(F32)).astype(BF16)
        return carry

    lax.fori_loop(0, n_tok // step, gates, 0)

    def gated(ys, rows):
        return _nn(gm[0, :, rows], ys) + (_nn(gm[1, :, rows], ys) + _nn(gm[2, :, rows], ys))

    for j in range(N_CH):
        ys = (own1_ref[:, j * cw:(j + 1) * cw] + got1_ref[:, j * cw:(j + 1) * cw]).astype(BF16)
        tb[j] = gated(ys, pl.ds(0, half_rows)).reshape(n_tok // tokens, tokens, cw)

    f_copies = []

    def finish(j, c_copies, x_copy):
        x_copy.wait_recv()
        own = tb[j, x * 2 + c] + tcr[j, x]
        new = (a_buf[:, j * cw:(j + 1) * cw].astype(F32) + (own + txr[j])).astype(BF16)
        xo[:, cols(mine + j)] = new
        f_copy = _rcopy(xo.at[:, cols(mine + j)], xo.at[:, cols(mine + j)], fsend.at[j], frecv.at[j], to_y)
        f_copy.start()
        f_copies.append((c_copies, x_copy, f_copy))

    last = None
    for j in range(N_CH):
        y_copies[j].wait_recv()
        ys = (own2_ref[:, j * cw:(j + 1) * cw] + yr[j]).astype(BF16)
        tb[j] = tb[j] + gated(ys, pl.ds(half_rows, half_rows)).reshape(n_tok // tokens, tokens, cw)
        c_copies = [_rcopy(tb.at[j, i * 2 + (1 - c)], tcr.at[j, i], csend.at[j, i], crecv.at[j, i], to_c) for i in range(2)]
        for cp in c_copies:
            cp.start()
        if last is not None:
            finish(*last)
        for cp in c_copies:
            cp.wait_recv()
        txs[j] = tb[j, (1 - x) * 2 + c] + tcr[j, 1 - x]
        x_copy = _rcopy(txs.at[j], txr.at[j], xsend.at[j], xrecv.at[j], to_x)
        x_copy.start()
        last = (j, c_copies, x_copy)
    finish(*last)
    for _, _, f_copy in f_copies:
        f_copy.wait_recv()
    out = pltpu.make_async_copy(xo, x_out, lsem)
    out.start()
    for cp in y_copies:
        cp.wait_send()
    for c_copies, x_copy, f_copy in f_copies:
        for cp in c_copies:
            cp.wait_send()
        x_copy.wait_send()
        f_copy.wait_send()
    out.wait()


def combine(layer, own1, got1, own2, send2, u, wr, ids, pos, a, a_got):
    half_rows = own1.shape[0]
    n_rows = 2 * half_rows
    half, half_cols = a.shape
    tokens = 2 * half
    n_tok, d_model = u.shape
    cw = half_cols // N_CH
    vmem = pl.BlockSpec(memory_space=pltpu.VMEM)
    blocks = n_tok // tokens
    dma = pltpu.SemaphoreType.DMA
    return pl.pallas_call(
        functools.partial(combine_kernel, layer),
        out_shape=jax.ShapeDtypeStruct((tokens, d_model), BF16),
        in_specs=[vmem] * 10,
        out_specs=pl.BlockSpec(memory_space=pl.ANY),
        scratch_shapes=[
            pltpu.VMEM((N_CH, half_rows, cw), F32), pltpu.VMEM((3, n_tok, n_rows), BF16), pltpu.VMEM((N_CH, blocks, tokens, cw), F32),
            pltpu.VMEM((N_CH, 2, tokens, cw), F32), pltpu.VMEM((N_CH, tokens, cw), F32), pltpu.VMEM((N_CH, tokens, cw), F32),
            pltpu.VMEM((tokens, d_model), BF16), pltpu.VMEM((tokens, half_cols), BF16),
            dma((N_CH,)), dma((N_CH,)), dma((N_CH, 2)), dma((N_CH, 2)), dma((N_CH,)), dma((N_CH,)), dma((N_CH,)), dma((N_CH,)), dma,
        ],
        compiler_params=pltpu.CompilerParams(collective_id=2 + layer, has_side_effects=True, vmem_limit_bytes=32 << 20),
        name=f"combine{layer}",
    )(own1, got1, own2, send2, u, wr, ids, pos, a, a_got)


def solution(mesh):
    tok_spec = P(("dp", "ep"), None)
    cache_spec = P(None, ("dp", "ep"), "pool", None, None)
    up_spec = P(None, "ep", None, "pool")
    down_spec = P(None, "ep", "pool", None)
    in_specs = (tok_spec, cache_spec, cache_spec, P(("dp", "ep")), P(), P(), P(), P(), P(), P(None, ("dp", "ep"), None), up_spec, up_spec, down_spec)

    def body(hidden, kc, vc, lens, wq, wk, wv, wo, wr, ids, w1, w3, w2):
        layers, tokens, seq, heads, dim = kc.shape
        n_local = w1.shape[1]
        top_k = ids.shape[2]
        kc = kc.reshape(layers, tokens, seq * heads, dim)
        vc = vc.reshape(layers, tokens, seq * heads, dim)
        w1 = jnp.swapaxes(w1, 2, 3)
        w3 = jnp.swapaxes(w3, 2, 3)
        wr = jnp.swapaxes(wr, 1, 2)
        n_rows = tokens * top_k
        ids = jnp.pad(jnp.swapaxes(ids, 1, 2), ((0, 0), (0, 8 - top_k), (0, 0)))
        for layer in range(layers):
            first = layer == 0
            u, a, a_got, *tables = attention(layer, hidden, lens, kc, vc, wq, wk, wv, wo, ids if first else None, n_local)
            if first:
                pos, ids_all, off = tables
            swap = [(0, 1), (1, 0)]
            own1, send1 = experts(layer, 0, off, u, pos, w1, w3, w2, n_rows // 2)
            got1 = lax.ppermute(send1, "pool", swap)
            own2, send2 = experts(layer, 1, off, u, pos, w1, w3, w2, n_rows // 2)
            hidden = combine(layer, own1, got1, own2, send2, u, wr, ids_all, pos, a, a_got)
        return hidden

    return jax.shard_map(body, mesh=mesh, in_specs=in_specs, out_specs=tok_spec, check_vma=False)
```

```python
import functools

import jax
import jax.numpy as jnp
from jax import lax
from jax.experimental import pallas as pl
from jax.experimental.pallas import tpu as pltpu
from jax.sharding import PartitionSpec as P


MESH = pl.DeviceIdType.MESH
F32 = jnp.float32
BF16 = jnp.bfloat16
I32 = jnp.int32
EPS = 1e-6
NEG = -1e30
TB = 8
SLOTS = 4
TILE_M = 128
PARTS = 3
DEPTH = 4
VMEM_MIB = (51, 51)


def _nn(a, b):
    return lax.dot_general(a, b, (((1,), (0,)), ((), ())), preferred_element_type=F32)


def _nt(a, b, precision=None):
    return lax.dot_general(a, b, (((1,), (1,)), ((), ())), preferred_element_type=F32, precision=precision)


def _rms(v):
    return v * lax.rsqrt(jnp.mean(v * v, axis=-1, keepdims=True) + EPS)


def _where_am_i():
    p = lax.axis_index("pool")
    b = lax.axis_index("ep")
    x, c = b // 2, b % 2
    to_y = {"pool": 1 - p}
    to_x = {"ep": (1 - x) * 2 + c}
    to_c = {"ep": x * 2 + (1 - c)}
    return p, b, x, c, to_y, to_x, to_c


def _greet(peers):
    sem = pltpu.get_barrier_semaphore()
    for peer in peers:
        pl.semaphore_signal(sem, inc=1, device_id=peer, device_id_type=MESH)
    pl.semaphore_wait(sem, len(peers))


def _rcopy(src, dst, send, recv, peer):
    return pltpu.make_async_remote_copy(src_ref=src, dst_ref=dst, send_sem=send, recv_sem=recv, device_id=peer, device_id_type=MESH)


def _route(b, idg, pos_out, ids_out, off_out):
    n_local, top_k = off_out.shape[1], 6
    n_tok = pos_out.shape[2]
    er = lax.broadcasted_iota(I32, (n_local, n_tok), 0)
    tri = (lax.broadcasted_iota(I32, (n_tok, n_tok), 0) <= lax.broadcasted_iota(I32, (n_tok, n_tok), 1)).astype(F32).astype(BF16)
    before = (lax.broadcasted_iota(I32, (n_local, n_local), 0) > lax.broadcasted_iota(I32, (n_local, n_local), 1)).astype(F32).astype(BF16)
    row = lax.broadcasted_iota(I32, (8, n_tok), 0)
    for layer in range(pos_out.shape[0]):
        ids = jnp.concatenate([idg[i, layer] for i in range(idg.shape[0])], axis=1)
        local = ids - b * n_local
        member = jnp.zeros((n_local, n_tok), F32)
        for k in range(top_k):
            member = member + jnp.where(er == local[k:k + 1, :], 1.0, 0.0)
        member = member.astype(BF16)
        cum = _nn(member, tri)
        first = jnp.sum(_nn(before, member), axis=1, keepdims=True)
        place = first + cum - 1.0
        pos = jnp.full((8, n_tok), -1.0, F32)
        for k in range(top_k):
            lk = local[k:k + 1, :]
            at = jnp.sum(jnp.where(er == lk, place, 0.0), axis=0, keepdims=True)
            at = jnp.where((lk >= 0) & (lk < n_local), at, -1.0)
            pos = jnp.where(row == k, at, pos)
        pos_out[layer] = pos.astype(I32)
        ids_out[layer] = ids
        off_out[layer] = jnp.broadcast_to(first, (n_local, 128)).astype(I32)


def attn_kernel(layer, routed, x_ref, len_ref, k_hbm, v_hbm, wq_hbm, wk_hbm, wv_hbm, wo_hbm, *refs):
    if routed:
        ids_ref, *refs = refs
    u_all, a_out, a_recv, *refs = refs
    if routed:
        pos_out, ids_out, off_out, *refs, idg, isend, irecv = refs
    (kbuf, vbuf, pbuf, wq, wk, wv, wo, q3, o3, o3r, k3, v3, mls, mlr, o2, a_own,
     ksem, vsem, wsem, osend, orecv, gsend, grecv) = refs
    p, b, x, c, to_y, to_x, to_c = _where_am_i()
    half = x_ref.shape[0] // 2
    heads, dim = q3.shape[1], q3.shape[2]
    rows = kbuf.shape[2]
    n_half = half // TB
    n_blocks = 2 * n_half
    scale = dim ** -0.5

    def tok_of(n):
        return ((1 - p) + (n // n_half) * (2 * p - 1)) * half + (n % n_half) * TB

    def kv_copies(n):
        slot = n % SLOTS
        src = pl.ds(tok_of(n), TB)
        return (pltpu.make_async_copy(k_hbm.at[layer, src], kbuf.at[slot], ksem.at[slot]),
                pltpu.make_async_copy(v_hbm.at[layer, src], vbuf.at[slot], vsem.at[slot]))

    w_copies = [pltpu.make_async_copy(src.at[layer], dst, wsem.at[i])
                for i, (src, dst) in enumerate(((wq_hbm, wq), (wk_hbm, wk), (wv_hbm, wv), (wo_hbm, wo)))]
    w_copies[0].start()
    for n in range(SLOTS):
        for cp in kv_copies(n):
            cp.start()
    for cp in w_copies[1:]:
        cp.start()

    if routed:
        to_d = {"ep": (1 - x) * 2 + (1 - c)}
        _greet((to_y, to_x, to_c, to_d))
        idg[b] = ids_ref[...]
        id_copies = [_rcopy(ids_ref, idg.at[b], isend.at[i], irecv.at[i], peer) for i, peer in enumerate((to_x, to_c, to_d))]
        for cp in id_copies:
            cp.start()
    else:
        _greet((to_y, to_x, to_c))

    normed = _rms(x_ref[...].astype(F32)).astype(BF16)
    w_copies[0].wait()
    for h in range(0, heads, 2):
        part = _nn(normed, wq[:, h * dim:(h + 2) * dim]).astype(BF16).astype(F32)
        q3[:, h, :] = part[:, :dim]
        q3[:, h + 1, :] = part[:, dim:]

    row_i = lax.broadcasted_iota(I32, (heads, rows), 0)
    lane_i = lax.broadcasted_iota(I32, (heads, rows), 1)
    posl = jnp.where(lane_i % heads == row_i, lane_i // heads + p * (rows // heads), 1 << 20)
    lane = lax.broadcasted_iota(I32, (heads, 128), 1)

    def block(n, acc):
        slot = n % SLOTS
        for cp in kv_copies(n):
            cp.wait()
        t0 = tok_of(n)

        def scores(_, acc):
            for j in range(TB):
                q = q3[t0 + j].astype(BF16)
                s = _nt(q, kbuf[slot, j])
                s = jnp.where(posl < len_ref[t0 + j], s * scale, NEG)
                m = jnp.max(s, axis=1, keepdims=True)
                pr = jnp.exp(s - m)
                l = jnp.sum(pr, axis=1, keepdims=True)
                pbuf[j] = pr.astype(BF16)
                at = (n % n_half) * TB + j
                acc = jnp.where(lane == at, m, acc)
                acc = jnp.where(lane == half + at, l, acc)
            return acc

        def values(_, none):
            for j in range(TB):
                o3[t0 + j] = _nn(pbuf[j], vbuf[slot, j])
            return none

        acc = lax.fori_loop(0, 1, scores, acc)
        lax.fori_loop(0, 1, values, 0)

        @pl.when(n + SLOTS < n_blocks)
        def _():
            for cp in kv_copies(n + SLOTS):
                cp.start()

        return acc

    theirs = (1 - p) * half
    mine = p * half

    def o_copy(i):
        return _rcopy(o3.at[pl.ds(theirs + i * TB, TB)], o3r.at[pl.ds(i * TB, TB)], osend.at[i], orecv.at[i], to_y)

    def first(n, acc):
        acc = block(n, acc)
        o_copy(n).start()
        return acc

    zero = jnp.zeros((heads, 128), F32)
    mls[...] = lax.fori_loop(0, n_half, first, zero)
    ml_copy = _rcopy(mls, mlr, osend.at[n_half], orecv.at[n_half], to_y)
    ml_copy.start()
    normed = _rms(x_ref[pl.ds(mine, half), :].astype(F32)).astype(BF16)
    for i, (w, dst) in enumerate(((wk, k3), (wv, v3))):
        w_copies[1 + i].wait()
        for h in range(0, heads, 2):
            part = _nn(normed, w[:, h * dim:(h + 2) * dim]).astype(BF16).astype(F32)
            dst[:, h, :] = part[:, :dim]
            dst[:, h + 1, :] = part[:, dim:]

    sn = zero
    for j in range(half):
        sn = jnp.where(lane == j, jnp.sum(q3[mine + j] * k3[j], axis=1, keepdims=True) * scale, sn)

    if routed:
        for cp in id_copies:
            cp.wait()
        _route(b, idg, pos_out, ids_out, off_out)

    ml_own = lax.fori_loop(n_half, n_blocks, block, zero)

    for i in range(n_half):
        o_copy(i).wait()
    ml_copy.wait()
    ml_their = mlr[...]
    top = jnp.maximum(jnp.maximum(ml_own, ml_their), sn)
    w_own, w_their, w_new = jnp.exp(ml_own - top), jnp.exp(ml_their - top), jnp.exp(sn - top)
    den = pltpu.roll(ml_own, half, 1) * w_own + pltpu.roll(ml_their, half, 1) * w_their + w_new
    w_own, w_their, w_new = w_own / den, w_their / den, w_new / den
    for j in range(half):
        o3r[j] = (o3[mine + j] * w_own[:, j:j + 1] + o3r[j] * w_their[:, j:j + 1] + v3[j] * w_new[:, j:j + 1])
    for h in range(heads):
        o2[:, h * dim:(h + 1) * dim] = o3r[:, h, :].astype(BF16)
    w_copies[3].wait()
    d_model = x_ref.shape[1]
    a = (x_ref[pl.ds(mine, half), :].astype(F32) + _nn(o2[...], wo[...])).astype(BF16)
    a_own[...] = a
    me = b * 2 + p
    u_all[me] = _rms(a.astype(F32)).astype(BF16)

    y_blk, x_blk = b * 2 + (1 - p), ((1 - x) * 2 + c) * 2 + p
    d_blk = ((1 - x) * 2 + c) * 2 + (1 - p)
    lo, hi = pl.ds(0, half // 2), pl.ds(half // 2, half // 2)

    def u_copy(i, src, peer, part=None):
        ref = u_all.at[src] if part is None else u_all.at[src, part]
        return _rcopy(ref, ref, gsend.at[i], grecv.at[i], peer)

    own_y = [u_copy(0, me, to_y, lo), u_copy(1, me, to_y, hi)]
    own_x = [u_copy(2, me, to_x, hi), u_copy(3, me, to_x, lo)]
    own_c = u_copy(4, me, to_c)
    for cp in (own_y[0], own_x[0], own_y[1], own_x[1], own_c):
        cp.start()
    cw = d_model // 2
    a_out[...] = a_own[:, pl.ds(pl.multiple_of(p * cw, 128), cw)]
    a_copy = _rcopy(a_own.at[:, pl.ds(pl.multiple_of((1 - p) * cw, 128), cw)], a_recv, gsend.at[10], grecv.at[10], to_y)
    own_y[0].wait_recv()
    fwd_x = u_copy(5, y_blk, to_x, lo)
    fwd_x.start()
    own_x[0].wait_recv()
    fwd_y = u_copy(6, x_blk, to_y, hi)
    fwd_y.start()
    a_copy.start()
    own_y[1].wait_recv()
    c_y = u_copy(7, y_blk, to_c)
    c_y.start()
    own_x[1].wait_recv()
    c_x = u_copy(8, x_blk, to_c)
    c_x.start()
    fwd_x.wait_recv()
    fwd_y.wait_recv()
    c_d = u_copy(9, d_blk, to_c)
    c_d.start()
    for cp in (own_c, c_y, c_x, c_d, a_copy):
        cp.wait_recv()
    for cp in (*own_y, *own_x, own_c, fwd_x, c_y, fwd_y, c_x, c_d, a_copy):
        cp.wait_send()


def attention(layer, x, lens, kc, vc, wq, wk, wv, wo, ids=None, n_local=0):
    tokens, d_model = x.shape
    rows, dim = kc.shape[2], kc.shape[3]
    heads = wq.shape[2] // dim
    half = tokens // 2
    hbm = pl.BlockSpec(memory_space=pltpu.HBM)
    vmem = pl.BlockSpec(memory_space=pltpu.VMEM)
    dma = pltpu.SemaphoreType.DMA
    scratch = [
        pltpu.VMEM((SLOTS, TB, rows, dim), BF16), pltpu.VMEM((SLOTS, TB, rows, dim), BF16), pltpu.VMEM((TB, heads, rows), BF16),
        pltpu.VMEM(wq.shape[1:], BF16), pltpu.VMEM(wk.shape[1:], BF16), pltpu.VMEM(wv.shape[1:], BF16), pltpu.VMEM(wo.shape[1:], BF16),
        pltpu.VMEM((tokens, heads, dim), F32), pltpu.VMEM((tokens, heads, dim), F32), pltpu.VMEM((half, heads, dim), F32),
        pltpu.VMEM((half, heads, dim), F32), pltpu.VMEM((half, heads, dim), F32),
        pltpu.VMEM((heads, 128), F32), pltpu.VMEM((heads, 128), F32), pltpu.VMEM((half, heads * dim), BF16),
        pltpu.VMEM((half, d_model), BF16),
        dma((SLOTS,)), dma((SLOTS,)), dma((4,)), dma((half // TB + 1,)), dma((half // TB + 1,)), dma((11,)), dma((11,)),
    ]
    out_shape = [jax.ShapeDtypeStruct((8, half, d_model), BF16)] + [jax.ShapeDtypeStruct((half, d_model // 2), BF16)] * 2
    in_specs = [vmem, pl.BlockSpec(memory_space=pltpu.SMEM)] + [hbm] * 6
    out_specs = [vmem] * 3
    args = [x, lens, kc, vc, wq, wk, wv, wo]
    if ids is not None:
        layers = ids.shape[0]
        args.append(ids)
        in_specs.append(vmem)
        out_shape += [jax.ShapeDtypeStruct((layers, 8, 8 * half), I32)] * 2 + [jax.ShapeDtypeStruct((layers, n_local, 128), I32)]
        out_specs += [vmem] * 3
        scratch += [pltpu.VMEM((4,) + ids.shape, I32), dma((3,)), dma((3,))]
    u, a, a_got, *rest = pl.pallas_call(
        functools.partial(attn_kernel, layer, ids is not None),
        out_shape=out_shape, in_specs=in_specs, out_specs=out_specs, scratch_shapes=scratch,
        compiler_params=pltpu.CompilerParams(collective_id=layer, has_side_effects=True, vmem_limit_bytes=VMEM_MIB[layer] << 20),
    )(*args)
    return (u.reshape(8 * half, d_model), a, a_got, *rest)


def expert_kernel(layer, part, off_ref, u_ref, pos_ref, w1_hbm, w3_hbm, w2_hbm, own_ref, send_ref,
                  xt, act, w1, w3, w2, t_exp, t_at, t_new, t_lo, t_hi, live, sem):
    n_tok = u_ref.shape[0]
    n_local = w1.shape[0]
    n_rows, cw = own_ref.shape
    p = lax.axis_index("pool")
    start = part * n_rows
    weights = ((w1_hbm, w1), (w3_hbm, w3), (w2_hbm, w2))

    def copies(e):
        return [pltpu.make_async_copy(src.at[layer, e], dst.at[e], sem.at[i, e]) for i, (src, dst) in enumerate(weights)]

    def plan(e, state):
        t, n = state
        end = jnp.where(e + 1 < n_local, off_ref[layer, jnp.minimum(e + 1, n_local - 1), 0], start + n_rows)
        lo = jnp.maximum(off_ref[layer, e, 0] - start, 0)
        hi = jnp.minimum(end - start, n_rows)
        base = lo // 16 * 16
        live[n] = e

        def put(i, t):
            t_exp[t] = e
            t_at[t] = jnp.minimum(base + i * TILE_M, n_rows - TILE_M)
            t_new[t] = jnp.where(i == 0, n + 1, 0)
            t_lo[t] = lo
            t_hi[t] = hi
            return t + 1

        some = lo < hi

        @pl.when(some & (n < DEPTH))
        def _():
            for cp in copies(e):
                cp.start()

        return lax.fori_loop(0, jnp.where(some, pl.cdiv(hi - base, TILE_M), 0), put, t), jnp.where(some, n + 1, n)

    tiles, n_live = lax.fori_loop(0, n_local, plan, (0, 0))
    t_new[tiles] = 0

    def start_nth(i):
        @pl.when(i < n_live)
        def _():
            for cp in copies(live[i]):
                cp.start()

    step = 128
    for r in range(n_rows // step):
        rid = lax.broadcasted_iota(I32, (step, n_tok), 0) + (r * step + start)
        hit = rid == pos_ref[layer, 0:1, :]
        for k in range(1, 6):
            hit = hit | (rid == pos_ref[layer, k:k + 1, :])
        rows = _nn(jnp.where(hit, 1.0, 0.0).astype(BF16), u_ref[...])
        xt[:, r * step:(r + 1) * step] = jnp.transpose(rows).astype(BF16)
    xt[:, n_rows:] = jnp.zeros((xt.shape[0], xt.shape[1] - n_rows), BF16)

    def arrive(k):
        @pl.when(t_new[k] > 0)
        def _():
            for cp in copies(t_exp[k]):
                cp.wait()
            start_nth(t_new[k] - 1 + DEPTH)

    def up(k):
        e, at = t_exp[k], t_at[k]
        cols = xt[:, pl.ds(pl.multiple_of(at // 128 * 128, 128), 2 * TILE_M)]
        h1 = _nn(w1[e], cols)
        h3 = _nn(w3[e], cols)
        return jnp.transpose(h1 * jax.nn.sigmoid(h1) * h3).astype(BF16)

    def down(k):
        at = pl.multiple_of(t_at[k], 16)
        rows = act[k % 2, pl.ds(pl.multiple_of(t_at[k] % 128, 16), TILE_M), :]
        rid = lax.broadcasted_iota(I32, (TILE_M, cw), 0) + at
        mask = (rid >= t_lo[k]) & (rid < t_hi[k])
        for ref, q in ((own_ref, p), (send_ref, 1 - p)):
            y = _nn(rows, w2[t_exp[k], :, pl.ds(pl.multiple_of(q * cw, 128), cw)])
            ref[pl.ds(at, TILE_M), :] = jnp.where(mask, y, ref[pl.ds(at, TILE_M), :])

    arrive(0)
    arrive(1)
    act[0] = up(0)

    def both(k, none):
        arrive(k + 1)
        act[k % 2] = up(k)
        down(k - 1)
        return none

    lax.fori_loop(1, tiles, both, 0)
    down(tiles - 1)


def experts(layer, part, off, u, pos_t, w1, w3, w2, n_rows):
    n_local, width, d_model = w1.shape[1:]
    hbm = pl.BlockSpec(memory_space=pl.ANY)
    vmem = pl.BlockSpec(memory_space=pltpu.VMEM)
    weights = pltpu.VMEM((n_local, width, d_model), BF16)
    table = pltpu.SMEM((64,), I32)
    return pl.pallas_call(
        functools.partial(expert_kernel, layer, part),
        out_shape=[jax.ShapeDtypeStruct((n_rows, d_model // 2), F32)] * 2,
        in_specs=[pl.BlockSpec(memory_space=pltpu.SMEM), vmem, vmem, hbm, hbm, hbm],
        out_specs=[vmem, vmem],
        scratch_shapes=[pltpu.VMEM((d_model, n_rows + 2 * TILE_M), BF16), pltpu.VMEM((2, 2 * TILE_M, width), BF16),
                        weights, weights, weights,
                        table, table, table, table, table, table, pltpu.SemaphoreType.DMA((3, n_local))],
        compiler_params=pltpu.CompilerParams(vmem_limit_bytes=45 << 20),
        cost_estimate=pl.CostEstimate(flops=int(4e9), bytes_accessed=18 << 20, transcendentals=0),
    )(off, u, pos_t, w1, w3, w2)


N_CH = 4


def combine_kernel(layer, *refs):
    early, refs = refs[:2 * (PARTS - 1)], refs[2 * (PARTS - 1):]
    _combine(layer, early, *refs)


def _combine(layer, early, own2_ref, send2_ref, u_ref, wr_ref, ids_ref, pos_ref, a_ref, a_got_ref, x_out,
                   yr, gm, tb, tcr, txs, txr, xo, a_buf, ysend, yrecv, csend, crecv, xsend, xrecv, fsend, frecv, lsem):
    p, _, x, c, to_y, to_x, to_c = _where_am_i()
    part_rows, cw = yr.shape[1], yr.shape[2]
    n_rows = PARTS * part_rows
    n_tok, top_k = u_ref.shape[0], 6
    tokens = 2 * a_ref.shape[0]
    mine = p * N_CH
    _greet((to_y, to_x, to_c))

    def cols(i):
        return pl.ds(pl.multiple_of(i * cw, 128), cw)

    y_copies = [_rcopy(send2_ref.at[:, j * cw:(j + 1) * cw], yr.at[j], ysend.at[j], yrecv.at[j], to_y) for j in range(N_CH)]
    for cp in y_copies:
        cp.start()

    half = a_ref.shape[0]
    a_buf[pl.ds(pl.multiple_of(p * half, half), half), :] = a_ref[...]
    a_buf[pl.ds(pl.multiple_of((1 - p) * half, half), half), :] = a_got_ref[...]
    step = 128
    n_exp = wr_ref.shape[1]
    wr = wr_ref[layer]
    wr1 = wr.astype(BF16)
    wr2 = (wr - wr1.astype(F32)).astype(BF16)
    wr3 = (wr - wr1.astype(F32) - wr2.astype(F32)).astype(BF16)

    def gates(i, carry):
        at = pl.ds(pl.multiple_of(i * step, step), step)
        rows = u_ref[at, :]
        logits = _nt(rows, wr1) + (_nt(rows, wr2) + _nt(rows, wr3))
        lane = lax.broadcasted_iota(I32, (step, n_exp), 1)
        ids = jnp.transpose(ids_ref[layer, :, at].astype(F32)).astype(I32)
        pos = jnp.transpose(pos_ref[layer, :, at].astype(F32)).astype(I32)
        g = [jnp.sum(jnp.where(lane == ids[:, k:k + 1], logits, 0.0), axis=1, keepdims=True) for k in range(top_k)]
        top = functools.reduce(jnp.maximum, g)
        g = [jnp.exp(v - top) for v in g]
        den = functools.reduce(jnp.add, g)
        g = [v / den for v in g]
        rid = lax.broadcasted_iota(I32, (step, n_rows), 1)
        mat = jnp.zeros((step, n_rows), F32)
        for k in range(top_k):
            mat = jnp.where(rid == pos[:, k:k + 1], g[k], mat)
        g1 = mat.astype(BF16)
        rest = mat - g1.astype(F32)
        g2 = rest.astype(BF16)
        gm[0, at, :] = g1
        gm[1, at, :] = g2
        gm[2, at, :] = (rest - g2.astype(F32)).astype(BF16)
        return carry

    lax.fori_loop(0, n_tok // step, gates, 0)

    def gated(ys, rows):
        return _nn(gm[0, :, rows], ys) + (_nn(gm[1, :, rows], ys) + _nn(gm[2, :, rows], ys))

    for j in range(N_CH):
        at = slice(j * cw, (j + 1) * cw)
        ys = [(early[2 * i][:, at] + early[2 * i + 1][:, at]).astype(BF16) for i in range(PARTS - 1)]
        tb[j] = gated(jnp.concatenate(ys, axis=0), pl.ds(0, n_rows - part_rows)).reshape(n_tok // tokens, tokens, cw)

    f_copies = []

    def finish(j, c_copies, x_copy):
        x_copy.wait_recv()
        own = tb[j, x * 2 + c] + tcr[j, x]
        new = (a_buf[:, j * cw:(j + 1) * cw].astype(F32) + (own + txr[j])).astype(BF16)
        xo[:, cols(mine + j)] = new
        f_copy = _rcopy(xo.at[:, cols(mine + j)], xo.at[:, cols(mine + j)], fsend.at[j], frecv.at[j], to_y)
        f_copy.start()
        f_copies.append((c_copies, x_copy, f_copy))

    last = None
    for j in range(N_CH):
        y_copies[j].wait_recv()
        ys = (own2_ref[:, j * cw:(j + 1) * cw] + yr[j]).astype(BF16)
        tb[j] = tb[j] + gated(ys, pl.ds(n_rows - part_rows, part_rows)).reshape(n_tok // tokens, tokens, cw)
        c_copies = [_rcopy(tb.at[j, i * 2 + (1 - c)], tcr.at[j, i], csend.at[j, i], crecv.at[j, i], to_c) for i in range(2)]
        for cp in c_copies:
            cp.start()
        if last is not None:
            finish(*last)
        for cp in c_copies:
            cp.wait_recv()
        txs[j] = tb[j, (1 - x) * 2 + c] + tcr[j, 1 - x]
        x_copy = _rcopy(txs.at[j], txr.at[j], xsend.at[j], xrecv.at[j], to_x)
        x_copy.start()
        last = (j, c_copies, x_copy)
    finish(*last)
    for _, _, f_copy in f_copies:
        f_copy.wait_recv()
    out = pltpu.make_async_copy(xo, x_out, lsem)
    out.start()
    for cp in y_copies:
        cp.wait_send()
    for c_copies, x_copy, f_copy in f_copies:
        for cp in c_copies:
            cp.wait_send()
        x_copy.wait_send()
        f_copy.wait_send()
    out.wait()


def combine(layer, early, own, send, u, wr, ids, pos, a, a_got):
    part_rows = own.shape[0]
    n_rows = PARTS * part_rows
    half, half_cols = a.shape
    tokens = 2 * half
    n_tok, d_model = u.shape
    cw = half_cols // N_CH
    vmem = pl.BlockSpec(memory_space=pltpu.VMEM)
    blocks = n_tok // tokens
    dma = pltpu.SemaphoreType.DMA
    return pl.pallas_call(
        functools.partial(combine_kernel, layer),
        out_shape=jax.ShapeDtypeStruct((tokens, d_model), BF16),
        in_specs=[vmem] * (len(early) + 8),
        out_specs=pl.BlockSpec(memory_space=pl.ANY),
        scratch_shapes=[
            pltpu.VMEM((N_CH, part_rows, cw), F32), pltpu.VMEM((3, n_tok, n_rows), BF16), pltpu.VMEM((N_CH, blocks, tokens, cw), F32),
            pltpu.VMEM((N_CH, 2, tokens, cw), F32), pltpu.VMEM((N_CH, tokens, cw), F32), pltpu.VMEM((N_CH, tokens, cw), F32),
            pltpu.VMEM((tokens, d_model), BF16), pltpu.VMEM((tokens, half_cols), BF16),
            dma((N_CH,)), dma((N_CH,)), dma((N_CH, 2)), dma((N_CH, 2)), dma((N_CH,)), dma((N_CH,)), dma((N_CH,)), dma((N_CH,)), dma,
        ],
        compiler_params=pltpu.CompilerParams(collective_id=2 + layer, has_side_effects=True, vmem_limit_bytes=32 << 20),
    )(*early, own, send, u, wr, ids, pos, a, a_got)


def solution(mesh):
    tok_spec = P(("dp", "ep"), None)
    cache_spec = P(None, ("dp", "ep"), "pool", None, None)
    up_spec = P(None, "ep", None, "pool")
    down_spec = P(None, "ep", "pool", None)
    in_specs = (tok_spec, cache_spec, cache_spec, P(("dp", "ep")), P(), P(), P(), P(), P(), P(None, ("dp", "ep"), None), up_spec, up_spec, down_spec)

    def body(hidden, kc, vc, lens, wq, wk, wv, wo, wr, ids, w1, w3, w2):
        layers, tokens, seq, heads, dim = kc.shape
        n_local = w1.shape[1]
        top_k = ids.shape[2]
        kc = kc.reshape(layers, tokens, seq * heads, dim)
        vc = vc.reshape(layers, tokens, seq * heads, dim)
        w1 = jnp.swapaxes(w1, 2, 3)
        w3 = jnp.swapaxes(w3, 2, 3)
        wr = jnp.swapaxes(wr, 1, 2)
        n_rows = tokens * top_k
        ids = jnp.pad(jnp.swapaxes(ids, 1, 2), ((0, 0), (0, 8 - top_k), (0, 0)))
        for layer in range(layers):
            first = layer == 0
            u, a, a_got, *tables = attention(layer, hidden, lens, kc, vc, wq, wk, wv, wo, ids if first else None, n_local)
            if first:
                pos, ids_all, off = tables
            early = []
            for part in range(PARTS):
                own, send = experts(layer, part, off, u, pos, w1, w3, w2, n_rows // PARTS)
                if part < PARTS - 1:
                    early += [own, lax.ppermute(send, "pool", [(0, 1), (1, 0)])]
            hidden = combine(layer, early, own, send, u, wr, ids_all, pos, a, a_got)
        return hidden

    return jax.shard_map(body, mesh=mesh, in_specs=in_specs, out_specs=tok_spec, check_vma=False)
```

```python
import functools

import jax
import jax.numpy as jnp
from jax import lax
from jax.experimental import pallas as pl
from jax.experimental.pallas import tpu as pltpu
from jax.sharding import PartitionSpec as P


MESH = pl.DeviceIdType.MESH
F32 = jnp.float32
BF16 = jnp.bfloat16
I32 = jnp.int32
EPS = 1e-6
NEG = -1e30
TB = 8
SLOTS = 4
TILE_M = 128
PART_ROWS = (256, 384, 128)
PARTS = len(PART_ROWS)
DEPTH = 4
VMEM_MIB = (51, 51)


def _nn(a, b):
    return lax.dot_general(a, b, (((1,), (0,)), ((), ())), preferred_element_type=F32)


def _nt(a, b, precision=None):
    return lax.dot_general(a, b, (((1,), (1,)), ((), ())), preferred_element_type=F32, precision=precision)


def _rms(v):
    return v * lax.rsqrt(jnp.mean(v * v, axis=-1, keepdims=True) + EPS)


def _where_am_i():
    p = lax.axis_index("pool")
    b = lax.axis_index("ep")
    x, c = b // 2, b % 2
    to_y = {"pool": 1 - p}
    to_x = {"ep": (1 - x) * 2 + c}
    to_c = {"ep": x * 2 + (1 - c)}
    return p, b, x, c, to_y, to_x, to_c


def _greet(peers):
    sem = pltpu.get_barrier_semaphore()
    for peer in peers:
        pl.semaphore_signal(sem, inc=1, device_id=peer, device_id_type=MESH)
    pl.semaphore_wait(sem, len(peers))


def _rcopy(src, dst, send, recv, peer):
    return pltpu.make_async_remote_copy(src_ref=src, dst_ref=dst, send_sem=send, recv_sem=recv, device_id=peer, device_id_type=MESH)


def _route(b, idg, pos_out, ids_out, off_out):
    n_local, top_k = off_out.shape[1], 6
    n_tok = pos_out.shape[2]
    er = lax.broadcasted_iota(I32, (n_local, n_tok), 0)
    tri = (lax.broadcasted_iota(I32, (n_tok, n_tok), 0) <= lax.broadcasted_iota(I32, (n_tok, n_tok), 1)).astype(F32).astype(BF16)
    before = (lax.broadcasted_iota(I32, (n_local, n_local), 0) > lax.broadcasted_iota(I32, (n_local, n_local), 1)).astype(F32).astype(BF16)
    row = lax.broadcasted_iota(I32, (8, n_tok), 0)
    for layer in range(pos_out.shape[0]):
        ids = jnp.concatenate([idg[i, layer] for i in range(idg.shape[0])], axis=1)
        local = ids - b * n_local
        member = jnp.zeros((n_local, n_tok), F32)
        for k in range(top_k):
            member = member + jnp.where(er == local[k:k + 1, :], 1.0, 0.0)
        member = member.astype(BF16)
        cum = _nn(member, tri)
        first = jnp.sum(_nn(before, member), axis=1, keepdims=True)
        place = first + cum - 1.0
        pos = jnp.full((8, n_tok), -1.0, F32)
        for k in range(top_k):
            lk = local[k:k + 1, :]
            at = jnp.sum(jnp.where(er == lk, place, 0.0), axis=0, keepdims=True)
            at = jnp.where((lk >= 0) & (lk < n_local), at, -1.0)
            pos = jnp.where(row == k, at, pos)
        pos_out[layer] = pos.astype(I32)
        ids_out[layer] = ids
        off_out[layer] = jnp.broadcast_to(first, (n_local, 128)).astype(I32)


def attn_kernel(layer, routed, x_ref, len_ref, k_hbm, v_hbm, wq_hbm, wk_hbm, wv_hbm, wo_hbm, *refs):
    if routed:
        ids_ref, *refs = refs
    u_all, a_out, a_recv, *refs = refs
    if routed:
        pos_out, ids_out, off_out, *refs, idg, isend, irecv = refs
    (kbuf, vbuf, pbuf, wq, wk, wv, wo, q3, o3, o3r, k3, v3, mls, mlr, o2, a_own,
     ksem, vsem, wsem, osend, orecv, gsend, grecv) = refs
    p, b, x, c, to_y, to_x, to_c = _where_am_i()
    half = x_ref.shape[0] // 2
    heads, dim = q3.shape[1], q3.shape[2]
    rows = kbuf.shape[2]
    n_half = half // TB
    n_blocks = 2 * n_half
    scale = dim ** -0.5

    def tok_of(n):
        return ((1 - p) + (n // n_half) * (2 * p - 1)) * half + (n % n_half) * TB

    def kv_copies(n):
        slot = n % SLOTS
        src = pl.ds(tok_of(n), TB)
        return (pltpu.make_async_copy(k_hbm.at[layer, src], kbuf.at[slot], ksem.at[slot]),
                pltpu.make_async_copy(v_hbm.at[layer, src], vbuf.at[slot], vsem.at[slot]))

    w_copies = [pltpu.make_async_copy(src.at[layer], dst, wsem.at[i])
                for i, (src, dst) in enumerate(((wq_hbm, wq), (wk_hbm, wk), (wv_hbm, wv), (wo_hbm, wo)))]
    w_copies[0].start()
    for n in range(SLOTS):
        for cp in kv_copies(n):
            cp.start()
    for cp in w_copies[1:]:
        cp.start()

    if routed:
        to_d = {"ep": (1 - x) * 2 + (1 - c)}
        _greet((to_y, to_x, to_c, to_d))
        idg[b] = ids_ref[...]
        id_copies = [_rcopy(ids_ref, idg.at[b], isend.at[i], irecv.at[i], peer) for i, peer in enumerate((to_x, to_c, to_d))]
        for cp in id_copies:
            cp.start()
    else:
        _greet((to_y, to_x, to_c))

    normed = _rms(x_ref[...].astype(F32)).astype(BF16)
    w_copies[0].wait()
    for h in range(0, heads, 2):
        part = _nn(normed, wq[:, h * dim:(h + 2) * dim]).astype(BF16).astype(F32)
        q3[:, h, :] = part[:, :dim]
        q3[:, h + 1, :] = part[:, dim:]

    row_i = lax.broadcasted_iota(I32, (heads, rows), 0)
    lane_i = lax.broadcasted_iota(I32, (heads, rows), 1)
    posl = jnp.where(lane_i % heads == row_i, lane_i // heads + p * (rows // heads), 1 << 20)
    lane = lax.broadcasted_iota(I32, (heads, 128), 1)

    def block(n, acc):
        slot = n % SLOTS
        for cp in kv_copies(n):
            cp.wait()
        t0 = tok_of(n)

        def scores(_, acc):
            for j in range(TB):
                q = q3[t0 + j].astype(BF16)
                s = _nt(q, kbuf[slot, j])
                s = jnp.where(posl < len_ref[t0 + j], s * scale, NEG)
                m = jnp.max(s, axis=1, keepdims=True)
                pr = jnp.exp(s - m)
                l = jnp.sum(pr, axis=1, keepdims=True)
                pbuf[j] = pr.astype(BF16)
                at = (n % n_half) * TB + j
                acc = jnp.where(lane == at, m, acc)
                acc = jnp.where(lane == half + at, l, acc)
            return acc

        def values(_, none):
            for j in range(TB):
                o3[t0 + j] = _nn(pbuf[j], vbuf[slot, j])
            return none

        acc = lax.fori_loop(0, 1, scores, acc)
        lax.fori_loop(0, 1, values, 0)

        @pl.when(n + SLOTS < n_blocks)
        def _():
            for cp in kv_copies(n + SLOTS):
                cp.start()

        return acc

    theirs = (1 - p) * half
    mine = p * half

    def o_copy(i):
        return _rcopy(o3.at[pl.ds(theirs + i * TB, TB)], o3r.at[pl.ds(i * TB, TB)], osend.at[i], orecv.at[i], to_y)

    def first(n, acc):
        acc = block(n, acc)
        o_copy(n).start()
        return acc

    zero = jnp.zeros((heads, 128), F32)
    mls[...] = lax.fori_loop(0, n_half, first, zero)
    ml_copy = _rcopy(mls, mlr, osend.at[n_half], orecv.at[n_half], to_y)
    ml_copy.start()
    normed = _rms(x_ref[pl.ds(mine, half), :].astype(F32)).astype(BF16)
    for i, (w, dst) in enumerate(((wk, k3), (wv, v3))):
        w_copies[1 + i].wait()
        for h in range(0, heads, 2):
            part = _nn(normed, w[:, h * dim:(h + 2) * dim]).astype(BF16).astype(F32)
            dst[:, h, :] = part[:, :dim]
            dst[:, h + 1, :] = part[:, dim:]

    sn = zero
    for j in range(half):
        sn = jnp.where(lane == j, jnp.sum(q3[mine + j] * k3[j], axis=1, keepdims=True) * scale, sn)

    if routed:
        for cp in id_copies:
            cp.wait()
        _route(b, idg, pos_out, ids_out, off_out)

    ml_own = lax.fori_loop(n_half, n_blocks, block, zero)

    for i in range(n_half):
        o_copy(i).wait()
    ml_copy.wait()
    ml_their = mlr[...]
    top = jnp.maximum(jnp.maximum(ml_own, ml_their), sn)
    w_own, w_their, w_new = jnp.exp(ml_own - top), jnp.exp(ml_their - top), jnp.exp(sn - top)
    den = pltpu.roll(ml_own, half, 1) * w_own + pltpu.roll(ml_their, half, 1) * w_their + w_new
    w_own, w_their, w_new = w_own / den, w_their / den, w_new / den
    for j in range(half):
        o3r[j] = (o3[mine + j] * w_own[:, j:j + 1] + o3r[j] * w_their[:, j:j + 1] + v3[j] * w_new[:, j:j + 1])
    for h in range(heads):
        o2[:, h * dim:(h + 1) * dim] = o3r[:, h, :].astype(BF16)
    w_copies[3].wait()
    d_model = x_ref.shape[1]
    a = (x_ref[pl.ds(mine, half), :].astype(F32) + _nn(o2[...], wo[...])).astype(BF16)
    a_own[...] = a
    me = b * 2 + p
    u_all[me] = _rms(a.astype(F32)).astype(BF16)

    y_blk, x_blk = b * 2 + (1 - p), ((1 - x) * 2 + c) * 2 + p
    d_blk = ((1 - x) * 2 + c) * 2 + (1 - p)
    lo, hi = pl.ds(0, half // 2), pl.ds(half // 2, half // 2)

    def u_copy(i, src, peer, part=None):
        ref = u_all.at[src] if part is None else u_all.at[src, part]
        return _rcopy(ref, ref, gsend.at[i], grecv.at[i], peer)

    own_y = [u_copy(0, me, to_y, lo), u_copy(1, me, to_y, hi)]
    own_x = [u_copy(2, me, to_x, hi), u_copy(3, me, to_x, lo)]
    own_c = u_copy(4, me, to_c)
    for cp in (own_y[0], own_x[0], own_y[1], own_x[1], own_c):
        cp.start()
    cw = d_model // 2
    a_out[...] = a_own[:, pl.ds(pl.multiple_of(p * cw, 128), cw)]
    a_copy = _rcopy(a_own.at[:, pl.ds(pl.multiple_of((1 - p) * cw, 128), cw)], a_recv, gsend.at[10], grecv.at[10], to_y)
    own_y[0].wait_recv()
    fwd_x = u_copy(5, y_blk, to_x, lo)
    fwd_x.start()
    own_x[0].wait_recv()
    fwd_y = u_copy(6, x_blk, to_y, hi)
    fwd_y.start()
    a_copy.start()
    own_y[1].wait_recv()
    c_y = u_copy(7, y_blk, to_c)
    c_y.start()
    own_x[1].wait_recv()
    c_x = u_copy(8, x_blk, to_c)
    c_x.start()
    fwd_x.wait_recv()
    fwd_y.wait_recv()
    c_d = u_copy(9, d_blk, to_c)
    c_d.start()
    for cp in (own_c, c_y, c_x, c_d, a_copy):
        cp.wait_recv()
    for cp in (*own_y, *own_x, own_c, fwd_x, c_y, fwd_y, c_x, c_d, a_copy):
        cp.wait_send()


def attention(layer, x, lens, kc, vc, wq, wk, wv, wo, ids=None, n_local=0):
    tokens, d_model = x.shape
    rows, dim = kc.shape[2], kc.shape[3]
    heads = wq.shape[2] // dim
    half = tokens // 2
    hbm = pl.BlockSpec(memory_space=pltpu.HBM)
    vmem = pl.BlockSpec(memory_space=pltpu.VMEM)
    dma = pltpu.SemaphoreType.DMA
    scratch = [
        pltpu.VMEM((SLOTS, TB, rows, dim), BF16), pltpu.VMEM((SLOTS, TB, rows, dim), BF16), pltpu.VMEM((TB, heads, rows), BF16),
        pltpu.VMEM(wq.shape[1:], BF16), pltpu.VMEM(wk.shape[1:], BF16), pltpu.VMEM(wv.shape[1:], BF16), pltpu.VMEM(wo.shape[1:], BF16),
        pltpu.VMEM((tokens, heads, dim), F32), pltpu.VMEM((tokens, heads, dim), F32), pltpu.VMEM((half, heads, dim), F32),
        pltpu.VMEM((half, heads, dim), F32), pltpu.VMEM((half, heads, dim), F32),
        pltpu.VMEM((heads, 128), F32), pltpu.VMEM((heads, 128), F32), pltpu.VMEM((half, heads * dim), BF16),
        pltpu.VMEM((half, d_model), BF16),
        dma((SLOTS,)), dma((SLOTS,)), dma((4,)), dma((half // TB + 1,)), dma((half // TB + 1,)), dma((11,)), dma((11,)),
    ]
    out_shape = [jax.ShapeDtypeStruct((8, half, d_model), BF16)] + [jax.ShapeDtypeStruct((half, d_model // 2), BF16)] * 2
    in_specs = [vmem, pl.BlockSpec(memory_space=pltpu.SMEM)] + [hbm] * 6
    out_specs = [vmem] * 3
    args = [x, lens, kc, vc, wq, wk, wv, wo]
    if ids is not None:
        layers = ids.shape[0]
        args.append(ids)
        in_specs.append(vmem)
        out_shape += [jax.ShapeDtypeStruct((layers, 8, 8 * half), I32)] * 2 + [jax.ShapeDtypeStruct((layers, n_local, 128), I32)]
        out_specs += [vmem] * 3
        scratch += [pltpu.VMEM((4,) + ids.shape, I32), dma((3,)), dma((3,))]
    u, a, a_got, *rest = pl.pallas_call(
        functools.partial(attn_kernel, layer, ids is not None),
        out_shape=out_shape, in_specs=in_specs, out_specs=out_specs, scratch_shapes=scratch,
        compiler_params=pltpu.CompilerParams(collective_id=layer, has_side_effects=True, vmem_limit_bytes=VMEM_MIB[layer] << 20),
    )(*args)
    return (u.reshape(8 * half, d_model), a, a_got, *rest)


def expert_kernel(layer, part, off_ref, u_ref, pos_ref, w1_hbm, w3_hbm, w2_hbm, own_ref, send_ref,
                  xt, act, w1, w3, w2, t_exp, t_at, t_new, t_lo, t_hi, live, sem):
    n_tok = u_ref.shape[0]
    n_local = w1.shape[0]
    n_rows, cw = own_ref.shape
    p = lax.axis_index("pool")
    start = sum(PART_ROWS[:part])
    weights = ((w1_hbm, w1), (w3_hbm, w3), (w2_hbm, w2))

    def copies(e):
        return [pltpu.make_async_copy(src.at[layer, e], dst.at[e], sem.at[i, e]) for i, (src, dst) in enumerate(weights)]

    def plan(e, state):
        t, n = state
        end = jnp.where(e + 1 < n_local, off_ref[layer, jnp.minimum(e + 1, n_local - 1), 0], start + n_rows)
        lo = jnp.maximum(off_ref[layer, e, 0] - start, 0)
        hi = jnp.minimum(end - start, n_rows)
        base = lo // 16 * 16
        live[n] = e

        def put(i, t):
            t_exp[t] = e
            t_at[t] = jnp.minimum(base + i * TILE_M, n_rows - TILE_M)
            t_new[t] = jnp.where(i == 0, n + 1, 0)
            t_lo[t] = lo
            t_hi[t] = hi
            return t + 1

        some = lo < hi

        @pl.when(some & (n < DEPTH))
        def _():
            for cp in copies(e):
                cp.start()

        return lax.fori_loop(0, jnp.where(some, pl.cdiv(hi - base, TILE_M), 0), put, t), jnp.where(some, n + 1, n)

    tiles, n_live = lax.fori_loop(0, n_local, plan, (0, 0))
    t_new[tiles] = 0

    def start_nth(i):
        @pl.when(i < n_live)
        def _():
            for cp in copies(live[i]):
                cp.start()

    step = 128
    for r in range(n_rows // step):
        rid = lax.broadcasted_iota(I32, (step, n_tok), 0) + (r * step + start)
        hit = rid == pos_ref[layer, 0:1, :]
        for k in range(1, 6):
            hit = hit | (rid == pos_ref[layer, k:k + 1, :])
        rows = _nn(jnp.where(hit, 1.0, 0.0).astype(BF16), u_ref[...])
        xt[:, r * step:(r + 1) * step] = jnp.transpose(rows).astype(BF16)
    xt[:, n_rows:] = jnp.zeros((xt.shape[0], xt.shape[1] - n_rows), BF16)

    def arrive(k):
        @pl.when(t_new[k] > 0)
        def _():
            for cp in copies(t_exp[k]):
                cp.wait()
            start_nth(t_new[k] - 1 + DEPTH)

    def up(k):
        e, at = t_exp[k], t_at[k]
        cols = xt[:, pl.ds(pl.multiple_of(at // 128 * 128, 128), 2 * TILE_M)]
        h1 = _nn(w1[e], cols)
        h3 = _nn(w3[e], cols)
        return jnp.transpose(h1 * jax.nn.sigmoid(h1) * h3).astype(BF16)

    def down(k):
        at = pl.multiple_of(t_at[k], 16)
        rows = act[k % 2, pl.ds(pl.multiple_of(t_at[k] % 128, 16), TILE_M), :]
        rid = lax.broadcasted_iota(I32, (TILE_M, cw), 0) + at
        mask = (rid >= t_lo[k]) & (rid < t_hi[k])
        for ref, q in ((own_ref, p), (send_ref, 1 - p)):
            y = _nn(rows, w2[t_exp[k], :, pl.ds(pl.multiple_of(q * cw, 128), cw)])
            ref[pl.ds(at, TILE_M), :] = jnp.where(mask, y, ref[pl.ds(at, TILE_M), :])

    arrive(0)
    arrive(1)
    act[0] = up(0)

    def both(k, none):
        arrive(k + 1)
        act[k % 2] = up(k)
        down(k - 1)
        return none

    lax.fori_loop(1, tiles, both, 0)
    down(tiles - 1)


def experts(layer, part, off, u, pos_t, w1, w3, w2, n_rows):
    n_local, width, d_model = w1.shape[1:]
    hbm = pl.BlockSpec(memory_space=pl.ANY)
    vmem = pl.BlockSpec(memory_space=pltpu.VMEM)
    weights = pltpu.VMEM((n_local, width, d_model), BF16)
    table = pltpu.SMEM((64,), I32)
    return pl.pallas_call(
        functools.partial(expert_kernel, layer, part),
        out_shape=[jax.ShapeDtypeStruct((n_rows, d_model // 2), F32)] * 2,
        in_specs=[pl.BlockSpec(memory_space=pltpu.SMEM), vmem, vmem, hbm, hbm, hbm],
        out_specs=[vmem, vmem],
        scratch_shapes=[pltpu.VMEM((d_model, n_rows + 2 * TILE_M), BF16), pltpu.VMEM((2, 2 * TILE_M, width), BF16),
                        weights, weights, weights,
                        table, table, table, table, table, table, pltpu.SemaphoreType.DMA((3, n_local))],
        compiler_params=pltpu.CompilerParams(vmem_limit_bytes=45 << 20),
        cost_estimate=pl.CostEstimate(flops=int(4e9), bytes_accessed=18 << 20, transcendentals=0),
    )(off, u, pos_t, w1, w3, w2)


N_CH = 4


def _gated(gm, rows, ys):
    return _nn(gm[0, :, rows], ys) + (_nn(gm[1, :, rows], ys) + _nn(gm[2, :, rows], ys))


def gate_kernel(layer, own_ref, got_ref, u_ref, wr_ref, ids_ref, pos_ref, gm, t0):
    n_rows, n_tok, top_k = gm.shape[2], gm.shape[1], 6
    step = 128
    n_exp = wr_ref.shape[1]
    wr = wr_ref[layer]
    wr1 = wr.astype(BF16)
    wr2 = (wr - wr1.astype(F32)).astype(BF16)
    wr3 = (wr - wr1.astype(F32) - wr2.astype(F32)).astype(BF16)

    def gates(i, carry):
        at = pl.ds(pl.multiple_of(i * step, step), step)
        rows = u_ref[at, :]
        logits = _nt(rows, wr1) + (_nt(rows, wr2) + _nt(rows, wr3))
        lane = lax.broadcasted_iota(I32, (step, n_exp), 1)
        ids = jnp.transpose(ids_ref[layer, :, at].astype(F32)).astype(I32)
        pos = jnp.transpose(pos_ref[layer, :, at].astype(F32)).astype(I32)
        g = [jnp.sum(jnp.where(lane == ids[:, k:k + 1], logits, 0.0), axis=1, keepdims=True) for k in range(top_k)]
        top = functools.reduce(jnp.maximum, g)
        g = [jnp.exp(v - top) for v in g]
        den = functools.reduce(jnp.add, g)
        g = [v / den for v in g]
        rid = lax.broadcasted_iota(I32, (step, n_rows), 1)
        mat = jnp.zeros((step, n_rows), F32)
        for k in range(top_k):
            mat = jnp.where(rid == pos[:, k:k + 1], g[k], mat)
        g1 = mat.astype(BF16)
        rest = mat - g1.astype(F32)
        g2 = rest.astype(BF16)
        gm[0, at, :] = g1
        gm[1, at, :] = g2
        gm[2, at, :] = (rest - g2.astype(F32)).astype(BF16)
        return carry

    lax.fori_loop(0, n_tok // step, gates, 0)

    part_rows, cols = own_ref.shape
    total = _gated(gm, pl.ds(0, part_rows), (own_ref[...] + got_ref[...]).astype(BF16))
    cw = cols // N_CH
    for j in range(N_CH):
        t0[j] = total[:, j * cw:(j + 1) * cw].reshape(t0.shape[1:])


def gates(layer, own, got, u, wr, ids, pos):
    n_tok = u.shape[0]
    tokens = n_tok // 4
    vmem = pl.BlockSpec(memory_space=pltpu.VMEM)
    return pl.pallas_call(
        functools.partial(gate_kernel, layer),
        out_shape=[jax.ShapeDtypeStruct((3, n_tok, sum(PART_ROWS)), BF16),
                   jax.ShapeDtypeStruct((N_CH, 4, tokens, own.shape[1] // N_CH), F32)],
        in_specs=[vmem] * 6, out_specs=[vmem] * 2,
        compiler_params=pltpu.CompilerParams(vmem_limit_bytes=20 << 20),
        cost_estimate=pl.CostEstimate(flops=int(2e9), bytes_accessed=4 << 20, transcendentals=0),
    )(own, got, u, wr, ids, pos)


def combine_kernel(own1_ref, got1_ref, own2_ref, send2_ref, gm, t0_ref, a_ref, a_got_ref, x_out,
                   yr, tb, tcr, txs, txr, xo, a_buf, ysend, yrecv, csend, crecv, xsend, xrecv, fsend, frecv, lsem):
    p, _, x, c, to_y, to_x, to_c = _where_am_i()
    cw = yr.shape[2]
    mine = p * N_CH
    _greet((to_y, to_x, to_c))

    def cols(i):
        return pl.ds(pl.multiple_of(i * cw, 128), cw)

    y_copies = [_rcopy(send2_ref.at[:, j * cw:(j + 1) * cw], yr.at[j], ysend.at[j], yrecv.at[j], to_y) for j in range(N_CH)]
    for cp in y_copies:
        cp.start()

    half = a_ref.shape[0]
    a_buf[pl.ds(pl.multiple_of(p * half, half), half), :] = a_ref[...]
    a_buf[pl.ds(pl.multiple_of((1 - p) * half, half), half), :] = a_got_ref[...]
    second, third = pl.ds(PART_ROWS[0], PART_ROWS[1]), pl.ds(PART_ROWS[0] + PART_ROWS[1], PART_ROWS[2])
    total = _gated(gm, second, (own1_ref[...] + got1_ref[...]).astype(BF16))
    for j in range(N_CH):
        tb[j] = t0_ref[j] + total[:, j * cw:(j + 1) * cw].reshape(tb.shape[1:])

    chunks = []

    def gather(j):
        y_copies[j].wait_recv()
        ys = (own2_ref[:, j * cw:(j + 1) * cw] + yr[j]).astype(BF16)
        tb[j] = tb[j] + _gated(gm, third, ys).reshape(tb.shape[1:])
        c_copies = [_rcopy(tb.at[j, i * 2 + (1 - c)], tcr.at[j, i], csend.at[j, i], crecv.at[j, i], to_c) for i in range(2)]
        for cp in c_copies:
            cp.start()
        chunks.append(c_copies)

    def cross(j):
        for cp in chunks[j]:
            cp.wait_recv()
        txs[j] = tb[j, (1 - x) * 2 + c] + tcr[j, 1 - x]
        x_copy = _rcopy(txs.at[j], txr.at[j], xsend.at[j], xrecv.at[j], to_x)
        x_copy.start()
        chunks[j].append(x_copy)

    def finish(j):
        chunks[j][-1].wait_recv()
        own = tb[j, x * 2 + c] + tcr[j, x]
        new = (a_buf[:, j * cw:(j + 1) * cw].astype(F32) + (own + txr[j])).astype(BF16)
        xo[:, cols(mine + j)] = new
        f_copy = _rcopy(xo.at[:, cols(mine + j)], xo.at[:, cols(mine + j)], fsend.at[j], frecv.at[j], to_y)
        f_copy.start()
        chunks[j].append(f_copy)

    for j in range(N_CH + 2):
        if j < N_CH:
            gather(j)
        if 0 <= j - 1 < N_CH:
            cross(j - 1)
        if 0 <= j - 2 < N_CH:
            finish(j - 2)
    for copies in chunks:
        copies[-1].wait_recv()
    out = pltpu.make_async_copy(xo, x_out, lsem)
    out.start()
    for cp in y_copies:
        cp.wait_send()
    for copies in chunks:
        for cp in copies:
            cp.wait_send()
    out.wait()


def combine(layer, own1, got1, own2, send2, gm, t0, a, a_got):
    half, half_cols = a.shape
    tokens = 2 * half
    cw = half_cols // N_CH
    vmem = pl.BlockSpec(memory_space=pltpu.VMEM)
    dma = pltpu.SemaphoreType.DMA
    return pl.pallas_call(
        combine_kernel,
        out_shape=jax.ShapeDtypeStruct((tokens, 2 * half_cols), BF16),
        in_specs=[vmem] * 8,
        out_specs=pl.BlockSpec(memory_space=pl.ANY),
        scratch_shapes=[
            pltpu.VMEM((N_CH, own2.shape[0], cw), F32), pltpu.VMEM(t0.shape, F32),
            pltpu.VMEM((N_CH, 2, tokens, cw), F32), pltpu.VMEM((N_CH, tokens, cw), F32), pltpu.VMEM((N_CH, tokens, cw), F32),
            pltpu.VMEM((tokens, 2 * half_cols), BF16), pltpu.VMEM((tokens, half_cols), BF16),
            dma((N_CH,)), dma((N_CH,)), dma((N_CH, 2)), dma((N_CH, 2)), dma((N_CH,)), dma((N_CH,)), dma((N_CH,)), dma((N_CH,)), dma,
        ],
        compiler_params=pltpu.CompilerParams(collective_id=2 + layer, has_side_effects=True, vmem_limit_bytes=32 << 20),
    )(own1, got1, own2, send2, gm, t0, a, a_got)


def solution(mesh):
    tok_spec = P(("dp", "ep"), None)
    cache_spec = P(None, ("dp", "ep"), "pool", None, None)
    up_spec = P(None, "ep", None, "pool")
    down_spec = P(None, "ep", "pool", None)
    in_specs = (tok_spec, cache_spec, cache_spec, P(("dp", "ep")), P(), P(), P(), P(), P(), P(None, ("dp", "ep"), None), up_spec, up_spec, down_spec)

    def body(hidden, kc, vc, lens, wq, wk, wv, wo, wr, ids, w1, w3, w2):
        layers, tokens, seq, heads, dim = kc.shape
        n_local = w1.shape[1]
        top_k = ids.shape[2]
        kc = kc.reshape(layers, tokens, seq * heads, dim)
        vc = vc.reshape(layers, tokens, seq * heads, dim)
        w1 = jnp.swapaxes(w1, 2, 3)
        w3 = jnp.swapaxes(w3, 2, 3)
        wr = jnp.swapaxes(wr, 1, 2)
        ids = jnp.pad(jnp.swapaxes(ids, 1, 2), ((0, 0), (0, 8 - top_k), (0, 0)))
        for layer in range(layers):
            first = layer == 0
            u, a, a_got, *tables = attention(layer, hidden, lens, kc, vc, wq, wk, wv, wo, ids if first else None, n_local)
            if first:
                pos, ids_all, off = tables
            own, got = [], []
            for part in range(PARTS):
                kept, send = experts(layer, part, off, u, pos, w1, w3, w2, PART_ROWS[part])
                own.append(kept)
                if part < PARTS - 1:
                    got.append(lax.ppermute(send, "pool", [(0, 1), (1, 0)]))
            gm, t0 = gates(layer, own[0], got[0], u, wr, ids_all, pos)
            hidden = combine(layer, own[1], got[1], own[2], send, gm, t0, a, a_got)
        return hidden

    return jax.shard_map(body, mesh=mesh, in_specs=in_specs, out_specs=tok_spec, check_vma=False)
```

```python
import functools

import jax
import jax.numpy as jnp
from jax import lax
from jax.experimental import pallas as pl
from jax.experimental.pallas import tpu as pltpu
from jax.sharding import PartitionSpec as P


MESH = pl.DeviceIdType.MESH
F32 = jnp.float32
BF16 = jnp.bfloat16
I32 = jnp.int32
EPS = 1e-6
NEG = -1e30
TB = 8
SLOTS = 4
TILE_M = 128
PART_ROWS = (256, 384, 128)
PARTS = len(PART_ROWS)
DEPTH = 4
VMEM_MIB = 51
AHEAD = 12


def _nn(a, b):
    return lax.dot_general(a, b, (((1,), (0,)), ((), ())), preferred_element_type=F32)


def _nt(a, b, precision=None):
    return lax.dot_general(a, b, (((1,), (1,)), ((), ())), preferred_element_type=F32, precision=precision)


def _rms(v):
    return v * lax.rsqrt(jnp.mean(v * v, axis=-1, keepdims=True) + EPS)


def _where_am_i():
    p = lax.axis_index("pool")
    b = lax.axis_index("ep")
    x, c = b // 2, b % 2
    to_y = {"pool": 1 - p}
    to_x = {"ep": (1 - x) * 2 + c}
    to_c = {"ep": x * 2 + (1 - c)}
    return p, b, x, c, to_y, to_x, to_c


def _greet(peers):
    sem = pltpu.get_barrier_semaphore()
    for peer in peers:
        pl.semaphore_signal(sem, inc=1, device_id=peer, device_id_type=MESH)
    pl.semaphore_wait(sem, len(peers))


def _rcopy(src, dst, send, recv, peer):
    return pltpu.make_async_remote_copy(src_ref=src, dst_ref=dst, send_sem=send, recv_sem=recv, device_id=peer, device_id_type=MESH)


def _route(b, idg, pos_out, ids_out, off_out):
    n_local, top_k = off_out.shape[1], 6
    n_tok = pos_out.shape[2]
    er = lax.broadcasted_iota(I32, (n_local, n_tok), 0)
    tri = (lax.broadcasted_iota(I32, (n_tok, n_tok), 0) <= lax.broadcasted_iota(I32, (n_tok, n_tok), 1)).astype(F32).astype(BF16)
    before = (lax.broadcasted_iota(I32, (n_local, n_local), 0) > lax.broadcasted_iota(I32, (n_local, n_local), 1)).astype(F32).astype(BF16)
    row = lax.broadcasted_iota(I32, (8, n_tok), 0)
    for layer in range(pos_out.shape[0]):
        ids = jnp.concatenate([idg[i, layer] for i in range(idg.shape[0])], axis=1)
        local = ids - b * n_local
        member = jnp.zeros((n_local, n_tok), F32)
        for k in range(top_k):
            member = member + jnp.where(er == local[k:k + 1, :], 1.0, 0.0)
        member = member.astype(BF16)
        cum = _nn(member, tri)
        first = jnp.sum(_nn(before, member), axis=1, keepdims=True)
        place = first + cum - 1.0
        pos = jnp.full((8, n_tok), -1.0, F32)
        for k in range(top_k):
            lk = local[k:k + 1, :]
            at = jnp.sum(jnp.where(er == lk, place, 0.0), axis=0, keepdims=True)
            at = jnp.where((lk >= 0) & (lk < n_local), at, -1.0)
            pos = jnp.where(row == k, at, pos)
        pos_out[layer] = pos.astype(I32)
        ids_out[layer] = ids
        off_out[layer] = jnp.broadcast_to(first, (n_local, 128)).astype(I32)


def attn_kernel(layer, routed, x_ref, len_ref, k_hbm, v_hbm, wq_hbm, wk_hbm, wv_hbm, wo_hbm, *refs):
    for _ in attn_steps(layer, routed, True, x_ref, len_ref, k_hbm, v_hbm, wq_hbm, wk_hbm, wv_hbm, wo_hbm, *refs):
        pass


def attn_steps(layer, routed, alone, x_ref, len_ref, k_hbm, v_hbm, wq_hbm, wk_hbm, wv_hbm, wo_hbm, *refs):
    if routed:
        ids_ref, *refs = refs
    u_all, a_out, a_recv, *refs = refs
    if routed:
        pos_out, ids_out, off_out, *refs, idg, isend, irecv = refs
    (kbuf, vbuf, pbuf, wq, wk, wv, wo, q3, o3, o3r, k3, v3, mls, mlr, o2, a_own,
     ksem, vsem, wsem, osend, orecv, gsend, grecv) = refs
    p, b, x, c, to_y, to_x, to_c = _where_am_i()
    half = x_ref.shape[0] // 2
    heads, dim = q3.shape[1], q3.shape[2]
    slots, rows = kbuf.shape[0], kbuf.shape[2]
    n_half = half // TB
    n_blocks = 2 * n_half
    scale = dim ** -0.5

    def tok_of(n):
        return ((1 - p) + (n // n_half) * (2 * p - 1)) * half + (n % n_half) * TB

    def kv_copies(n):
        slot = n % slots
        src = pl.ds(tok_of(n), TB)
        return (pltpu.make_async_copy(k_hbm.at[layer, src], kbuf.at[slot], ksem.at[slot]),
                pltpu.make_async_copy(v_hbm.at[layer, src], vbuf.at[slot], vsem.at[slot]))

    w_copies = [pltpu.make_async_copy(src.at[layer], dst, wsem.at[i])
                for i, (src, dst) in enumerate(((wq_hbm, wq), (wk_hbm, wk), (wv_hbm, wv), (wo_hbm, wo)))]
    w_copies[0].start()
    for n in range(slots):
        for cp in kv_copies(n):
            cp.start()
    for cp in w_copies[1:]:
        cp.start()

    yield

    if routed:
        to_d = {"ep": (1 - x) * 2 + (1 - c)}
        _greet((to_y, to_x, to_c, to_d))
        idg[b] = ids_ref[...]
        id_copies = [_rcopy(ids_ref, idg.at[b], isend.at[i], irecv.at[i], peer) for i, peer in enumerate((to_x, to_c, to_d))]
        for cp in id_copies:
            cp.start()
    elif alone:
        _greet((to_y, to_x, to_c))

    normed = _rms(x_ref[...].astype(F32)).astype(BF16)
    w_copies[0].wait()
    for h in range(0, heads, 2):
        part = _nn(normed, wq[:, h * dim:(h + 2) * dim]).astype(BF16).astype(F32)
        q3[:, h, :] = part[:, :dim]
        q3[:, h + 1, :] = part[:, dim:]

    row_i = lax.broadcasted_iota(I32, (heads, rows), 0)
    lane_i = lax.broadcasted_iota(I32, (heads, rows), 1)
    posl = jnp.where(lane_i % heads == row_i, lane_i // heads + p * (rows // heads), 1 << 20)
    lane = lax.broadcasted_iota(I32, (heads, 128), 1)

    def block(n, acc):
        slot = n % slots
        for cp in kv_copies(n):
            cp.wait()
        t0 = tok_of(n)

        def scores(_, acc):
            for j in range(TB):
                q = q3[t0 + j].astype(BF16)
                s = _nt(q, kbuf[slot, j])
                s = jnp.where(posl < len_ref[t0 + j], s * scale, NEG)
                m = jnp.max(s, axis=1, keepdims=True)
                pr = jnp.exp(s - m)
                l = jnp.sum(pr, axis=1, keepdims=True)
                pbuf[j] = pr.astype(BF16)
                at = (n % n_half) * TB + j
                acc = jnp.where(lane == at, m, acc)
                acc = jnp.where(lane == half + at, l, acc)
            return acc

        def values(_, none):
            for j in range(TB):
                o3[t0 + j] = _nn(pbuf[j], vbuf[slot, j])
            return none

        acc = lax.fori_loop(0, 1, scores, acc)
        lax.fori_loop(0, 1, values, 0)

        @pl.when(n + slots < n_blocks)
        def _():
            for cp in kv_copies(n + slots):
                cp.start()

        return acc

    theirs = (1 - p) * half
    mine = p * half

    def o_copy(i):
        return _rcopy(o3.at[pl.ds(theirs + i * TB, TB)], o3r.at[pl.ds(i * TB, TB)], osend.at[i], orecv.at[i], to_y)

    def first(n, acc):
        acc = block(n, acc)
        o_copy(n).start()
        return acc

    zero = jnp.zeros((heads, 128), F32)
    mls[...] = lax.fori_loop(0, n_half, first, zero)
    ml_copy = _rcopy(mls, mlr, osend.at[n_half], orecv.at[n_half], to_y)
    ml_copy.start()
    normed = _rms(x_ref[pl.ds(mine, half), :].astype(F32)).astype(BF16)
    for i, (w, dst) in enumerate(((wk, k3), (wv, v3))):
        w_copies[1 + i].wait()
        for h in range(0, heads, 2):
            part = _nn(normed, w[:, h * dim:(h + 2) * dim]).astype(BF16).astype(F32)
            dst[:, h, :] = part[:, :dim]
            dst[:, h + 1, :] = part[:, dim:]

    sn = zero
    for j in range(half):
        sn = jnp.where(lane == j, jnp.sum(q3[mine + j] * k3[j], axis=1, keepdims=True) * scale, sn)

    if routed:
        for cp in id_copies:
            cp.wait()
        _route(b, idg, pos_out, ids_out, off_out)

    ml_own = lax.fori_loop(n_half, n_blocks, block, zero)

    for i in range(n_half):
        o_copy(i).wait()
    ml_copy.wait()
    ml_their = mlr[...]
    top = jnp.maximum(jnp.maximum(ml_own, ml_their), sn)
    w_own, w_their, w_new = jnp.exp(ml_own - top), jnp.exp(ml_their - top), jnp.exp(sn - top)
    den = pltpu.roll(ml_own, half, 1) * w_own + pltpu.roll(ml_their, half, 1) * w_their + w_new
    w_own, w_their, w_new = w_own / den, w_their / den, w_new / den
    for j in range(half):
        o3r[j] = (o3[mine + j] * w_own[:, j:j + 1] + o3r[j] * w_their[:, j:j + 1] + v3[j] * w_new[:, j:j + 1])
    for h in range(heads):
        o2[:, h * dim:(h + 1) * dim] = o3r[:, h, :].astype(BF16)
    w_copies[3].wait()
    d_model = x_ref.shape[1]
    a = (x_ref[pl.ds(mine, half), :].astype(F32) + _nn(o2[...], wo[...])).astype(BF16)
    a_own[...] = a
    me = b * 2 + p
    u_all[me] = _rms(a.astype(F32)).astype(BF16)

    y_blk, x_blk = b * 2 + (1 - p), ((1 - x) * 2 + c) * 2 + p
    d_blk = ((1 - x) * 2 + c) * 2 + (1 - p)
    lo, hi = pl.ds(0, half // 2), pl.ds(half // 2, half // 2)

    def u_copy(i, src, peer, part=None):
        ref = u_all.at[src] if part is None else u_all.at[src, part]
        return _rcopy(ref, ref, gsend.at[i], grecv.at[i], peer)

    own_y = [u_copy(0, me, to_y, lo), u_copy(1, me, to_y, hi)]
    own_x = [u_copy(2, me, to_x, hi), u_copy(3, me, to_x, lo)]
    own_c = u_copy(4, me, to_c)
    for cp in (own_y[0], own_x[0], own_y[1], own_x[1], own_c):
        cp.start()
    cw = d_model // 2
    a_out[...] = a_own[:, pl.ds(pl.multiple_of(p * cw, 128), cw)]
    a_copy = _rcopy(a_own.at[:, pl.ds(pl.multiple_of((1 - p) * cw, 128), cw)], a_recv, gsend.at[10], grecv.at[10], to_y)
    own_y[0].wait_recv()
    fwd_x = u_copy(5, y_blk, to_x, lo)
    fwd_x.start()
    own_x[0].wait_recv()
    fwd_y = u_copy(6, x_blk, to_y, hi)
    fwd_y.start()
    a_copy.start()
    own_y[1].wait_recv()
    c_y = u_copy(7, y_blk, to_c)
    c_y.start()
    own_x[1].wait_recv()
    c_x = u_copy(8, x_blk, to_c)
    c_x.start()
    fwd_x.wait_recv()
    fwd_y.wait_recv()
    c_d = u_copy(9, d_blk, to_c)
    c_d.start()
    for cp in (own_c, c_y, c_x, c_d, a_copy):
        cp.wait_recv()
    for cp in (*own_y, *own_x, own_c, fwd_x, c_y, fwd_y, c_x, c_d, a_copy):
        cp.wait_send()


def attn_scratch(slots, tokens, rows, dim, wq):
    d_model, heads, half = wq.shape[1], wq.shape[2] // dim, tokens // 2
    dma = pltpu.SemaphoreType.DMA
    weight = pltpu.VMEM(wq.shape[1:], BF16)
    return [
        pltpu.VMEM((slots, TB, rows, dim), BF16), pltpu.VMEM((slots, TB, rows, dim), BF16), pltpu.VMEM((TB, heads, rows), BF16),
        weight, weight, weight, weight,
        pltpu.VMEM((tokens, heads, dim), F32), pltpu.VMEM((tokens, heads, dim), F32), pltpu.VMEM((half, heads, dim), F32),
        pltpu.VMEM((half, heads, dim), F32), pltpu.VMEM((half, heads, dim), F32),
        pltpu.VMEM((heads, 128), F32), pltpu.VMEM((heads, 128), F32), pltpu.VMEM((half, heads * dim), BF16),
        pltpu.VMEM((half, d_model), BF16),
        dma((slots,)), dma((slots,)), dma((4,)), dma((half // TB + 1,)), dma((half // TB + 1,)), dma((11,)), dma((11,)),
    ]


def attention(layer, x, lens, kc, vc, wq, wk, wv, wo, ids, n_local):
    tokens, d_model = x.shape
    rows, dim = kc.shape[2], kc.shape[3]
    half = tokens // 2
    hbm = pl.BlockSpec(memory_space=pltpu.HBM)
    vmem = pl.BlockSpec(memory_space=pltpu.VMEM)
    dma = pltpu.SemaphoreType.DMA
    scratch = attn_scratch(SLOTS, tokens, rows, dim, wq)
    out_shape = [jax.ShapeDtypeStruct((8, half, d_model), BF16)] + [jax.ShapeDtypeStruct((half, d_model // 2), BF16)] * 2
    in_specs = [vmem, pl.BlockSpec(memory_space=pltpu.SMEM)] + [hbm] * 6
    out_specs = [vmem] * 3
    args = [x, lens, kc, vc, wq, wk, wv, wo]
    layers = ids.shape[0]
    args.append(ids)
    in_specs.append(vmem)
    out_shape += [jax.ShapeDtypeStruct((layers, 8, 8 * half), I32)] * 2 + [jax.ShapeDtypeStruct((layers, n_local, 128), I32)]
    out_specs += [vmem] * 3
    scratch += [pltpu.VMEM((4,) + ids.shape, I32), dma((3,)), dma((3,))]
    u, a, a_got, *rest = pl.pallas_call(
        functools.partial(attn_kernel, layer, True),
        out_shape=out_shape, in_specs=in_specs, out_specs=out_specs, scratch_shapes=scratch,
        compiler_params=pltpu.CompilerParams(collective_id=layer, has_side_effects=True, vmem_limit_bytes=VMEM_MIB << 20),
    )(*args)
    return (u.reshape(8 * half, d_model), a, a_got, *rest)


def expert_kernel(layer, part, off_ref, u_ref, pos_ref, w1_hbm, w3_hbm, w2_hbm, own_ref, send_ref,
                  xt, act, w1, w3, w2, t_exp, t_at, t_new, t_lo, t_hi, live, sem):
    n_tok = u_ref.shape[0]
    n_local = w1.shape[0]
    n_rows, cw = own_ref.shape
    p = lax.axis_index("pool")
    start = sum(PART_ROWS[:part])
    weights = ((w1_hbm, w1), (w3_hbm, w3), (w2_hbm, w2))

    def copies(e):
        return [pltpu.make_async_copy(src.at[layer, e], dst.at[e], sem.at[i, e]) for i, (src, dst) in enumerate(weights)]

    def plan(e, state):
        t, n = state
        end = jnp.where(e + 1 < n_local, off_ref[layer, jnp.minimum(e + 1, n_local - 1), 0], start + n_rows)
        lo = jnp.maximum(off_ref[layer, e, 0] - start, 0)
        hi = jnp.minimum(end - start, n_rows)
        base = lo // 16 * 16
        live[n] = e

        def put(i, t):
            t_exp[t] = e
            t_at[t] = jnp.minimum(base + i * TILE_M, n_rows - TILE_M)
            t_new[t] = jnp.where(i == 0, n + 1, 0)
            t_lo[t] = lo
            t_hi[t] = hi
            return t + 1

        some = lo < hi

        @pl.when(some & (n < DEPTH))
        def _():
            for cp in copies(e):
                cp.start()

        return lax.fori_loop(0, jnp.where(some, pl.cdiv(hi - base, TILE_M), 0), put, t), jnp.where(some, n + 1, n)

    tiles, n_live = lax.fori_loop(0, n_local, plan, (0, 0))
    t_new[tiles] = 0

    def start_nth(i):
        @pl.when(i < n_live)
        def _():
            for cp in copies(live[i]):
                cp.start()

    step = 128
    for r in range(n_rows // step):
        rid = lax.broadcasted_iota(I32, (step, n_tok), 0) + (r * step + start)
        hit = rid == pos_ref[layer, 0:1, :]
        for k in range(1, 6):
            hit = hit | (rid == pos_ref[layer, k:k + 1, :])
        rows = _nn(jnp.where(hit, 1.0, 0.0).astype(BF16), u_ref[...])
        xt[:, r * step:(r + 1) * step] = jnp.transpose(rows).astype(BF16)
    xt[:, n_rows:] = jnp.zeros((xt.shape[0], xt.shape[1] - n_rows), BF16)

    def arrive(k):
        @pl.when(t_new[k] > 0)
        def _():
            for cp in copies(t_exp[k]):
                cp.wait()
            start_nth(t_new[k] - 1 + DEPTH)

    def up(k):
        e, at = t_exp[k], t_at[k]
        cols = xt[:, pl.ds(pl.multiple_of(at // 128 * 128, 128), 2 * TILE_M)]
        h1 = _nn(w1[e], cols)
        h3 = _nn(w3[e], cols)
        return jnp.transpose(h1 * jax.nn.sigmoid(h1) * h3).astype(BF16)

    def down(k):
        at = pl.multiple_of(t_at[k], 16)
        rows = act[k % 2, pl.ds(pl.multiple_of(t_at[k] % 128, 16), TILE_M), :]
        rid = lax.broadcasted_iota(I32, (TILE_M, cw), 0) + at
        mask = (rid >= t_lo[k]) & (rid < t_hi[k])
        for ref, q in ((own_ref, p), (send_ref, 1 - p)):
            y = _nn(rows, w2[t_exp[k], :, pl.ds(pl.multiple_of(q * cw, 128), cw)])
            ref[pl.ds(at, TILE_M), :] = jnp.where(mask, y, ref[pl.ds(at, TILE_M), :])

    arrive(0)
    arrive(1)
    act[0] = up(0)

    def both(k, none):
        arrive(k + 1)
        act[k % 2] = up(k)
        down(k - 1)
        return none

    lax.fori_loop(1, tiles, both, 0)
    down(tiles - 1)


def experts(layer, part, off, u, pos_t, w1, w3, w2, n_rows):
    n_local, width, d_model = w1.shape[1:]
    hbm = pl.BlockSpec(memory_space=pl.ANY)
    vmem = pl.BlockSpec(memory_space=pltpu.VMEM)
    weights = pltpu.VMEM((n_local, width, d_model), BF16)
    table = pltpu.SMEM((64,), I32)
    return pl.pallas_call(
        functools.partial(expert_kernel, layer, part),
        out_shape=[jax.ShapeDtypeStruct((n_rows, d_model // 2), F32)] * 2,
        in_specs=[pl.BlockSpec(memory_space=pltpu.SMEM), vmem, vmem, hbm, hbm, hbm],
        out_specs=[vmem, vmem],
        scratch_shapes=[pltpu.VMEM((d_model, n_rows + 2 * TILE_M), BF16), pltpu.VMEM((2, 2 * TILE_M, width), BF16),
                        weights, weights, weights,
                        table, table, table, table, table, table, pltpu.SemaphoreType.DMA((3, n_local))],
        compiler_params=pltpu.CompilerParams(vmem_limit_bytes=45 << 20),
        cost_estimate=pl.CostEstimate(flops=int(4e9), bytes_accessed=18 << 20, transcendentals=0),
    )(off, u, pos_t, w1, w3, w2)


N_CH = 4


def _gated(gm, rows, ys):
    return _nn(gm[0, :, rows], ys) + (_nn(gm[1, :, rows], ys) + _nn(gm[2, :, rows], ys))


def gate_kernel(layer, own_ref, got_ref, u_ref, wr_ref, ids_ref, pos_ref, gm, t0):
    n_rows, n_tok, top_k = gm.shape[2], gm.shape[1], 6
    step = 128
    n_exp = wr_ref.shape[1]
    wr = wr_ref[layer]
    wr1 = wr.astype(BF16)
    wr2 = (wr - wr1.astype(F32)).astype(BF16)
    wr3 = (wr - wr1.astype(F32) - wr2.astype(F32)).astype(BF16)

    def gates(i, carry):
        at = pl.ds(pl.multiple_of(i * step, step), step)
        rows = u_ref[at, :]
        logits = _nt(rows, wr1) + (_nt(rows, wr2) + _nt(rows, wr3))
        lane = lax.broadcasted_iota(I32, (step, n_exp), 1)
        ids = jnp.transpose(ids_ref[layer, :, at].astype(F32)).astype(I32)
        pos = jnp.transpose(pos_ref[layer, :, at].astype(F32)).astype(I32)
        g = [jnp.sum(jnp.where(lane == ids[:, k:k + 1], logits, 0.0), axis=1, keepdims=True) for k in range(top_k)]
        top = functools.reduce(jnp.maximum, g)
        g = [jnp.exp(v - top) for v in g]
        den = functools.reduce(jnp.add, g)
        g = [v / den for v in g]
        rid = lax.broadcasted_iota(I32, (step, n_rows), 1)
        mat = jnp.zeros((step, n_rows), F32)
        for k in range(top_k):
            mat = jnp.where(rid == pos[:, k:k + 1], g[k], mat)
        g1 = mat.astype(BF16)
        rest = mat - g1.astype(F32)
        g2 = rest.astype(BF16)
        gm[0, at, :] = g1
        gm[1, at, :] = g2
        gm[2, at, :] = (rest - g2.astype(F32)).astype(BF16)
        return carry

    lax.fori_loop(0, n_tok // step, gates, 0)

    part_rows, cols = own_ref.shape
    total = _gated(gm, pl.ds(0, part_rows), (own_ref[...] + got_ref[...]).astype(BF16))
    cw = cols // N_CH
    for j in range(N_CH):
        t0[j] = total[:, j * cw:(j + 1) * cw].reshape(t0.shape[1:])


def gates(layer, own, got, u, wr, ids, pos):
    n_tok = u.shape[0]
    tokens = n_tok // 4
    vmem = pl.BlockSpec(memory_space=pltpu.VMEM)
    return pl.pallas_call(
        functools.partial(gate_kernel, layer),
        out_shape=[jax.ShapeDtypeStruct((3, n_tok, sum(PART_ROWS)), BF16),
                   jax.ShapeDtypeStruct((N_CH, 4, tokens, own.shape[1] // N_CH), F32)],
        in_specs=[vmem] * 6, out_specs=[vmem] * 2,
        compiler_params=pltpu.CompilerParams(vmem_limit_bytes=20 << 20),
        cost_estimate=pl.CostEstimate(flops=int(2e9), bytes_accessed=4 << 20, transcendentals=0),
    )(own, got, u, wr, ids, pos)


def combine_kernel(*refs):
    _combine(refs[:8], refs[8], refs[9:])


def next_layer_kernel(layer, *refs):
    inputs, operands, outs, scratch = refs[:8], refs[8:15], refs[15:18], refs[18:]
    shared, mixing, attending = scratch[0], scratch[1:15], scratch[15:]
    steps = attn_steps(layer, False, False, shared, *operands, *outs, *attending)
    next(steps)
    _combine(inputs, shared, mixing)
    for _ in steps:
        pass


def _combine(inputs, xo, scratch):
    own1_ref, got1_ref, own2_ref, send2_ref, gm, t0_ref, a_ref, a_got_ref = inputs
    yr, tb, tcr, txs, txr, a_buf, ysend, yrecv, csend, crecv, xsend, xrecv, fsend, frecv = scratch
    p, _, x, c, to_y, to_x, to_c = _where_am_i()
    cw = yr.shape[2]
    mine = p * N_CH
    _greet((to_y, to_x, to_c))

    def cols(i):
        return pl.ds(pl.multiple_of(i * cw, 128), cw)

    y_copies = [_rcopy(send2_ref.at[:, j * cw:(j + 1) * cw], yr.at[j], ysend.at[j], yrecv.at[j], to_y) for j in range(N_CH)]
    for cp in y_copies:
        cp.start()

    half = a_ref.shape[0]
    a_buf[pl.ds(pl.multiple_of(p * half, half), half), :] = a_ref[...]
    a_buf[pl.ds(pl.multiple_of((1 - p) * half, half), half), :] = a_got_ref[...]
    second, third = pl.ds(PART_ROWS[0], PART_ROWS[1]), pl.ds(PART_ROWS[0] + PART_ROWS[1], PART_ROWS[2])
    total = _gated(gm, second, (own1_ref[...] + got1_ref[...]).astype(BF16))
    for j in range(N_CH):
        tb[j] = t0_ref[j] + total[:, j * cw:(j + 1) * cw].reshape(tb.shape[1:])

    chunks = []

    def gather(j):
        y_copies[j].wait_recv()
        ys = (own2_ref[:, j * cw:(j + 1) * cw] + yr[j]).astype(BF16)
        tb[j] = tb[j] + _gated(gm, third, ys).reshape(tb.shape[1:])
        c_copies = [_rcopy(tb.at[j, i * 2 + (1 - c)], tcr.at[j, i], csend.at[j, i], crecv.at[j, i], to_c) for i in range(2)]
        for cp in c_copies:
            cp.start()
        chunks.append(c_copies)

    def cross(j):
        for cp in chunks[j]:
            cp.wait_recv()
        txs[j] = tb[j, (1 - x) * 2 + c] + tcr[j, 1 - x]
        x_copy = _rcopy(txs.at[j], txr.at[j], xsend.at[j], xrecv.at[j], to_x)
        x_copy.start()
        chunks[j].append(x_copy)

    def finish(j):
        chunks[j][-1].wait_recv()
        own = tb[j, x * 2 + c] + tcr[j, x]
        new = (a_buf[:, j * cw:(j + 1) * cw].astype(F32) + (own + txr[j])).astype(BF16)
        xo[:, cols(mine + j)] = new
        f_copy = _rcopy(xo.at[:, cols(mine + j)], xo.at[:, cols(mine + j)], fsend.at[j], frecv.at[j], to_y)
        f_copy.start()
        chunks[j].append(f_copy)

    for j in range(N_CH + 2):
        if j < N_CH:
            gather(j)
        if 0 <= j - 1 < N_CH:
            cross(j - 1)
        if 0 <= j - 2 < N_CH:
            finish(j - 2)
    for copies in chunks:
        copies[-1].wait_recv()
    for cp in y_copies:
        cp.wait_send()
    for copies in chunks:
        for cp in copies:
            cp.wait_send()


def combine_scratch(own2, t0, a):
    half, half_cols = a.shape
    tokens, cw = 2 * half, half_cols // N_CH
    dma = pltpu.SemaphoreType.DMA
    return [
        pltpu.VMEM((N_CH, own2.shape[0], cw), F32), pltpu.VMEM(t0.shape, F32),
        pltpu.VMEM((N_CH, 2, tokens, cw), F32), pltpu.VMEM((N_CH, tokens, cw), F32), pltpu.VMEM((N_CH, tokens, cw), F32),
        pltpu.VMEM((tokens, half_cols), BF16),
        dma((N_CH,)), dma((N_CH,)), dma((N_CH, 2)), dma((N_CH, 2)), dma((N_CH,)), dma((N_CH,)), dma((N_CH,)), dma((N_CH,)),
    ]


def combine(args):
    half, half_cols = args[6].shape
    vmem = pl.BlockSpec(memory_space=pltpu.VMEM)
    return pl.pallas_call(
        combine_kernel,
        out_shape=jax.ShapeDtypeStruct((2 * half, 2 * half_cols), BF16),
        in_specs=[vmem] * 8,
        out_specs=vmem,
        scratch_shapes=combine_scratch(args[2], args[5], args[6]),
        compiler_params=pltpu.CompilerParams(collective_id=8, has_side_effects=True, vmem_limit_bytes=32 << 20),
    )(*args)


def next_layer(layer, args, lens, kc, vc, wq, wk, wv, wo):
    half, half_cols = args[6].shape
    tokens, d_model = 2 * half, 2 * half_cols
    vmem = pl.BlockSpec(memory_space=pltpu.VMEM)
    hbm = pl.BlockSpec(memory_space=pltpu.HBM)
    u, a, a_got = pl.pallas_call(
        functools.partial(next_layer_kernel, layer),
        out_shape=[jax.ShapeDtypeStruct((8, half, d_model), BF16)] + [jax.ShapeDtypeStruct((half, half_cols), BF16)] * 2,
        in_specs=[vmem] * 8 + [pl.BlockSpec(memory_space=pltpu.SMEM)] + [hbm] * 6,
        out_specs=[vmem] * 3,
        scratch_shapes=[pltpu.VMEM((tokens, d_model), BF16)] + combine_scratch(args[2], args[5], args[6])
        + attn_scratch(AHEAD, tokens, kc.shape[2], kc.shape[3], wq),
        compiler_params=pltpu.CompilerParams(collective_id=layer, has_side_effects=True, vmem_limit_bytes=46 << 20),
    )(*args, lens, kc, vc, wq, wk, wv, wo)
    return u.reshape(8 * half, d_model), a, a_got


def solution(mesh):
    tok_spec = P(("dp", "ep"), None)
    cache_spec = P(None, ("dp", "ep"), "pool", None, None)
    up_spec = P(None, "ep", None, "pool")
    down_spec = P(None, "ep", "pool", None)
    in_specs = (tok_spec, cache_spec, cache_spec, P(("dp", "ep")), P(), P(), P(), P(), P(), P(None, ("dp", "ep"), None), up_spec, up_spec, down_spec)

    def body(hidden, kc, vc, lens, wq, wk, wv, wo, wr, ids, w1, w3, w2):
        layers, tokens, seq, heads, dim = kc.shape
        n_local = w1.shape[1]
        top_k = ids.shape[2]
        kc = kc.reshape(layers, tokens, seq * heads, dim)
        vc = vc.reshape(layers, tokens, seq * heads, dim)
        w1 = jnp.swapaxes(w1, 2, 3)
        w3 = jnp.swapaxes(w3, 2, 3)
        wr = jnp.swapaxes(wr, 1, 2)
        ids = jnp.pad(jnp.swapaxes(ids, 1, 2), ((0, 0), (0, 8 - top_k), (0, 0)))
        weights = (lens, kc, vc, wq, wk, wv, wo)
        u, a, a_got, pos, ids_all, off = attention(0, hidden, *weights, ids, n_local)
        for layer in range(layers):
            own, got = [], []
            for part in range(PARTS):
                kept, send = experts(layer, part, off, u, pos, w1, w3, w2, PART_ROWS[part])
                own.append(kept)
                if part < PARTS - 1:
                    got.append(lax.ppermute(send, "pool", [(0, 1), (1, 0)]))
            gm, t0 = gates(layer, own[0], got[0], u, wr, ids_all, pos)
            args = (own[1], got[1], own[2], send, gm, t0, a, a_got)
            if layer + 1 < layers:
                u, a, a_got = next_layer(layer + 1, args, *weights)
        return combine(args)

    return jax.shard_map(body, mesh=mesh, in_specs=in_specs, out_specs=tok_spec, check_vma=False)
```

```python
import functools

import jax
import jax.numpy as jnp
from jax import lax
from jax.experimental import pallas as pl
from jax.experimental.pallas import tpu as pltpu
from jax.sharding import PartitionSpec as P


MESH = pl.DeviceIdType.MESH
F32 = jnp.float32
BF16 = jnp.bfloat16
I32 = jnp.int32
EPS = 1e-6
NEG = -1e30
TB = 8
SLOTS = 4
TILE_M = 128
PART_ROWS = (256, 384, 128)
PARTS = len(PART_ROWS)
DEPTH = 4
VMEM_MIB = 51
AHEAD = 12


def _nn(a, b):
    return lax.dot_general(a, b, (((1,), (0,)), ((), ())), preferred_element_type=F32)


def _nt(a, b, precision=None):
    return lax.dot_general(a, b, (((1,), (1,)), ((), ())), preferred_element_type=F32, precision=precision)


def _rms(v):
    return v * lax.rsqrt(jnp.mean(v * v, axis=-1, keepdims=True) + EPS)


def _where_am_i():
    p = lax.axis_index("pool")
    b = lax.axis_index("ep")
    x, c = b // 2, b % 2
    to_y = {"pool": 1 - p}
    to_x = {"ep": (1 - x) * 2 + c}
    to_c = {"ep": x * 2 + (1 - c)}
    return p, b, x, c, to_y, to_x, to_c


def _greet(peers):
    sem = pltpu.get_barrier_semaphore()
    for peer in peers:
        pl.semaphore_signal(sem, inc=1, device_id=peer, device_id_type=MESH)
    pl.semaphore_wait(sem, len(peers))


def _rcopy(src, dst, send, recv, peer):
    return pltpu.make_async_remote_copy(src_ref=src, dst_ref=dst, send_sem=send, recv_sem=recv, device_id=peer, device_id_type=MESH)


def _route(b, idg, pos_out, ids_out, off_out):
    n_local, top_k = off_out.shape[1], 6
    n_tok = pos_out.shape[2]
    er = lax.broadcasted_iota(I32, (n_local, n_tok), 0)
    tri = (lax.broadcasted_iota(I32, (n_tok, n_tok), 0) <= lax.broadcasted_iota(I32, (n_tok, n_tok), 1)).astype(F32).astype(BF16)
    before = (lax.broadcasted_iota(I32, (n_local, n_local), 0) > lax.broadcasted_iota(I32, (n_local, n_local), 1)).astype(F32).astype(BF16)
    row = lax.broadcasted_iota(I32, (8, n_tok), 0)
    for layer in range(pos_out.shape[0]):
        ids = jnp.concatenate([idg[i, layer] for i in range(idg.shape[0])], axis=1)
        local = ids - b * n_local
        member = jnp.zeros((n_local, n_tok), F32)
        for k in range(top_k):
            member = member + jnp.where(er == local[k:k + 1, :], 1.0, 0.0)
        member = member.astype(BF16)
        cum = _nn(member, tri)
        first = jnp.sum(_nn(before, member), axis=1, keepdims=True)
        place = first + cum - 1.0
        pos = jnp.full((8, n_tok), -1.0, F32)
        for k in range(top_k):
            lk = local[k:k + 1, :]
            at = jnp.sum(jnp.where(er == lk, place, 0.0), axis=0, keepdims=True)
            at = jnp.where((lk >= 0) & (lk < n_local), at, -1.0)
            pos = jnp.where(row == k, at, pos)
        pos_out[layer] = pos.astype(I32)
        ids_out[layer] = ids
        off_out[layer] = jnp.broadcast_to(first, (n_local, 128)).astype(I32)


def attn_kernel(layer, routed, x_ref, len_ref, k_hbm, v_hbm, wq_hbm, wk_hbm, wv_hbm, wo_hbm, *refs):
    for _ in attn_steps(layer, routed, True, x_ref, len_ref, k_hbm, v_hbm, wq_hbm, wk_hbm, wv_hbm, wo_hbm, *refs):
        pass


def attn_steps(layer, routed, alone, x_ref, len_ref, k_hbm, v_hbm, wq_hbm, wk_hbm, wv_hbm, wo_hbm, *refs):
    if routed:
        ids_ref, *refs = refs
    u_all, a_out, a_recv, *refs = refs
    if routed:
        pos_out, ids_out, off_out, *refs, idg, isend, irecv = refs
    (kbuf, vbuf, pbuf, wq, wk, wv, wo, q3, o3, o3r, k3, v3, mls, mlr, o2, a_own,
     ksem, vsem, wsem, osend, orecv, gsend, grecv) = refs
    p, b, x, c, to_y, to_x, to_c = _where_am_i()
    half = x_ref.shape[0] // 2
    heads, dim = q3.shape[1], q3.shape[2]
    slots, rows = kbuf.shape[0], kbuf.shape[2]
    n_half = half // TB
    n_blocks = 2 * n_half
    scale = dim ** -0.5

    def tok_of(n):
        return ((1 - p) + (n // n_half) * (2 * p - 1)) * half + (n % n_half) * TB

    def kv_copies(n):
        slot = n % slots
        src = pl.ds(tok_of(n), TB)
        return (pltpu.make_async_copy(k_hbm.at[layer, src], kbuf.at[slot], ksem.at[slot]),
                pltpu.make_async_copy(v_hbm.at[layer, src], vbuf.at[slot], vsem.at[slot]))

    w_copies = [pltpu.make_async_copy(src.at[layer], dst, wsem.at[i])
                for i, (src, dst) in enumerate(((wq_hbm, wq), (wk_hbm, wk), (wv_hbm, wv), (wo_hbm, wo)))]
    w_copies[0].start()
    for n in range(slots):
        for cp in kv_copies(n):
            cp.start()
    for cp in w_copies[1:]:
        cp.start()

    yield

    if routed:
        to_d = {"ep": (1 - x) * 2 + (1 - c)}
        _greet((to_y, to_x, to_c, to_d))
        idg[b] = ids_ref[...]
        id_copies = [_rcopy(ids_ref, idg.at[b], isend.at[i], irecv.at[i], peer) for i, peer in enumerate((to_x, to_c, to_d))]
        for cp in id_copies:
            cp.start()
    elif alone:
        _greet((to_y, to_x, to_c))

    normed = _rms(x_ref[...].astype(F32)).astype(BF16)
    w_copies[0].wait()
    for h in range(0, heads, 2):
        part = _nn(normed, wq[:, h * dim:(h + 2) * dim]).astype(BF16).astype(F32)
        q3[:, h, :] = part[:, :dim]
        q3[:, h + 1, :] = part[:, dim:]

    row_i = lax.broadcasted_iota(I32, (heads, rows), 0)
    lane_i = lax.broadcasted_iota(I32, (heads, rows), 1)
    posl = jnp.where(lane_i % heads == row_i, lane_i // heads + p * (rows // heads), 1 << 20)
    lane = lax.broadcasted_iota(I32, (heads, 128), 1)

    group = pbuf.shape[0] // TB

    def block(i, acc):
        for g in range(group):
            for cp in kv_copies(i * group + g):
                cp.wait()

        def scores(_, acc):
            for g in range(group):
                n = i * group + g
                t0 = tok_of(n)
                for j in range(TB):
                    q = q3[t0 + j].astype(BF16)
                    s = _nt(q, kbuf[n % slots, j])
                    s = jnp.where(posl < len_ref[t0 + j], s * scale, NEG)
                    m = jnp.max(s, axis=1, keepdims=True)
                    pr = jnp.exp(s - m)
                    l = jnp.sum(pr, axis=1, keepdims=True)
                    pbuf[g * TB + j] = pr.astype(BF16)
                    at = (n % n_half) * TB + j
                    acc = jnp.where(lane == at, m, acc)
                    acc = jnp.where(lane == half + at, l, acc)
            return acc

        def values(_, none):
            for g in range(group):
                n = i * group + g
                t0 = tok_of(n)
                for j in range(TB):
                    o3[t0 + j] = _nn(pbuf[g * TB + j], vbuf[n % slots, j])
            return none

        acc = lax.fori_loop(0, 1, scores, acc)
        lax.fori_loop(0, 1, values, 0)

        for g in range(group):
            n = i * group + g

            @pl.when(n + slots < n_blocks)
            def _(n=n):
                for cp in kv_copies(n + slots):
                    cp.start()

        return acc

    theirs = (1 - p) * half
    mine = p * half

    def o_copy(i):
        return _rcopy(o3.at[pl.ds(theirs + i * TB, TB)], o3r.at[pl.ds(i * TB, TB)], osend.at[i], orecv.at[i], to_y)

    def first(i, acc):
        acc = block(i, acc)
        for g in range(group):
            o_copy(i * group + g).start()
        return acc

    zero = jnp.zeros((heads, 128), F32)
    mls[...] = lax.fori_loop(0, n_half // group, first, zero)
    ml_copy = _rcopy(mls, mlr, osend.at[n_half], orecv.at[n_half], to_y)
    ml_copy.start()
    normed = _rms(x_ref[pl.ds(mine, half), :].astype(F32)).astype(BF16)
    for i, (w, dst) in enumerate(((wk, k3), (wv, v3))):
        w_copies[1 + i].wait()
        for h in range(0, heads, 2):
            part = _nn(normed, w[:, h * dim:(h + 2) * dim]).astype(BF16).astype(F32)
            dst[:, h, :] = part[:, :dim]
            dst[:, h + 1, :] = part[:, dim:]

    sn = zero
    for j in range(half):
        sn = jnp.where(lane == j, jnp.sum(q3[mine + j] * k3[j], axis=1, keepdims=True) * scale, sn)

    if routed:
        for cp in id_copies:
            cp.wait()
        _route(b, idg, pos_out, ids_out, off_out)

    ml_own = lax.fori_loop(n_half // group, n_blocks // group, block, zero)

    for i in range(n_half):
        o_copy(i).wait()
    ml_copy.wait()
    ml_their = mlr[...]
    top = jnp.maximum(jnp.maximum(ml_own, ml_their), sn)
    w_own, w_their, w_new = jnp.exp(ml_own - top), jnp.exp(ml_their - top), jnp.exp(sn - top)
    den = pltpu.roll(ml_own, half, 1) * w_own + pltpu.roll(ml_their, half, 1) * w_their + w_new
    w_own, w_their, w_new = w_own / den, w_their / den, w_new / den
    for j in range(half):
        o3r[j] = (o3[mine + j] * w_own[:, j:j + 1] + o3r[j] * w_their[:, j:j + 1] + v3[j] * w_new[:, j:j + 1])
    for h in range(heads):
        o2[:, h * dim:(h + 1) * dim] = o3r[:, h, :].astype(BF16)
    w_copies[3].wait()
    d_model = x_ref.shape[1]
    a = (x_ref[pl.ds(mine, half), :].astype(F32) + _nn(o2[...], wo[...])).astype(BF16)
    a_own[...] = a
    me = b * 2 + p
    u_all[me] = _rms(a.astype(F32)).astype(BF16)

    y_blk, x_blk = b * 2 + (1 - p), ((1 - x) * 2 + c) * 2 + p
    d_blk = ((1 - x) * 2 + c) * 2 + (1 - p)
    lo, hi = pl.ds(0, half // 2), pl.ds(half // 2, half // 2)

    def u_copy(i, src, peer, part=None):
        ref = u_all.at[src] if part is None else u_all.at[src, part]
        return _rcopy(ref, ref, gsend.at[i], grecv.at[i], peer)

    own_y = [u_copy(0, me, to_y, lo), u_copy(1, me, to_y, hi)]
    own_x = [u_copy(2, me, to_x, hi), u_copy(3, me, to_x, lo)]
    own_c = u_copy(4, me, to_c)
    for cp in (own_y[0], own_x[0], own_y[1], own_x[1], own_c):
        cp.start()
    cw = d_model // 2
    a_out[...] = a_own[:, pl.ds(pl.multiple_of(p * cw, 128), cw)]
    a_copy = _rcopy(a_own.at[:, pl.ds(pl.multiple_of((1 - p) * cw, 128), cw)], a_recv, gsend.at[10], grecv.at[10], to_y)
    own_y[0].wait_recv()
    fwd_x = u_copy(5, y_blk, to_x, lo)
    fwd_x.start()
    own_x[0].wait_recv()
    fwd_y = u_copy(6, x_blk, to_y, hi)
    fwd_y.start()
    a_copy.start()
    own_y[1].wait_recv()
    c_y = u_copy(7, y_blk, to_c)
    c_y.start()
    own_x[1].wait_recv()
    c_x = u_copy(8, x_blk, to_c)
    c_x.start()
    fwd_x.wait_recv()
    fwd_y.wait_recv()
    c_d = u_copy(9, d_blk, to_c)
    c_d.start()
    for cp in (own_c, c_y, c_x, c_d, a_copy):
        cp.wait_recv()
    for cp in (*own_y, *own_x, own_c, fwd_x, c_y, fwd_y, c_x, c_d, a_copy):
        cp.wait_send()


def attn_scratch(slots, group, tokens, rows, dim, wq):
    d_model, heads, half = wq.shape[1], wq.shape[2] // dim, tokens // 2
    dma = pltpu.SemaphoreType.DMA
    weight = pltpu.VMEM(wq.shape[1:], BF16)
    return [
        pltpu.VMEM((slots, TB, rows, dim), BF16), pltpu.VMEM((slots, TB, rows, dim), BF16), pltpu.VMEM((group * TB, heads, rows), BF16),
        weight, weight, weight, weight,
        pltpu.VMEM((tokens, heads, dim), F32), pltpu.VMEM((tokens, heads, dim), F32), pltpu.VMEM((half, heads, dim), F32),
        pltpu.VMEM((half, heads, dim), F32), pltpu.VMEM((half, heads, dim), F32),
        pltpu.VMEM((heads, 128), F32), pltpu.VMEM((heads, 128), F32), pltpu.VMEM((half, heads * dim), BF16),
        pltpu.VMEM((half, d_model), BF16),
        dma((slots,)), dma((slots,)), dma((4,)), dma((half // TB + 1,)), dma((half // TB + 1,)), dma((11,)), dma((11,)),
    ]


def attention(layer, x, lens, kc, vc, wq, wk, wv, wo, ids, n_local):
    tokens, d_model = x.shape
    rows, dim = kc.shape[2], kc.shape[3]
    half = tokens // 2
    hbm = pl.BlockSpec(memory_space=pltpu.HBM)
    vmem = pl.BlockSpec(memory_space=pltpu.VMEM)
    dma = pltpu.SemaphoreType.DMA
    scratch = attn_scratch(SLOTS, 1, tokens, rows, dim, wq)
    out_shape = [jax.ShapeDtypeStruct((8, half, d_model), BF16)] + [jax.ShapeDtypeStruct((half, d_model // 2), BF16)] * 2
    in_specs = [vmem, pl.BlockSpec(memory_space=pltpu.SMEM)] + [hbm] * 6
    out_specs = [vmem] * 3
    args = [x, lens, kc, vc, wq, wk, wv, wo]
    layers = ids.shape[0]
    args.append(ids)
    in_specs.append(vmem)
    out_shape += [jax.ShapeDtypeStruct((layers, 8, 8 * half), I32)] * 2 + [jax.ShapeDtypeStruct((layers, n_local, 128), I32)]
    out_specs += [vmem] * 3
    scratch += [pltpu.VMEM((4,) + ids.shape, I32), dma((3,)), dma((3,))]
    u, a, a_got, *rest = pl.pallas_call(
        functools.partial(attn_kernel, layer, True),
        out_shape=out_shape, in_specs=in_specs, out_specs=out_specs, scratch_shapes=scratch,
        compiler_params=pltpu.CompilerParams(collective_id=layer, has_side_effects=True, vmem_limit_bytes=VMEM_MIB << 20),
    )(*args)
    return (u.reshape(8 * half, d_model), a, a_got, *rest)


def expert_kernel(layer, part, off_ref, u_ref, pos_ref, w1_hbm, w3_hbm, w2_hbm, own_ref, send_ref,
                  xt, act, w1, w3, w2, t_exp, t_at, t_new, t_lo, t_hi, live, sem):
    n_tok = u_ref.shape[0]
    n_local = w1.shape[0]
    n_rows, cw = own_ref.shape
    p = lax.axis_index("pool")
    start = sum(PART_ROWS[:part])
    weights = ((w1_hbm, w1), (w3_hbm, w3), (w2_hbm, w2))

    def copies(e):
        return [pltpu.make_async_copy(src.at[layer, e], dst.at[e], sem.at[i, e]) for i, (src, dst) in enumerate(weights)]

    def plan(e, state):
        t, n = state
        end = jnp.where(e + 1 < n_local, off_ref[layer, jnp.minimum(e + 1, n_local - 1), 0], start + n_rows)
        lo = jnp.maximum(off_ref[layer, e, 0] - start, 0)
        hi = jnp.minimum(end - start, n_rows)
        base = lo // 16 * 16
        live[n] = e

        def put(i, t):
            t_exp[t] = e
            t_at[t] = jnp.minimum(base + i * TILE_M, n_rows - TILE_M)
            t_new[t] = jnp.where(i == 0, n + 1, 0)
            t_lo[t] = lo
            t_hi[t] = hi
            return t + 1

        some = lo < hi

        @pl.when(some & (n < DEPTH))
        def _():
            for cp in copies(e):
                cp.start()

        return lax.fori_loop(0, jnp.where(some, pl.cdiv(hi - base, TILE_M), 0), put, t), jnp.where(some, n + 1, n)

    tiles, n_live = lax.fori_loop(0, n_local, plan, (0, 0))
    t_new[tiles] = 0

    def start_nth(i):
        @pl.when(i < n_live)
        def _():
            for cp in copies(live[i]):
                cp.start()

    step = 128
    for r in range(n_rows // step):
        rid = lax.broadcasted_iota(I32, (step, n_tok), 0) + (r * step + start)
        hit = rid == pos_ref[layer, 0:1, :]
        for k in range(1, 6):
            hit = hit | (rid == pos_ref[layer, k:k + 1, :])
        rows = _nn(jnp.where(hit, 1.0, 0.0).astype(BF16), u_ref[...])
        xt[:, r * step:(r + 1) * step] = jnp.transpose(rows).astype(BF16)
    xt[:, n_rows:] = jnp.zeros((xt.shape[0], xt.shape[1] - n_rows), BF16)

    def arrive(k):
        @pl.when(t_new[k] > 0)
        def _():
            for cp in copies(t_exp[k]):
                cp.wait()
            start_nth(t_new[k] - 1 + DEPTH)

    def up(k):
        e, at = t_exp[k], t_at[k]
        cols = xt[:, pl.ds(pl.multiple_of(at // 128 * 128, 128), 2 * TILE_M)]
        h1 = _nn(w1[e], cols)
        h3 = _nn(w3[e], cols)
        return jnp.transpose(h1 * jax.nn.sigmoid(h1) * h3).astype(BF16)

    def down(k):
        at = pl.multiple_of(t_at[k], 16)
        rows = act[k % 2, pl.ds(pl.multiple_of(t_at[k] % 128, 16), TILE_M), :]
        rid = lax.broadcasted_iota(I32, (TILE_M, cw), 0) + at
        mask = (rid >= t_lo[k]) & (rid < t_hi[k])
        for ref, q in ((own_ref, p), (send_ref, 1 - p)):
            y = _nn(rows, w2[t_exp[k], :, pl.ds(pl.multiple_of(q * cw, 128), cw)])
            ref[pl.ds(at, TILE_M), :] = jnp.where(mask, y, ref[pl.ds(at, TILE_M), :])

    arrive(0)
    arrive(1)
    act[0] = up(0)

    def both(k, none):
        arrive(k + 1)
        act[k % 2] = up(k)
        down(k - 1)
        return none

    lax.fori_loop(1, tiles, both, 0)
    down(tiles - 1)


def experts(layer, part, off, u, pos_t, w1, w3, w2, n_rows):
    n_local, width, d_model = w1.shape[1:]
    hbm = pl.BlockSpec(memory_space=pl.ANY)
    vmem = pl.BlockSpec(memory_space=pltpu.VMEM)
    weights = pltpu.VMEM((n_local, width, d_model), BF16)
    table = pltpu.SMEM((64,), I32)
    return pl.pallas_call(
        functools.partial(expert_kernel, layer, part),
        out_shape=[jax.ShapeDtypeStruct((n_rows, d_model // 2), F32)] * 2,
        in_specs=[pl.BlockSpec(memory_space=pltpu.SMEM), vmem, vmem, hbm, hbm, hbm],
        out_specs=[vmem, vmem],
        scratch_shapes=[pltpu.VMEM((d_model, n_rows + 2 * TILE_M), BF16), pltpu.VMEM((2, 2 * TILE_M, width), BF16),
                        weights, weights, weights,
                        table, table, table, table, table, table, pltpu.SemaphoreType.DMA((3, n_local))],
        compiler_params=pltpu.CompilerParams(vmem_limit_bytes=45 << 20),
        cost_estimate=pl.CostEstimate(flops=int(4e9), bytes_accessed=18 << 20, transcendentals=0),
    )(off, u, pos_t, w1, w3, w2)


N_CH = 4


def _gated(gm, rows, ys):
    return _nn(gm[0, :, rows], ys) + (_nn(gm[1, :, rows], ys) + _nn(gm[2, :, rows], ys))


def gate_kernel(layer, own_ref, got_ref, u_ref, wr_ref, ids_ref, pos_ref, gm, t0):
    n_rows, n_tok, top_k = gm.shape[2], gm.shape[1], 6
    step = 128
    n_exp = wr_ref.shape[1]
    wr = wr_ref[layer]
    wr1 = wr.astype(BF16)
    wr2 = (wr - wr1.astype(F32)).astype(BF16)
    wr3 = (wr - wr1.astype(F32) - wr2.astype(F32)).astype(BF16)

    def gates(i, carry):
        at = pl.ds(pl.multiple_of(i * step, step), step)
        rows = u_ref[at, :]
        logits = _nt(rows, wr1) + (_nt(rows, wr2) + _nt(rows, wr3))
        lane = lax.broadcasted_iota(I32, (step, n_exp), 1)
        ids = jnp.transpose(ids_ref[layer, :, at].astype(F32)).astype(I32)
        pos = jnp.transpose(pos_ref[layer, :, at].astype(F32)).astype(I32)
        g = [jnp.sum(jnp.where(lane == ids[:, k:k + 1], logits, 0.0), axis=1, keepdims=True) for k in range(top_k)]
        top = functools.reduce(jnp.maximum, g)
        g = [jnp.exp(v - top) for v in g]
        den = functools.reduce(jnp.add, g)
        g = [v / den for v in g]
        rid = lax.broadcasted_iota(I32, (step, n_rows), 1)
        mat = jnp.zeros((step, n_rows), F32)
        for k in range(top_k):
            mat = jnp.where(rid == pos[:, k:k + 1], g[k], mat)
        g1 = mat.astype(BF16)
        rest = mat - g1.astype(F32)
        g2 = rest.astype(BF16)
        gm[0, at, :] = g1
        gm[1, at, :] = g2
        gm[2, at, :] = (rest - g2.astype(F32)).astype(BF16)
        return carry

    lax.fori_loop(0, n_tok // step, gates, 0)

    part_rows, cols = own_ref.shape
    total = _gated(gm, pl.ds(0, part_rows), (own_ref[...] + got_ref[...]).astype(BF16))
    cw = cols // N_CH
    for j in range(N_CH):
        t0[j] = total[:, j * cw:(j + 1) * cw].reshape(t0.shape[1:])


def gates(layer, own, got, u, wr, ids, pos):
    n_tok = u.shape[0]
    tokens = n_tok // 4
    vmem = pl.BlockSpec(memory_space=pltpu.VMEM)
    return pl.pallas_call(
        functools.partial(gate_kernel, layer),
        out_shape=[jax.ShapeDtypeStruct((3, n_tok, sum(PART_ROWS)), BF16),
                   jax.ShapeDtypeStruct((N_CH, 4, tokens, own.shape[1] // N_CH), F32)],
        in_specs=[vmem] * 6, out_specs=[vmem] * 2,
        compiler_params=pltpu.CompilerParams(vmem_limit_bytes=20 << 20),
        cost_estimate=pl.CostEstimate(flops=int(2e9), bytes_accessed=4 << 20, transcendentals=0),
    )(own, got, u, wr, ids, pos)


def combine_kernel(*refs):
    _combine(refs[:8], refs[8], refs[9:])


def next_layer_kernel(layer, *refs):
    inputs, operands, outs, scratch = refs[:8], refs[8:15], refs[15:18], refs[18:]
    shared, mixing, attending = scratch[0], scratch[1:15], scratch[15:]
    steps = attn_steps(layer, False, False, shared, *operands, *outs, *attending)
    next(steps)
    _combine(inputs, shared, mixing)
    for _ in steps:
        pass


def _combine(inputs, xo, scratch):
    own1_ref, got1_ref, own2_ref, send2_ref, gm, t0_ref, a_ref, a_got_ref = inputs
    yr, tb, tcr, txs, txr, a_buf, ysend, yrecv, csend, crecv, xsend, xrecv, fsend, frecv = scratch
    p, _, x, c, to_y, to_x, to_c = _where_am_i()
    cw = yr.shape[2]
    mine = p * N_CH
    _greet((to_y, to_x, to_c))

    def cols(i):
        return pl.ds(pl.multiple_of(i * cw, 128), cw)

    y_copies = [_rcopy(send2_ref.at[:, j * cw:(j + 1) * cw], yr.at[j], ysend.at[j], yrecv.at[j], to_y) for j in range(N_CH)]
    for cp in y_copies:
        cp.start()

    half = a_ref.shape[0]
    a_buf[pl.ds(pl.multiple_of(p * half, half), half), :] = a_ref[...]
    a_buf[pl.ds(pl.multiple_of((1 - p) * half, half), half), :] = a_got_ref[...]
    second, third = pl.ds(PART_ROWS[0], PART_ROWS[1]), pl.ds(PART_ROWS[0] + PART_ROWS[1], PART_ROWS[2])
    total = _gated(gm, second, (own1_ref[...] + got1_ref[...]).astype(BF16))
    for j in range(N_CH):
        tb[j] = t0_ref[j] + total[:, j * cw:(j + 1) * cw].reshape(tb.shape[1:])

    chunks = []

    def gather(j):
        y_copies[j].wait_recv()
        ys = (own2_ref[:, j * cw:(j + 1) * cw] + yr[j]).astype(BF16)
        tb[j] = tb[j] + _gated(gm, third, ys).reshape(tb.shape[1:])
        c_copies = [_rcopy(tb.at[j, i * 2 + (1 - c)], tcr.at[j, i], csend.at[j, i], crecv.at[j, i], to_c) for i in range(2)]
        for cp in c_copies:
            cp.start()
        chunks.append(c_copies)

    def cross(j):
        for cp in chunks[j]:
            cp.wait_recv()
        txs[j] = tb[j, (1 - x) * 2 + c] + tcr[j, 1 - x]
        x_copy = _rcopy(txs.at[j], txr.at[j], xsend.at[j], xrecv.at[j], to_x)
        x_copy.start()
        chunks[j].append(x_copy)

    def finish(j):
        chunks[j][-1].wait_recv()
        own = tb[j, x * 2 + c] + tcr[j, x]
        new = (a_buf[:, j * cw:(j + 1) * cw].astype(F32) + (own + txr[j])).astype(BF16)
        xo[:, cols(mine + j)] = new
        f_copy = _rcopy(xo.at[:, cols(mine + j)], xo.at[:, cols(mine + j)], fsend.at[j], frecv.at[j], to_y)
        f_copy.start()
        chunks[j].append(f_copy)

    for j in range(N_CH + 2):
        if j < N_CH:
            gather(j)
        if 0 <= j - 1 < N_CH:
            cross(j - 1)
        if 0 <= j - 2 < N_CH:
            finish(j - 2)
    for copies in chunks:
        copies[-1].wait_recv()
    for cp in y_copies:
        cp.wait_send()
    for copies in chunks:
        for cp in copies:
            cp.wait_send()


def combine_scratch(own2, t0, a):
    half, half_cols = a.shape
    tokens, cw = 2 * half, half_cols // N_CH
    dma = pltpu.SemaphoreType.DMA
    return [
        pltpu.VMEM((N_CH, own2.shape[0], cw), F32), pltpu.VMEM(t0.shape, F32),
        pltpu.VMEM((N_CH, 2, tokens, cw), F32), pltpu.VMEM((N_CH, tokens, cw), F32), pltpu.VMEM((N_CH, tokens, cw), F32),
        pltpu.VMEM((tokens, half_cols), BF16),
        dma((N_CH,)), dma((N_CH,)), dma((N_CH, 2)), dma((N_CH, 2)), dma((N_CH,)), dma((N_CH,)), dma((N_CH,)), dma((N_CH,)),
    ]


def combine(args):
    half, half_cols = args[6].shape
    vmem = pl.BlockSpec(memory_space=pltpu.VMEM)
    return pl.pallas_call(
        combine_kernel,
        out_shape=jax.ShapeDtypeStruct((2 * half, 2 * half_cols), BF16),
        in_specs=[vmem] * 8,
        out_specs=vmem,
        scratch_shapes=combine_scratch(args[2], args[5], args[6]),
        compiler_params=pltpu.CompilerParams(collective_id=8, has_side_effects=True, vmem_limit_bytes=32 << 20),
    )(*args)


def next_layer(layer, args, lens, kc, vc, wq, wk, wv, wo):
    half, half_cols = args[6].shape
    tokens, d_model = 2 * half, 2 * half_cols
    vmem = pl.BlockSpec(memory_space=pltpu.VMEM)
    hbm = pl.BlockSpec(memory_space=pltpu.HBM)
    u, a, a_got = pl.pallas_call(
        functools.partial(next_layer_kernel, layer),
        out_shape=[jax.ShapeDtypeStruct((8, half, d_model), BF16)] + [jax.ShapeDtypeStruct((half, half_cols), BF16)] * 2,
        in_specs=[vmem] * 8 + [pl.BlockSpec(memory_space=pltpu.SMEM)] + [hbm] * 6,
        out_specs=[vmem] * 3,
        scratch_shapes=[pltpu.VMEM((tokens, d_model), BF16)] + combine_scratch(args[2], args[5], args[6])
        + attn_scratch(AHEAD, 2, tokens, kc.shape[2], kc.shape[3], wq),
        compiler_params=pltpu.CompilerParams(collective_id=layer, has_side_effects=True, vmem_limit_bytes=46 << 20),
    )(*args, lens, kc, vc, wq, wk, wv, wo)
    return u.reshape(8 * half, d_model), a, a_got


def solution(mesh):
    tok_spec = P(("dp", "ep"), None)
    cache_spec = P(None, ("dp", "ep"), "pool", None, None)
    up_spec = P(None, "ep", None, "pool")
    down_spec = P(None, "ep", "pool", None)
    in_specs = (tok_spec, cache_spec, cache_spec, P(("dp", "ep")), P(), P(), P(), P(), P(), P(None, ("dp", "ep"), None), up_spec, up_spec, down_spec)

    def body(hidden, kc, vc, lens, wq, wk, wv, wo, wr, ids, w1, w3, w2):
        layers, tokens, seq, heads, dim = kc.shape
        n_local = w1.shape[1]
        top_k = ids.shape[2]
        kc = kc.reshape(layers, tokens, seq * heads, dim)
        vc = vc.reshape(layers, tokens, seq * heads, dim)
        w1 = jnp.swapaxes(w1, 2, 3)
        w3 = jnp.swapaxes(w3, 2, 3)
        wr = jnp.swapaxes(wr, 1, 2)
        ids = jnp.pad(jnp.swapaxes(ids, 1, 2), ((0, 0), (0, 8 - top_k), (0, 0)))
        weights = (lens, kc, vc, wq, wk, wv, wo)
        u, a, a_got, pos, ids_all, off = attention(0, hidden, *weights, ids, n_local)
        for layer in range(layers):
            own, got = [], []
            for part in range(PARTS):
                kept, send = experts(layer, part, off, u, pos, w1, w3, w2, PART_ROWS[part])
                own.append(kept)
                if part < PARTS - 1:
                    got.append(lax.ppermute(send, "pool", [(0, 1), (1, 0)]))
            gm, t0 = gates(layer, own[0], got[0], u, wr, ids_all, pos)
            args = (own[1], got[1], own[2], send, gm, t0, a, a_got)
            if layer + 1 < layers:
                u, a, a_got = next_layer(layer + 1, args, *weights)
        return combine(args)

    return jax.shard_map(body, mesh=mesh, in_specs=in_specs, out_specs=tok_spec, check_vma=False)
```

```python
import functools

import jax
import jax.numpy as jnp
from jax import lax
from jax.experimental import pallas as pl
from jax.experimental.pallas import tpu as pltpu
from jax.sharding import PartitionSpec as P


MESH = pl.DeviceIdType.MESH
F32 = jnp.float32
BF16 = jnp.bfloat16
I32 = jnp.int32
EPS = 1e-6
NEG = -1e30
TB = 8
SLOTS = 4
TILE_M = 128
PART_ROWS = (256, 384, 128)
PARTS = len(PART_ROWS)
DEPTH = 4
VMEM_MIB = 51
AHEAD = 12


def _nn(a, b):
    return lax.dot_general(a, b, (((1,), (0,)), ((), ())), preferred_element_type=F32)


def _nt(a, b, precision=None):
    return lax.dot_general(a, b, (((1,), (1,)), ((), ())), preferred_element_type=F32, precision=precision)


def _rms(v):
    return v * lax.rsqrt(jnp.mean(v * v, axis=-1, keepdims=True) + EPS)


def _where_am_i():
    p = lax.axis_index("pool")
    b = lax.axis_index("ep")
    x, c = b // 2, b % 2
    to_y = {"pool": 1 - p}
    to_x = {"ep": (1 - x) * 2 + c}
    to_c = {"ep": x * 2 + (1 - c)}
    return p, b, x, c, to_y, to_x, to_c


def _greet(peers):
    sem = pltpu.get_barrier_semaphore()
    for peer in peers:
        pl.semaphore_signal(sem, inc=1, device_id=peer, device_id_type=MESH)
    pl.semaphore_wait(sem, len(peers))


def _rcopy(src, dst, send, recv, peer):
    return pltpu.make_async_remote_copy(src_ref=src, dst_ref=dst, send_sem=send, recv_sem=recv, device_id=peer, device_id_type=MESH)


def _route(b, idg, pos_out, ids_out, off_out):
    n_local, top_k = off_out.shape[1], 6
    n_tok = pos_out.shape[2]
    er = lax.broadcasted_iota(I32, (n_local, n_tok), 0)
    tri = (lax.broadcasted_iota(I32, (n_tok, n_tok), 0) <= lax.broadcasted_iota(I32, (n_tok, n_tok), 1)).astype(F32).astype(BF16)
    before = (lax.broadcasted_iota(I32, (n_local, n_local), 0) > lax.broadcasted_iota(I32, (n_local, n_local), 1)).astype(F32).astype(BF16)
    row = lax.broadcasted_iota(I32, (8, n_tok), 0)
    for layer in range(pos_out.shape[0]):
        ids = jnp.concatenate([idg[i, layer] for i in range(idg.shape[0])], axis=1)
        local = ids - b * n_local
        member = jnp.zeros((n_local, n_tok), F32)
        for k in range(top_k):
            member = member + jnp.where(er == local[k:k + 1, :], 1.0, 0.0)
        member = member.astype(BF16)
        cum = _nn(member, tri)
        first = jnp.sum(_nn(before, member), axis=1, keepdims=True)
        place = first + cum - 1.0
        pos = jnp.full((8, n_tok), -1.0, F32)
        for k in range(top_k):
            lk = local[k:k + 1, :]
            at = jnp.sum(jnp.where(er == lk, place, 0.0), axis=0, keepdims=True)
            at = jnp.where((lk >= 0) & (lk < n_local), at, -1.0)
            pos = jnp.where(row == k, at, pos)
        pos_out[layer] = pos.astype(I32)
        ids_out[layer] = ids
        off_out[layer] = jnp.broadcast_to(first, (n_local, 128)).astype(I32)


def attn_kernel(layer, routed, x_ref, len_ref, k_hbm, v_hbm, wq_hbm, wk_hbm, wv_hbm, wo_hbm, *refs):
    for _ in attn_steps(layer, routed, True, x_ref, len_ref, k_hbm, v_hbm, wq_hbm, wk_hbm, wv_hbm, wo_hbm, *refs):
        pass


def attn_steps(layer, routed, alone, x_ref, len_ref, k_hbm, v_hbm, wq_hbm, wk_hbm, wv_hbm, wo_hbm, *refs):
    if routed:
        ids_ref, *refs = refs
    u_all, a_out, a_recv, *refs = refs
    if routed:
        pos_out, ids_out, off_out, *refs, idg, isend, irecv = refs
    (kbuf, vbuf, pbuf, wq, wk, wv, wo, q3, o3, o3r, k3, v3, mls, mlr, o2, a_own,
     ksem, vsem, wsem, osend, orecv, gsend, grecv) = refs
    p, b, x, c, to_y, to_x, to_c = _where_am_i()
    half = x_ref.shape[0] // 2
    heads, dim = q3.shape[1], q3.shape[2]
    slots, rows = kbuf.shape[0], kbuf.shape[2]
    n_half = half // TB
    n_blocks = 2 * n_half
    scale = dim ** -0.5

    def tok_of(n):
        return ((1 - p) + (n // n_half) * (2 * p - 1)) * half + (n % n_half) * TB

    def kv_copies(n):
        slot = n % slots
        src = pl.ds(tok_of(n), TB)
        return (pltpu.make_async_copy(k_hbm.at[layer, src], kbuf.at[slot], ksem.at[slot]),
                pltpu.make_async_copy(v_hbm.at[layer, src], vbuf.at[slot], vsem.at[slot]))

    w_copies = [pltpu.make_async_copy(src.at[layer], dst, wsem.at[i])
                for i, (src, dst) in enumerate(((wq_hbm, wq), (wk_hbm, wk), (wv_hbm, wv), (wo_hbm, wo)))]
    w_copies[0].start()
    for n in range(slots):
        for cp in kv_copies(n):
            cp.start()
    for cp in w_copies[1:]:
        cp.start()

    yield

    if routed:
        to_d = {"ep": (1 - x) * 2 + (1 - c)}
        _greet((to_y, to_x, to_c, to_d))
        idg[b] = ids_ref[...]
        id_copies = [_rcopy(ids_ref, idg.at[b], isend.at[i], irecv.at[i], peer) for i, peer in enumerate((to_x, to_c, to_d))]
        for cp in id_copies:
            cp.start()
    elif alone:
        _greet((to_y, to_x, to_c))

    normed = _rms(x_ref[...].astype(F32)).astype(BF16)
    w_copies[0].wait()
    for h in range(0, heads, 2):
        part = _nn(normed, wq[:, h * dim:(h + 2) * dim]).astype(BF16).astype(F32)
        q3[:, h, :] = part[:, :dim]
        q3[:, h + 1, :] = part[:, dim:]

    row_i = lax.broadcasted_iota(I32, (heads, rows), 0)
    lane_i = lax.broadcasted_iota(I32, (heads, rows), 1)
    posl = jnp.where(lane_i % heads == row_i, lane_i // heads + p * (rows // heads), 1 << 20)
    lane = lax.broadcasted_iota(I32, (heads, 128), 1)

    group = pbuf.shape[0] // TB

    def block(i, acc):
        for g in range(group):
            for cp in kv_copies(i * group + g):
                cp.wait()

        def scores(_, acc):
            for g in range(group):
                n = i * group + g
                t0 = tok_of(n)
                for j in range(TB):
                    q = q3[t0 + j].astype(BF16)
                    s = _nt(q, kbuf[n % slots, j])
                    s = jnp.where(posl < len_ref[t0 + j], s * scale, NEG)
                    m = jnp.max(s, axis=1, keepdims=True)
                    pr = jnp.exp(s - m)
                    l = jnp.sum(pr, axis=1, keepdims=True)
                    pbuf[g * TB + j] = pr.astype(BF16)
                    at = (n % n_half) * TB + j
                    acc = jnp.where(lane == at, m, acc)
                    acc = jnp.where(lane == half + at, l, acc)
            return acc

        def values(_, none):
            for g in range(group):
                n = i * group + g
                t0 = tok_of(n)
                for j in range(TB):
                    o3[t0 + j] = _nn(pbuf[g * TB + j], vbuf[n % slots, j])
            return none

        acc = lax.fori_loop(0, 1, scores, acc)
        lax.fori_loop(0, 1, values, 0)

        for g in range(group):
            n = i * group + g

            @pl.when(n + slots < n_blocks)
            def _(n=n):
                for cp in kv_copies(n + slots):
                    cp.start()

        return acc

    theirs = (1 - p) * half
    mine = p * half

    def o_copy(i):
        return _rcopy(o3.at[pl.ds(theirs + i * TB, TB)], o3r.at[pl.ds(i * TB, TB)], osend.at[i], orecv.at[i], to_y)

    def first(i, acc):
        acc = block(i, acc)
        for g in range(group):
            o_copy(i * group + g).start()
        return acc

    zero = jnp.zeros((heads, 128), F32)
    mls[...] = lax.fori_loop(0, n_half // group, first, zero)
    ml_copy = _rcopy(mls, mlr, osend.at[n_half], orecv.at[n_half], to_y)
    ml_copy.start()
    normed = _rms(x_ref[pl.ds(mine, half), :].astype(F32)).astype(BF16)
    for i, (w, dst) in enumerate(((wk, k3), (wv, v3))):
        w_copies[1 + i].wait()
        for h in range(0, heads, 2):
            part = _nn(normed, w[:, h * dim:(h + 2) * dim]).astype(BF16).astype(F32)
            dst[:, h, :] = part[:, :dim]
            dst[:, h + 1, :] = part[:, dim:]

    sn = zero
    for j in range(half):
        sn = jnp.where(lane == j, jnp.sum(q3[mine + j] * k3[j], axis=1, keepdims=True) * scale, sn)

    if routed:
        for cp in id_copies:
            cp.wait()
        _route(b, idg, pos_out, ids_out, off_out)

    ml_own = lax.fori_loop(n_half // group, n_blocks // group, block, zero)

    for i in range(n_half):
        o_copy(i).wait()
    ml_copy.wait()
    ml_their = mlr[...]
    top = jnp.maximum(jnp.maximum(ml_own, ml_their), sn)
    w_own, w_their, w_new = jnp.exp(ml_own - top), jnp.exp(ml_their - top), jnp.exp(sn - top)
    den = pltpu.roll(ml_own, half, 1) * w_own + pltpu.roll(ml_their, half, 1) * w_their + w_new
    w_own, w_their, w_new = w_own / den, w_their / den, w_new / den
    for j in range(half):
        o3r[j] = (o3[mine + j] * w_own[:, j:j + 1] + o3r[j] * w_their[:, j:j + 1] + v3[j] * w_new[:, j:j + 1])
    for h in range(heads):
        o2[:, h * dim:(h + 1) * dim] = o3r[:, h, :].astype(BF16)
    w_copies[3].wait()
    d_model = x_ref.shape[1]
    a = (x_ref[pl.ds(mine, half), :].astype(F32) + _nn(o2[...], wo[...])).astype(BF16)
    a_own[...] = a
    me = b * 2 + p
    u_all[me] = _rms(a.astype(F32)).astype(BF16)

    y_blk, x_blk = b * 2 + (1 - p), ((1 - x) * 2 + c) * 2 + p
    d_blk = ((1 - x) * 2 + c) * 2 + (1 - p)
    lo, hi = pl.ds(0, half // 2), pl.ds(half // 2, half // 2)

    def u_copy(i, src, peer, part=None):
        ref = u_all.at[src] if part is None else u_all.at[src, part]
        return _rcopy(ref, ref, gsend.at[i], grecv.at[i], peer)

    quarter = [pl.ds(k * (half // 4), half // 4) for k in range(4)]
    own_y = [u_copy(k, me, to_y, quarter[k]) for k in range(4)]
    own_x = [u_copy(4 + k, me, to_x, quarter[k]) for k in range(4)]
    own_c = u_copy(8, me, to_c)
    for k in range(4):
        own_y[k].start()
        own_x[(k + 2) % 4].start()
    own_c.start()
    cw = d_model // 2
    a_out[...] = a_own[:, pl.ds(pl.multiple_of(p * cw, 128), cw)]
    a_copy = _rcopy(a_own.at[:, pl.ds(pl.multiple_of((1 - p) * cw, 128), cw)], a_recv, gsend.at[9], grecv.at[9], to_y)
    fwd_x = [u_copy(10 + k, y_blk, to_x, quarter[k]) for k in range(2)]
    fwd_y = [u_copy(12 + k, x_blk, to_y, quarter[2 + k]) for k in range(2)]
    for k in range(2):
        own_y[k].wait_recv()
        fwd_x[k].start()
        own_x[2 + k].wait_recv()
        fwd_y[k].start()
    a_copy.start()
    own_y[2].wait_recv()
    own_y[3].wait_recv()
    c_y = u_copy(14, y_blk, to_c)
    c_y.start()
    own_x[0].wait_recv()
    own_x[1].wait_recv()
    c_x = u_copy(15, x_blk, to_c)
    c_x.start()
    for cp in fwd_x:
        cp.wait_recv()
    c_lo = u_copy(16, d_blk, to_c, lo)
    c_lo.start()
    for cp in fwd_y:
        cp.wait_recv()
    c_hi = u_copy(17, d_blk, to_c, hi)
    c_hi.start()
    for cp in (own_c, c_y, c_x, c_lo, c_hi, a_copy):
        cp.wait_recv()
    for cp in (*own_y, *own_x, own_c, *fwd_x, c_y, *fwd_y, c_x, c_lo, c_hi, a_copy):
        cp.wait_send()


def attn_scratch(slots, group, tokens, rows, dim, wq):
    d_model, heads, half = wq.shape[1], wq.shape[2] // dim, tokens // 2
    dma = pltpu.SemaphoreType.DMA
    weight = pltpu.VMEM(wq.shape[1:], BF16)
    return [
        pltpu.VMEM((slots, TB, rows, dim), BF16), pltpu.VMEM((slots, TB, rows, dim), BF16), pltpu.VMEM((group * TB, heads, rows), BF16),
        weight, weight, weight, weight,
        pltpu.VMEM((tokens, heads, dim), F32), pltpu.VMEM((tokens, heads, dim), F32), pltpu.VMEM((half, heads, dim), F32),
        pltpu.VMEM((half, heads, dim), F32), pltpu.VMEM((half, heads, dim), F32),
        pltpu.VMEM((heads, 128), F32), pltpu.VMEM((heads, 128), F32), pltpu.VMEM((half, heads * dim), BF16),
        pltpu.VMEM((half, d_model), BF16),
        dma((slots,)), dma((slots,)), dma((4,)), dma((half // TB + 1,)), dma((half // TB + 1,)), dma((18,)), dma((18,)),
    ]


def attention(layer, x, lens, kc, vc, wq, wk, wv, wo, ids, n_local):
    tokens, d_model = x.shape
    rows, dim = kc.shape[2], kc.shape[3]
    half = tokens // 2
    hbm = pl.BlockSpec(memory_space=pltpu.HBM)
    vmem = pl.BlockSpec(memory_space=pltpu.VMEM)
    dma = pltpu.SemaphoreType.DMA
    scratch = attn_scratch(SLOTS, 1, tokens, rows, dim, wq)
    out_shape = [jax.ShapeDtypeStruct((8, half, d_model), BF16)] + [jax.ShapeDtypeStruct((half, d_model // 2), BF16)] * 2
    in_specs = [vmem, pl.BlockSpec(memory_space=pltpu.SMEM)] + [hbm] * 6
    out_specs = [vmem] * 3
    args = [x, lens, kc, vc, wq, wk, wv, wo]
    layers = ids.shape[0]
    args.append(ids)
    in_specs.append(vmem)
    out_shape += [jax.ShapeDtypeStruct((layers, 8, 8 * half), I32)] * 2 + [jax.ShapeDtypeStruct((layers, n_local, 128), I32)]
    out_specs += [vmem] * 3
    scratch += [pltpu.VMEM((4,) + ids.shape, I32), dma((3,)), dma((3,))]
    u, a, a_got, *rest = pl.pallas_call(
        functools.partial(attn_kernel, layer, True),
        out_shape=out_shape, in_specs=in_specs, out_specs=out_specs, scratch_shapes=scratch,
        compiler_params=pltpu.CompilerParams(collective_id=layer, has_side_effects=True, vmem_limit_bytes=VMEM_MIB << 20),
    )(*args)
    return (u.reshape(8 * half, d_model), a, a_got, *rest)


def expert_kernel(layer, part, off_ref, u_ref, pos_ref, w1_hbm, w3_hbm, w2_hbm, own_ref, send_ref,
                  xt, act, w1, w3, w2, t_exp, t_at, t_new, t_lo, t_hi, live, sem):
    n_tok = u_ref.shape[0]
    n_local = w1.shape[0]
    n_rows, cw = own_ref.shape
    p = lax.axis_index("pool")
    start = sum(PART_ROWS[:part])
    weights = ((w1_hbm, w1), (w3_hbm, w3), (w2_hbm, w2))

    def copies(e):
        return [pltpu.make_async_copy(src.at[layer, e], dst.at[e], sem.at[i, e]) for i, (src, dst) in enumerate(weights)]

    def plan(e, state):
        t, n = state
        end = jnp.where(e + 1 < n_local, off_ref[layer, jnp.minimum(e + 1, n_local - 1), 0], start + n_rows)
        lo = jnp.maximum(off_ref[layer, e, 0] - start, 0)
        hi = jnp.minimum(end - start, n_rows)
        base = lo // 16 * 16
        live[n] = e

        def put(i, t):
            t_exp[t] = e
            t_at[t] = jnp.minimum(base + i * TILE_M, n_rows - TILE_M)
            t_new[t] = jnp.where(i == 0, n + 1, 0)
            t_lo[t] = lo
            t_hi[t] = hi
            return t + 1

        some = lo < hi

        @pl.when(some & (n < DEPTH))
        def _():
            for cp in copies(e):
                cp.start()

        return lax.fori_loop(0, jnp.where(some, pl.cdiv(hi - base, TILE_M), 0), put, t), jnp.where(some, n + 1, n)

    tiles, n_live = lax.fori_loop(0, n_local, plan, (0, 0))
    t_new[tiles] = 0

    def start_nth(i):
        @pl.when(i < n_live)
        def _():
            for cp in copies(live[i]):
                cp.start()

    step = 128
    for r in range(n_rows // step):
        rid = lax.broadcasted_iota(I32, (step, n_tok), 0) + (r * step + start)
        hit = rid == pos_ref[layer, 0:1, :]
        for k in range(1, 6):
            hit = hit | (rid == pos_ref[layer, k:k + 1, :])
        rows = _nn(jnp.where(hit, 1.0, 0.0).astype(BF16), u_ref[...])
        xt[:, r * step:(r + 1) * step] = jnp.transpose(rows).astype(BF16)
    xt[:, n_rows:] = jnp.zeros((xt.shape[0], xt.shape[1] - n_rows), BF16)

    def arrive(k):
        @pl.when(t_new[k] > 0)
        def _():
            for cp in copies(t_exp[k]):
                cp.wait()
            start_nth(t_new[k] - 1 + DEPTH)

    def up(k):
        e, at = t_exp[k], t_at[k]
        cols = xt[:, pl.ds(pl.multiple_of(at // 128 * 128, 128), 2 * TILE_M)]
        h1 = _nn(w1[e], cols)
        h3 = _nn(w3[e], cols)
        return jnp.transpose(h1 * jax.nn.sigmoid(h1) * h3).astype(BF16)

    def down(k):
        at = pl.multiple_of(t_at[k], 16)
        rows = act[k % 2, pl.ds(pl.multiple_of(t_at[k] % 128, 16), TILE_M), :]
        rid = lax.broadcasted_iota(I32, (TILE_M, cw), 0) + at
        mask = (rid >= t_lo[k]) & (rid < t_hi[k])
        for ref, q in ((own_ref, p), (send_ref, 1 - p)):
            y = _nn(rows, w2[t_exp[k], :, pl.ds(pl.multiple_of(q * cw, 128), cw)])
            ref[pl.ds(at, TILE_M), :] = jnp.where(mask, y, ref[pl.ds(at, TILE_M), :])

    arrive(0)
    arrive(1)
    act[0] = up(0)

    def both(k, none):
        arrive(k + 1)
        act[k % 2] = up(k)
        down(k - 1)
        return none

    lax.fori_loop(1, tiles, both, 0)
    down(tiles - 1)


def experts(layer, part, off, u, pos_t, w1, w3, w2, n_rows):
    n_local, width, d_model = w1.shape[1:]
    hbm = pl.BlockSpec(memory_space=pl.ANY)
    vmem = pl.BlockSpec(memory_space=pltpu.VMEM)
    weights = pltpu.VMEM((n_local, width, d_model), BF16)
    table = pltpu.SMEM((64,), I32)
    return pl.pallas_call(
        functools.partial(expert_kernel, layer, part),
        out_shape=[jax.ShapeDtypeStruct((n_rows, d_model // 2), F32)] * 2,
        in_specs=[pl.BlockSpec(memory_space=pltpu.SMEM), vmem, vmem, hbm, hbm, hbm],
        out_specs=[vmem, vmem],
        scratch_shapes=[pltpu.VMEM((d_model, n_rows + 2 * TILE_M), BF16), pltpu.VMEM((2, 2 * TILE_M, width), BF16),
                        weights, weights, weights,
                        table, table, table, table, table, table, pltpu.SemaphoreType.DMA((3, n_local))],
        compiler_params=pltpu.CompilerParams(vmem_limit_bytes=45 << 20),
        cost_estimate=pl.CostEstimate(flops=int(4e9), bytes_accessed=18 << 20, transcendentals=0),
    )(off, u, pos_t, w1, w3, w2)


N_CH = 4


def _gated(gm, rows, ys):
    return _nn(gm[0, :, rows], ys) + (_nn(gm[1, :, rows], ys) + _nn(gm[2, :, rows], ys))


def gate_kernel(layer, own_ref, got_ref, u_ref, wr_ref, ids_ref, pos_ref, gm, t0):
    n_rows, n_tok, top_k = gm.shape[2], gm.shape[1], 6
    step = 128
    n_exp = wr_ref.shape[1]
    wr = wr_ref[layer]
    wr1 = wr.astype(BF16)
    wr2 = (wr - wr1.astype(F32)).astype(BF16)
    wr3 = (wr - wr1.astype(F32) - wr2.astype(F32)).astype(BF16)

    def gates(i, carry):
        at = pl.ds(pl.multiple_of(i * step, step), step)
        rows = u_ref[at, :]
        logits = _nt(rows, wr1) + (_nt(rows, wr2) + _nt(rows, wr3))
        lane = lax.broadcasted_iota(I32, (step, n_exp), 1)
        ids = jnp.transpose(ids_ref[layer, :, at].astype(F32)).astype(I32)
        pos = jnp.transpose(pos_ref[layer, :, at].astype(F32)).astype(I32)
        g = [jnp.sum(jnp.where(lane == ids[:, k:k + 1], logits, 0.0), axis=1, keepdims=True) for k in range(top_k)]
        top = functools.reduce(jnp.maximum, g)
        g = [jnp.exp(v - top) for v in g]
        den = functools.reduce(jnp.add, g)
        g = [v / den for v in g]
        rid = lax.broadcasted_iota(I32, (step, n_rows), 1)
        mat = jnp.zeros((step, n_rows), F32)
        for k in range(top_k):
            mat = jnp.where(rid == pos[:, k:k + 1], g[k], mat)
        g1 = mat.astype(BF16)
        rest = mat - g1.astype(F32)
        g2 = rest.astype(BF16)
        gm[0, at, :] = g1
        gm[1, at, :] = g2
        gm[2, at, :] = (rest - g2.astype(F32)).astype(BF16)
        return carry

    lax.fori_loop(0, n_tok // step, gates, 0)

    part_rows, cols = own_ref.shape
    total = _gated(gm, pl.ds(0, part_rows), (own_ref[...] + got_ref[...]).astype(BF16))
    cw = cols // N_CH
    for j in range(N_CH):
        t0[j] = total[:, j * cw:(j + 1) * cw].reshape(t0.shape[1:])


def gates(layer, own, got, u, wr, ids, pos):
    n_tok = u.shape[0]
    tokens = n_tok // 4
    vmem = pl.BlockSpec(memory_space=pltpu.VMEM)
    return pl.pallas_call(
        functools.partial(gate_kernel, layer),
        out_shape=[jax.ShapeDtypeStruct((3, n_tok, sum(PART_ROWS)), BF16),
                   jax.ShapeDtypeStruct((N_CH, 4, tokens, own.shape[1] // N_CH), F32)],
        in_specs=[vmem] * 6, out_specs=[vmem] * 2,
        compiler_params=pltpu.CompilerParams(vmem_limit_bytes=20 << 20),
        cost_estimate=pl.CostEstimate(flops=int(2e9), bytes_accessed=4 << 20, transcendentals=0),
    )(own, got, u, wr, ids, pos)


def combine_kernel(*refs):
    _combine(refs[:8], refs[8], refs[9:])


def next_layer_kernel(layer, *refs):
    inputs, operands, outs, scratch = refs[:8], refs[8:15], refs[15:18], refs[18:]
    shared, mixing, attending = scratch[0], scratch[1:15], scratch[15:]
    steps = attn_steps(layer, False, False, shared, *operands, *outs, *attending)
    next(steps)
    _combine(inputs, shared, mixing)
    for _ in steps:
        pass


def _combine(inputs, xo, scratch):
    own1_ref, got1_ref, own2_ref, send2_ref, gm, t0_ref, a_ref, a_got_ref = inputs
    yr, tb, tcr, txs, txr, a_buf, ysend, yrecv, csend, crecv, xsend, xrecv, fsend, frecv = scratch
    p, _, x, c, to_y, to_x, to_c = _where_am_i()
    cw = yr.shape[2]
    mine = p * N_CH
    _greet((to_y, to_x, to_c))

    def cols(i):
        return pl.ds(pl.multiple_of(i * cw, 128), cw)

    y_copies = [_rcopy(send2_ref.at[:, j * cw:(j + 1) * cw], yr.at[j], ysend.at[j], yrecv.at[j], to_y) for j in range(N_CH)]
    for cp in y_copies:
        cp.start()

    half = a_ref.shape[0]
    a_buf[pl.ds(pl.multiple_of(p * half, half), half), :] = a_ref[...]
    a_buf[pl.ds(pl.multiple_of((1 - p) * half, half), half), :] = a_got_ref[...]
    second, third = pl.ds(PART_ROWS[0], PART_ROWS[1]), pl.ds(PART_ROWS[0] + PART_ROWS[1], PART_ROWS[2])
    total = _gated(gm, second, (own1_ref[...] + got1_ref[...]).astype(BF16))
    for j in range(N_CH):
        tb[j] = t0_ref[j] + total[:, j * cw:(j + 1) * cw].reshape(tb.shape[1:])

    chunks = []

    def gather(j):
        y_copies[j].wait_recv()
        ys = (own2_ref[:, j * cw:(j + 1) * cw] + yr[j]).astype(BF16)
        tb[j] = tb[j] + _gated(gm, third, ys).reshape(tb.shape[1:])
        c_copies = [_rcopy(tb.at[j, i * 2 + (1 - c)], tcr.at[j, i], csend.at[j, i], crecv.at[j, i], to_c) for i in range(2)]
        for cp in c_copies:
            cp.start()
        chunks.append(c_copies)

    def cross(j):
        for cp in chunks[j]:
            cp.wait_recv()
        txs[j] = tb[j, (1 - x) * 2 + c] + tcr[j, 1 - x]
        x_copy = _rcopy(txs.at[j], txr.at[j], xsend.at[j], xrecv.at[j], to_x)
        x_copy.start()
        chunks[j].append(x_copy)

    def finish(j):
        chunks[j][-1].wait_recv()
        own = tb[j, x * 2 + c] + tcr[j, x]
        new = (a_buf[:, j * cw:(j + 1) * cw].astype(F32) + (own + txr[j])).astype(BF16)
        xo[:, cols(mine + j)] = new
        f_copy = _rcopy(xo.at[:, cols(mine + j)], xo.at[:, cols(mine + j)], fsend.at[j], frecv.at[j], to_y)
        f_copy.start()
        chunks[j].append(f_copy)

    for j in range(N_CH + 2):
        if j < N_CH:
            gather(j)
        if 0 <= j - 1 < N_CH:
            cross(j - 1)
        if 0 <= j - 2 < N_CH:
            finish(j - 2)
    for copies in chunks:
        copies[-1].wait_recv()
    for cp in y_copies:
        cp.wait_send()
    for copies in chunks:
        for cp in copies:
            cp.wait_send()


def combine_scratch(own2, t0, a):
    half, half_cols = a.shape
    tokens, cw = 2 * half, half_cols // N_CH
    dma = pltpu.SemaphoreType.DMA
    return [
        pltpu.VMEM((N_CH, own2.shape[0], cw), F32), pltpu.VMEM(t0.shape, F32),
        pltpu.VMEM((N_CH, 2, tokens, cw), F32), pltpu.VMEM((N_CH, tokens, cw), F32), pltpu.VMEM((N_CH, tokens, cw), F32),
        pltpu.VMEM((tokens, half_cols), BF16),
        dma((N_CH,)), dma((N_CH,)), dma((N_CH, 2)), dma((N_CH, 2)), dma((N_CH,)), dma((N_CH,)), dma((N_CH,)), dma((N_CH,)),
    ]


def combine(args):
    half, half_cols = args[6].shape
    vmem = pl.BlockSpec(memory_space=pltpu.VMEM)
    return pl.pallas_call(
        combine_kernel,
        out_shape=jax.ShapeDtypeStruct((2 * half, 2 * half_cols), BF16),
        in_specs=[vmem] * 8,
        out_specs=vmem,
        scratch_shapes=combine_scratch(args[2], args[5], args[6]),
        compiler_params=pltpu.CompilerParams(collective_id=8, has_side_effects=True, vmem_limit_bytes=32 << 20),
    )(*args)


def next_layer(layer, args, lens, kc, vc, wq, wk, wv, wo):
    half, half_cols = args[6].shape
    tokens, d_model = 2 * half, 2 * half_cols
    vmem = pl.BlockSpec(memory_space=pltpu.VMEM)
    hbm = pl.BlockSpec(memory_space=pltpu.HBM)
    u, a, a_got = pl.pallas_call(
        functools.partial(next_layer_kernel, layer),
        out_shape=[jax.ShapeDtypeStruct((8, half, d_model), BF16)] + [jax.ShapeDtypeStruct((half, half_cols), BF16)] * 2,
        in_specs=[vmem] * 8 + [pl.BlockSpec(memory_space=pltpu.SMEM)] + [hbm] * 6,
        out_specs=[vmem] * 3,
        scratch_shapes=[pltpu.VMEM((tokens, d_model), BF16)] + combine_scratch(args[2], args[5], args[6])
        + attn_scratch(AHEAD, 4, tokens, kc.shape[2], kc.shape[3], wq),
        compiler_params=pltpu.CompilerParams(collective_id=layer, has_side_effects=True, vmem_limit_bytes=46 << 20),
    )(*args, lens, kc, vc, wq, wk, wv, wo)
    return u.reshape(8 * half, d_model), a, a_got


def solution(mesh):
    tok_spec = P(("dp", "ep"), None)
    cache_spec = P(None, ("dp", "ep"), "pool", None, None)
    up_spec = P(None, "ep", None, "pool")
    down_spec = P(None, "ep", "pool", None)
    in_specs = (tok_spec, cache_spec, cache_spec, P(("dp", "ep")), P(), P(), P(), P(), P(), P(None, ("dp", "ep"), None), up_spec, up_spec, down_spec)

    def body(hidden, kc, vc, lens, wq, wk, wv, wo, wr, ids, w1, w3, w2):
        layers, tokens, seq, heads, dim = kc.shape
        n_local = w1.shape[1]
        top_k = ids.shape[2]
        kc = kc.reshape(layers, tokens, seq * heads, dim)
        vc = vc.reshape(layers, tokens, seq * heads, dim)
        w1 = jnp.swapaxes(w1, 2, 3)
        w3 = jnp.swapaxes(w3, 2, 3)
        wr = jnp.swapaxes(wr, 1, 2)
        ids = jnp.pad(jnp.swapaxes(ids, 1, 2), ((0, 0), (0, 8 - top_k), (0, 0)))
        weights = (lens, kc, vc, wq, wk, wv, wo)
        u, a, a_got, pos, ids_all, off = attention(0, hidden, *weights, ids, n_local)
        for layer in range(layers):
            own, got = [], []
            for part in range(PARTS):
                kept, send = experts(layer, part, off, u, pos, w1, w3, w2, PART_ROWS[part])
                own.append(kept)
                if part < PARTS - 1:
                    got.append(lax.ppermute(send, "pool", [(0, 1), (1, 0)]))
            gm, t0 = gates(layer, own[0], got[0], u, wr, ids_all, pos)
            args = (own[1], got[1], own[2], send, gm, t0, a, a_got)
            if layer + 1 < layers:
                u, a, a_got = next_layer(layer + 1, args, *weights)
        return combine(args)

    return jax.shard_map(body, mesh=mesh, in_specs=in_specs, out_specs=tok_spec, check_vma=False)
```

```python
import functools

import jax
import jax.numpy as jnp
from jax import lax
from jax.experimental import pallas as pl
from jax.experimental.pallas import tpu as pltpu
from jax.sharding import PartitionSpec as P


MESH = pl.DeviceIdType.MESH
F32 = jnp.float32
BF16 = jnp.bfloat16
I32 = jnp.int32
EPS = 1e-6
NEG = -1e30
TB = 8
SLOTS = 4
TILE_M = 128
PART_ROWS = (256, 384, 128)
PARTS = len(PART_ROWS)
DEPTH = 4
VMEM_MIB = 51
AHEAD = 12


def _nn(a, b):
    return lax.dot_general(a, b, (((1,), (0,)), ((), ())), preferred_element_type=F32)


def _nt(a, b, precision=None):
    return lax.dot_general(a, b, (((1,), (1,)), ((), ())), preferred_element_type=F32, precision=precision)


def _rms(v):
    return v * lax.rsqrt(jnp.mean(v * v, axis=-1, keepdims=True) + EPS)


def _where_am_i():
    p = lax.axis_index("pool")
    b = lax.axis_index("ep")
    x, c = b // 2, b % 2
    to_y = {"pool": 1 - p}
    to_x = {"ep": (1 - x) * 2 + c}
    to_c = {"ep": x * 2 + (1 - c)}
    return p, b, x, c, to_y, to_x, to_c


def _greet(peers):
    sem = pltpu.get_barrier_semaphore()
    for peer in peers:
        pl.semaphore_signal(sem, inc=1, device_id=peer, device_id_type=MESH)
    pl.semaphore_wait(sem, len(peers))


def _rcopy(src, dst, send, recv, peer):
    return pltpu.make_async_remote_copy(src_ref=src, dst_ref=dst, send_sem=send, recv_sem=recv, device_id=peer, device_id_type=MESH)


def _route(b, idg, pos_out, ids_out, off_out):
    n_local, top_k = off_out.shape[1], 6
    n_tok = pos_out.shape[2]
    er = lax.broadcasted_iota(I32, (n_local, n_tok), 0)
    tri = (lax.broadcasted_iota(I32, (n_tok, n_tok), 0) <= lax.broadcasted_iota(I32, (n_tok, n_tok), 1)).astype(F32).astype(BF16)
    before = (lax.broadcasted_iota(I32, (n_local, n_local), 0) > lax.broadcasted_iota(I32, (n_local, n_local), 1)).astype(F32).astype(BF16)
    row = lax.broadcasted_iota(I32, (8, n_tok), 0)
    for layer in range(pos_out.shape[0]):
        ids = jnp.concatenate([idg[i, layer] for i in range(idg.shape[0])], axis=1)
        local = ids - b * n_local
        member = jnp.zeros((n_local, n_tok), F32)
        for k in range(top_k):
            member = member + jnp.where(er == local[k:k + 1, :], 1.0, 0.0)
        member = member.astype(BF16)
        cum = _nn(member, tri)
        first = jnp.sum(_nn(before, member), axis=1, keepdims=True)
        place = first + cum - 1.0
        pos = jnp.full((8, n_tok), -1.0, F32)
        for k in range(top_k):
            lk = local[k:k + 1, :]
            at = jnp.sum(jnp.where(er == lk, place, 0.0), axis=0, keepdims=True)
            at = jnp.where((lk >= 0) & (lk < n_local), at, -1.0)
            pos = jnp.where(row == k, at, pos)
        pos_out[layer] = pos.astype(I32)
        ids_out[layer] = ids
        off_out[layer] = jnp.broadcast_to(first, (n_local, 128)).astype(I32)


def attn_kernel(layer, routed, x_ref, len_ref, k_hbm, v_hbm, wq_hbm, wk_hbm, wv_hbm, wo_hbm, *refs):
    for _ in attn_steps(layer, routed, True, x_ref, len_ref, k_hbm, v_hbm, wq_hbm, wk_hbm, wv_hbm, wo_hbm, *refs):
        pass


def attn_steps(layer, routed, alone, x_ref, len_ref, k_hbm, v_hbm, wq_hbm, wk_hbm, wv_hbm, wo_hbm, *refs):
    if routed:
        ids_ref, *refs = refs
    u_all, a_out, a_recv, *refs = refs
    if routed:
        pos_out, ids_out, off_out, *refs, idg, isend, irecv = refs
    (kbuf, vbuf, pbuf, wq, wk, wv, wo, q3, o3, o3r, k3, v3, mls, mlr, o2, a_own,
     ksem, vsem, wsem, osend, orecv, gsend, grecv) = refs
    p, b, x, c, to_y, to_x, to_c = _where_am_i()
    half = x_ref.shape[0] // 2
    heads, dim = q3.shape[1], q3.shape[2]
    slots, rows = kbuf.shape[0], kbuf.shape[2]
    n_half = half // TB
    n_blocks = 2 * n_half
    scale = dim ** -0.5

    def tok_of(n):
        return ((1 - p) + (n // n_half) * (2 * p - 1)) * half + (n % n_half) * TB

    def kv_copies(n):
        slot = n % slots
        src = pl.ds(tok_of(n), TB)
        return (pltpu.make_async_copy(k_hbm.at[layer, src], kbuf.at[slot], ksem.at[slot]),
                pltpu.make_async_copy(v_hbm.at[layer, src], vbuf.at[slot], vsem.at[slot]))

    w_copies = [pltpu.make_async_copy(src.at[layer], dst, wsem.at[i])
                for i, (src, dst) in enumerate(((wq_hbm, wq), (wk_hbm, wk), (wv_hbm, wv), (wo_hbm, wo)))]
    w_copies[0].start()
    for n in range(slots):
        for cp in kv_copies(n):
            cp.start()
    for cp in w_copies[1:]:
        cp.start()

    yield

    if routed:
        to_d = {"ep": (1 - x) * 2 + (1 - c)}
        _greet((to_y, to_x, to_c, to_d))
        idg[b] = ids_ref[...]
        id_copies = [_rcopy(ids_ref, idg.at[b], isend.at[i], irecv.at[i], peer) for i, peer in enumerate((to_x, to_c, to_d))]
        for cp in id_copies:
            cp.start()
    elif alone:
        _greet((to_y, to_x, to_c))

    normed = _rms(x_ref[...].astype(F32)).astype(BF16)
    w_copies[0].wait()
    for h in range(0, heads, 2):
        part = _nn(normed, wq[:, h * dim:(h + 2) * dim]).astype(BF16).astype(F32)
        q3[:, h, :] = part[:, :dim]
        q3[:, h + 1, :] = part[:, dim:]

    row_i = lax.broadcasted_iota(I32, (heads, rows), 0)
    lane_i = lax.broadcasted_iota(I32, (heads, rows), 1)
    posl = jnp.where(lane_i % heads == row_i, lane_i // heads + p * (rows // heads), 1 << 20)
    lane = lax.broadcasted_iota(I32, (heads, 128), 1)

    group = pbuf.shape[0] // TB

    def block(i, acc):
        for g in range(group):
            for cp in kv_copies(i * group + g):
                cp.wait()

        def scores(_, acc):
            for g in range(group):
                n = i * group + g
                t0 = tok_of(n)
                for j in range(TB):
                    q = q3[t0 + j].astype(BF16)
                    s = _nt(q, kbuf[n % slots, j])
                    seen = posl < len_ref[t0 + j]
                    s = jnp.where(seen, s * scale, NEG)
                    m = jnp.max(s, axis=1, keepdims=True)
                    pr = jnp.where(seen, jnp.exp(s - m), 0.0)
                    l = jnp.sum(pr, axis=1, keepdims=True)
                    pbuf[g * TB + j] = pr.astype(BF16)
                    at = (n % n_half) * TB + j
                    acc = jnp.where(lane == at, m, acc)
                    acc = jnp.where(lane == half + at, l, acc)
            return acc

        def values(_, none):
            for g in range(group):
                n = i * group + g
                t0 = tok_of(n)
                for j in range(TB):
                    o3[t0 + j] = _nn(pbuf[g * TB + j], vbuf[n % slots, j])
            return none

        acc = lax.fori_loop(0, 1, scores, acc)
        lax.fori_loop(0, 1, values, 0)

        for g in range(group):
            n = i * group + g

            @pl.when(n + slots < n_blocks)
            def _(n=n):
                for cp in kv_copies(n + slots):
                    cp.start()

        return acc

    theirs = (1 - p) * half
    mine = p * half

    def o_copy(i):
        return _rcopy(o3.at[pl.ds(theirs + i * TB, TB)], o3r.at[pl.ds(i * TB, TB)], osend.at[i], orecv.at[i], to_y)

    def first(i, acc):
        acc = block(i, acc)
        for g in range(group):
            o_copy(i * group + g).start()
        return acc

    zero = jnp.zeros((heads, 128), F32)
    mls[...] = lax.fori_loop(0, n_half // group, first, zero)
    ml_copy = _rcopy(mls, mlr, osend.at[n_half], orecv.at[n_half], to_y)
    ml_copy.start()
    normed = _rms(x_ref[pl.ds(mine, half), :].astype(F32)).astype(BF16)
    for i, (w, dst) in enumerate(((wk, k3), (wv, v3))):
        w_copies[1 + i].wait()
        for h in range(0, heads, 2):
            part = _nn(normed, w[:, h * dim:(h + 2) * dim]).astype(BF16).astype(F32)
            dst[:, h, :] = part[:, :dim]
            dst[:, h + 1, :] = part[:, dim:]

    sn = zero
    for j in range(half):
        sn = jnp.where(lane == j, jnp.sum(q3[mine + j] * k3[j], axis=1, keepdims=True) * scale, sn)

    if routed:
        for cp in id_copies:
            cp.wait()
        _route(b, idg, pos_out, ids_out, off_out)

    ml_own = lax.fori_loop(n_half // group, n_blocks // group, block, zero)

    for i in range(n_half):
        o_copy(i).wait()
    ml_copy.wait()
    ml_their = mlr[...]
    top = jnp.maximum(jnp.maximum(ml_own, ml_their), sn)
    w_own, w_their, w_new = jnp.exp(ml_own - top), jnp.exp(ml_their - top), jnp.exp(sn - top)
    den = pltpu.roll(ml_own, half, 1) * w_own + pltpu.roll(ml_their, half, 1) * w_their + w_new
    w_own, w_their, w_new = w_own / den, w_their / den, w_new / den
    for j in range(half):
        o3r[j] = (o3[mine + j] * w_own[:, j:j + 1] + o3r[j] * w_their[:, j:j + 1] + v3[j] * w_new[:, j:j + 1])
    for h in range(heads):
        o2[:, h * dim:(h + 1) * dim] = o3r[:, h, :].astype(BF16)
    w_copies[3].wait()
    d_model = x_ref.shape[1]
    a = (x_ref[pl.ds(mine, half), :].astype(F32) + _nn(o2[...], wo[...])).astype(BF16)
    a_own[...] = a
    me = b * 2 + p
    u_all[me] = _rms(a.astype(F32)).astype(BF16)

    y_blk, x_blk = b * 2 + (1 - p), ((1 - x) * 2 + c) * 2 + p
    d_blk = ((1 - x) * 2 + c) * 2 + (1 - p)
    lo, hi = pl.ds(0, half // 2), pl.ds(half // 2, half // 2)

    def u_copy(i, src, peer, part=None):
        ref = u_all.at[src] if part is None else u_all.at[src, part]
        return _rcopy(ref, ref, gsend.at[i], grecv.at[i], peer)

    quarter = [pl.ds(k * (half // 4), half // 4) for k in range(4)]
    own_y = [u_copy(k, me, to_y, quarter[k]) for k in range(4)]
    own_x = [u_copy(4 + k, me, to_x, quarter[k]) for k in range(4)]
    own_c = u_copy(8, me, to_c)
    for k in range(4):
        own_y[k].start()
        own_x[(k + 2) % 4].start()
    own_c.start()
    cw = d_model // 2
    a_out[...] = a_own[:, pl.ds(pl.multiple_of(p * cw, 128), cw)]
    a_copy = _rcopy(a_own.at[:, pl.ds(pl.multiple_of((1 - p) * cw, 128), cw)], a_recv, gsend.at[9], grecv.at[9], to_y)
    fwd_x = [u_copy(10 + k, y_blk, to_x, quarter[k]) for k in range(2)]
    fwd_y = [u_copy(12 + k, x_blk, to_y, quarter[2 + k]) for k in range(2)]
    for k in range(2):
        own_y[k].wait_recv()
        fwd_x[k].start()
        own_x[2 + k].wait_recv()
        fwd_y[k].start()
    a_copy.start()
    own_y[2].wait_recv()
    own_y[3].wait_recv()
    c_y = u_copy(14, y_blk, to_c)
    c_y.start()
    own_x[0].wait_recv()
    own_x[1].wait_recv()
    c_x = u_copy(15, x_blk, to_c)
    c_x.start()
    for cp in fwd_x:
        cp.wait_recv()
    c_lo = u_copy(16, d_blk, to_c, lo)
    c_lo.start()
    for cp in fwd_y:
        cp.wait_recv()
    c_hi = u_copy(17, d_blk, to_c, hi)
    c_hi.start()
    for cp in (own_c, c_y, c_x, c_lo, c_hi, a_copy):
        cp.wait_recv()
    for cp in (*own_y, *own_x, own_c, *fwd_x, c_y, *fwd_y, c_x, c_lo, c_hi, a_copy):
        cp.wait_send()


def attn_scratch(slots, group, tokens, rows, dim, wq):
    d_model, heads, half = wq.shape[1], wq.shape[2] // dim, tokens // 2
    dma = pltpu.SemaphoreType.DMA
    weight = pltpu.VMEM(wq.shape[1:], BF16)
    return [
        pltpu.VMEM((slots, TB, rows, dim), BF16), pltpu.VMEM((slots, TB, rows, dim), BF16), pltpu.VMEM((group * TB, heads, rows), BF16),
        weight, weight, weight, weight,
        pltpu.VMEM((tokens, heads, dim), F32), pltpu.VMEM((tokens, heads, dim), F32), pltpu.VMEM((half, heads, dim), F32),
        pltpu.VMEM((half, heads, dim), F32), pltpu.VMEM((half, heads, dim), F32),
        pltpu.VMEM((heads, 128), F32), pltpu.VMEM((heads, 128), F32), pltpu.VMEM((half, heads * dim), BF16),
        pltpu.VMEM((half, d_model), BF16),
        dma((slots,)), dma((slots,)), dma((4,)), dma((half // TB + 1,)), dma((half // TB + 1,)), dma((18,)), dma((18,)),
    ]


def attention(layer, x, lens, kc, vc, wq, wk, wv, wo, ids, n_local):
    tokens, d_model = x.shape
    rows, dim = kc.shape[2], kc.shape[3]
    half = tokens // 2
    hbm = pl.BlockSpec(memory_space=pltpu.HBM)
    vmem = pl.BlockSpec(memory_space=pltpu.VMEM)
    dma = pltpu.SemaphoreType.DMA
    scratch = attn_scratch(SLOTS, 1, tokens, rows, dim, wq)
    out_shape = [jax.ShapeDtypeStruct((8, half, d_model), BF16)] + [jax.ShapeDtypeStruct((half, d_model // 2), BF16)] * 2
    in_specs = [vmem, pl.BlockSpec(memory_space=pltpu.SMEM)] + [hbm] * 6
    out_specs = [vmem] * 3
    args = [x, lens, kc, vc, wq, wk, wv, wo]
    layers = ids.shape[0]
    args.append(ids)
    in_specs.append(vmem)
    out_shape += [jax.ShapeDtypeStruct((layers, 8, 8 * half), I32)] * 2 + [jax.ShapeDtypeStruct((layers, n_local, 128), I32)]
    out_specs += [vmem] * 3
    scratch += [pltpu.VMEM((4,) + ids.shape, I32), dma((3,)), dma((3,))]
    u, a, a_got, *rest = pl.pallas_call(
        functools.partial(attn_kernel, layer, True),
        out_shape=out_shape, in_specs=in_specs, out_specs=out_specs, scratch_shapes=scratch,
        compiler_params=pltpu.CompilerParams(collective_id=layer, has_side_effects=True, vmem_limit_bytes=VMEM_MIB << 20),
    )(*args)
    return (u.reshape(8 * half, d_model), a, a_got, *rest)


def expert_kernel(layer, part, off_ref, u_ref, pos_ref, w1_hbm, w3_hbm, w2_hbm, own_ref, send_ref,
                  xt, act, w1, w3, w2, t_exp, t_at, t_new, t_lo, t_hi, live, sem):
    n_tok = u_ref.shape[0]
    n_local = w1.shape[0]
    n_rows, cw = own_ref.shape
    p = lax.axis_index("pool")
    start = sum(PART_ROWS[:part])
    weights = ((w1_hbm, w1), (w3_hbm, w3), (w2_hbm, w2))

    def copies(e):
        return [pltpu.make_async_copy(src.at[layer, e], dst.at[e], sem.at[i, e]) for i, (src, dst) in enumerate(weights)]

    def plan(e, state):
        t, n = state
        end = jnp.where(e + 1 < n_local, off_ref[layer, jnp.minimum(e + 1, n_local - 1), 0], start + n_rows)
        lo = jnp.maximum(off_ref[layer, e, 0] - start, 0)
        hi = jnp.minimum(end - start, n_rows)
        base = lo // 16 * 16
        live[n] = e

        def put(i, t):
            t_exp[t] = e
            t_at[t] = jnp.minimum(base + i * TILE_M, n_rows - TILE_M)
            t_new[t] = jnp.where(i == 0, n + 1, 0)
            t_lo[t] = lo
            t_hi[t] = hi
            return t + 1

        some = lo < hi

        @pl.when(some & (n < DEPTH))
        def _():
            for cp in copies(e):
                cp.start()

        return lax.fori_loop(0, jnp.where(some, pl.cdiv(hi - base, TILE_M), 0), put, t), jnp.where(some, n + 1, n)

    tiles, n_live = lax.fori_loop(0, n_local, plan, (0, 0))
    t_new[tiles] = 0

    def start_nth(i):
        @pl.when(i < n_live)
        def _():
            for cp in copies(live[i]):
                cp.start()

    step = 128
    for r in range(n_rows // step):
        rid = lax.broadcasted_iota(I32, (step, n_tok), 0) + (r * step + start)
        hit = rid == pos_ref[layer, 0:1, :]
        for k in range(1, 6):
            hit = hit | (rid == pos_ref[layer, k:k + 1, :])
        rows = _nn(jnp.where(hit, 1.0, 0.0).astype(BF16), u_ref[...])
        xt[:, r * step:(r + 1) * step] = jnp.transpose(rows).astype(BF16)
    xt[:, n_rows:] = jnp.zeros((xt.shape[0], xt.shape[1] - n_rows), BF16)

    def arrive(k):
        @pl.when(t_new[k] > 0)
        def _():
            for cp in copies(t_exp[k]):
                cp.wait()
            start_nth(t_new[k] - 1 + DEPTH)

    def up(k):
        e, at = t_exp[k], t_at[k]
        cols = xt[:, pl.ds(pl.multiple_of(at // 128 * 128, 128), 2 * TILE_M)]
        h1 = _nn(w1[e], cols)
        h3 = _nn(w3[e], cols)
        return jnp.transpose(h1 * jax.nn.sigmoid(h1) * h3).astype(BF16)

    def down(k):
        at = pl.multiple_of(t_at[k], 16)
        rows = act[k % 2, pl.ds(pl.multiple_of(t_at[k] % 128, 16), TILE_M), :]
        rid = lax.broadcasted_iota(I32, (TILE_M, cw), 0) + at
        mask = (rid >= t_lo[k]) & (rid < t_hi[k])
        for ref, q in ((own_ref, p), (send_ref, 1 - p)):
            y = _nn(rows, w2[t_exp[k], :, pl.ds(pl.multiple_of(q * cw, 128), cw)])
            ref[pl.ds(at, TILE_M), :] = jnp.where(mask, y, ref[pl.ds(at, TILE_M), :])

    arrive(0)
    arrive(1)
    act[0] = up(0)

    def both(k, none):
        arrive(k + 1)
        act[k % 2] = up(k)
        down(k - 1)
        return none

    lax.fori_loop(1, tiles, both, 0)
    down(tiles - 1)


def experts(layer, part, off, u, pos_t, w1, w3, w2, n_rows):
    n_local, width, d_model = w1.shape[1:]
    hbm = pl.BlockSpec(memory_space=pl.ANY)
    vmem = pl.BlockSpec(memory_space=pltpu.VMEM)
    weights = pltpu.VMEM((n_local, width, d_model), BF16)
    table = pltpu.SMEM((64,), I32)
    return pl.pallas_call(
        functools.partial(expert_kernel, layer, part),
        out_shape=[jax.ShapeDtypeStruct((n_rows, d_model // 2), F32)] * 2,
        in_specs=[pl.BlockSpec(memory_space=pltpu.SMEM), vmem, vmem, hbm, hbm, hbm],
        out_specs=[vmem, vmem],
        scratch_shapes=[pltpu.VMEM((d_model, n_rows + 2 * TILE_M), BF16), pltpu.VMEM((2, 2 * TILE_M, width), BF16),
                        weights, weights, weights,
                        table, table, table, table, table, table, pltpu.SemaphoreType.DMA((3, n_local))],
        compiler_params=pltpu.CompilerParams(vmem_limit_bytes=45 << 20),
        cost_estimate=pl.CostEstimate(flops=int(4e9), bytes_accessed=18 << 20, transcendentals=0),
    )(off, u, pos_t, w1, w3, w2)


N_CH = 4


def _gated(gm, rows, ys):
    return _nn(gm[0, :, rows], ys) + (_nn(gm[1, :, rows], ys) + _nn(gm[2, :, rows], ys))


def gate_kernel(layer, own_ref, got_ref, u_ref, wr_ref, ids_ref, pos_ref, gm, t0):
    n_rows, n_tok, top_k = gm.shape[2], gm.shape[1], 6
    step = 128
    n_exp = wr_ref.shape[1]
    wr = wr_ref[layer]
    wr1 = wr.astype(BF16)
    wr2 = (wr - wr1.astype(F32)).astype(BF16)
    wr3 = (wr - wr1.astype(F32) - wr2.astype(F32)).astype(BF16)

    def gates(i, carry):
        at = pl.ds(pl.multiple_of(i * step, step), step)
        rows = u_ref[at, :]
        logits = _nt(rows, wr1) + (_nt(rows, wr2) + _nt(rows, wr3))
        lane = lax.broadcasted_iota(I32, (step, n_exp), 1)
        ids = jnp.transpose(ids_ref[layer, :, at].astype(F32)).astype(I32)
        pos = jnp.transpose(pos_ref[layer, :, at].astype(F32)).astype(I32)
        g = [jnp.sum(jnp.where(lane == ids[:, k:k + 1], logits, 0.0), axis=1, keepdims=True) for k in range(top_k)]
        top = functools.reduce(jnp.maximum, g)
        g = [jnp.exp(v - top) for v in g]
        den = functools.reduce(jnp.add, g)
        g = [v / den for v in g]
        rid = lax.broadcasted_iota(I32, (step, n_rows), 1)
        mat = jnp.zeros((step, n_rows), F32)
        for k in range(top_k):
            mat = jnp.where(rid == pos[:, k:k + 1], g[k], mat)
        g1 = mat.astype(BF16)
        rest = mat - g1.astype(F32)
        g2 = rest.astype(BF16)
        gm[0, at, :] = g1
        gm[1, at, :] = g2
        gm[2, at, :] = (rest - g2.astype(F32)).astype(BF16)
        return carry

    lax.fori_loop(0, n_tok // step, gates, 0)

    part_rows, cols = own_ref.shape
    total = _gated(gm, pl.ds(0, part_rows), (own_ref[...] + got_ref[...]).astype(BF16))
    cw = cols // N_CH
    for j in range(N_CH):
        t0[j] = total[:, j * cw:(j + 1) * cw].reshape(t0.shape[1:])


def gates(layer, own, got, u, wr, ids, pos):
    n_tok = u.shape[0]
    tokens = n_tok // 4
    vmem = pl.BlockSpec(memory_space=pltpu.VMEM)
    return pl.pallas_call(
        functools.partial(gate_kernel, layer),
        out_shape=[jax.ShapeDtypeStruct((3, n_tok, sum(PART_ROWS)), BF16),
                   jax.ShapeDtypeStruct((N_CH, 4, tokens, own.shape[1] // N_CH), F32)],
        in_specs=[vmem] * 6, out_specs=[vmem] * 2,
        compiler_params=pltpu.CompilerParams(vmem_limit_bytes=20 << 20),
        cost_estimate=pl.CostEstimate(flops=int(2e9), bytes_accessed=4 << 20, transcendentals=0),
    )(own, got, u, wr, ids, pos)


def combine_kernel(*refs):
    _combine(refs[:8], refs[8], refs[9:])


def next_layer_kernel(layer, *refs):
    inputs, operands, outs, scratch = refs[:8], refs[8:15], refs[15:18], refs[18:]
    shared, mixing, attending = scratch[0], scratch[1:15], scratch[15:]
    steps = attn_steps(layer, False, False, shared, *operands, *outs, *attending)
    next(steps)
    _combine(inputs, shared, mixing)
    for _ in steps:
        pass


def _combine(inputs, xo, scratch):
    own1_ref, got1_ref, own2_ref, send2_ref, gm, t0_ref, a_ref, a_got_ref = inputs
    yr, tb, tcr, txs, txr, a_buf, ysend, yrecv, csend, crecv, xsend, xrecv, fsend, frecv = scratch
    p, _, x, c, to_y, to_x, to_c = _where_am_i()
    cw = yr.shape[2]
    mine = p * N_CH
    _greet((to_y, to_x, to_c))

    def cols(i):
        return pl.ds(pl.multiple_of(i * cw, 128), cw)

    y_copies = [_rcopy(send2_ref.at[:, j * cw:(j + 1) * cw], yr.at[j], ysend.at[j], yrecv.at[j], to_y) for j in range(N_CH)]
    for cp in y_copies:
        cp.start()

    half = a_ref.shape[0]
    a_buf[pl.ds(pl.multiple_of(p * half, half), half), :] = a_ref[...]
    a_buf[pl.ds(pl.multiple_of((1 - p) * half, half), half), :] = a_got_ref[...]
    second, third = pl.ds(PART_ROWS[0], PART_ROWS[1]), pl.ds(PART_ROWS[0] + PART_ROWS[1], PART_ROWS[2])
    total = _gated(gm, second, (own1_ref[...] + got1_ref[...]).astype(BF16))
    for j in range(N_CH):
        tb[j] = t0_ref[j] + total[:, j * cw:(j + 1) * cw].reshape(tb.shape[1:])

    chunks = []

    def gather(j):
        y_copies[j].wait_recv()
        ys = (own2_ref[:, j * cw:(j + 1) * cw] + yr[j]).astype(BF16)
        tb[j] = tb[j] + _gated(gm, third, ys).reshape(tb.shape[1:])
        c_copies = [_rcopy(tb.at[j, i * 2 + (1 - c)], tcr.at[j, i], csend.at[j, i], crecv.at[j, i], to_c) for i in range(2)]
        for cp in c_copies:
            cp.start()
        chunks.append(c_copies)

    def cross(j):
        for cp in chunks[j]:
            cp.wait_recv()
        txs[j] = tb[j, (1 - x) * 2 + c] + tcr[j, 1 - x]
        x_copy = _rcopy(txs.at[j], txr.at[j], xsend.at[j], xrecv.at[j], to_x)
        x_copy.start()
        chunks[j].append(x_copy)

    def finish(j):
        chunks[j][-1].wait_recv()
        own = tb[j, x * 2 + c] + tcr[j, x]
        new = (a_buf[:, j * cw:(j + 1) * cw].astype(F32) + (own + txr[j])).astype(BF16)
        xo[:, cols(mine + j)] = new
        f_copy = _rcopy(xo.at[:, cols(mine + j)], xo.at[:, cols(mine + j)], fsend.at[j], frecv.at[j], to_y)
        f_copy.start()
        chunks[j].append(f_copy)

    for j in range(N_CH + 2):
        if j < N_CH:
            gather(j)
        if 0 <= j - 1 < N_CH:
            cross(j - 1)
        if 0 <= j - 2 < N_CH:
            finish(j - 2)
    for copies in chunks:
        copies[-1].wait_recv()
    for cp in y_copies:
        cp.wait_send()
    for copies in chunks:
        for cp in copies:
            cp.wait_send()


def combine_scratch(own2, t0, a):
    half, half_cols = a.shape
    tokens, cw = 2 * half, half_cols // N_CH
    dma = pltpu.SemaphoreType.DMA
    return [
        pltpu.VMEM((N_CH, own2.shape[0], cw), F32), pltpu.VMEM(t0.shape, F32),
        pltpu.VMEM((N_CH, 2, tokens, cw), F32), pltpu.VMEM((N_CH, tokens, cw), F32), pltpu.VMEM((N_CH, tokens, cw), F32),
        pltpu.VMEM((tokens, half_cols), BF16),
        dma((N_CH,)), dma((N_CH,)), dma((N_CH, 2)), dma((N_CH, 2)), dma((N_CH,)), dma((N_CH,)), dma((N_CH,)), dma((N_CH,)),
    ]


def combine(args):
    half, half_cols = args[6].shape
    vmem = pl.BlockSpec(memory_space=pltpu.VMEM)
    return pl.pallas_call(
        combine_kernel,
        out_shape=jax.ShapeDtypeStruct((2 * half, 2 * half_cols), BF16),
        in_specs=[vmem] * 8,
        out_specs=vmem,
        scratch_shapes=combine_scratch(args[2], args[5], args[6]),
        compiler_params=pltpu.CompilerParams(collective_id=8, has_side_effects=True, vmem_limit_bytes=32 << 20),
    )(*args)


def next_layer(layer, args, lens, kc, vc, wq, wk, wv, wo):
    half, half_cols = args[6].shape
    tokens, d_model = 2 * half, 2 * half_cols
    vmem = pl.BlockSpec(memory_space=pltpu.VMEM)
    hbm = pl.BlockSpec(memory_space=pltpu.HBM)
    u, a, a_got = pl.pallas_call(
        functools.partial(next_layer_kernel, layer),
        out_shape=[jax.ShapeDtypeStruct((8, half, d_model), BF16)] + [jax.ShapeDtypeStruct((half, half_cols), BF16)] * 2,
        in_specs=[vmem] * 8 + [pl.BlockSpec(memory_space=pltpu.SMEM)] + [hbm] * 6,
        out_specs=[vmem] * 3,
        scratch_shapes=[pltpu.VMEM((tokens, d_model), BF16)] + combine_scratch(args[2], args[5], args[6])
        + attn_scratch(AHEAD, 4, tokens, kc.shape[2], kc.shape[3], wq),
        compiler_params=pltpu.CompilerParams(collective_id=layer, has_side_effects=True, vmem_limit_bytes=46 << 20),
    )(*args, lens, kc, vc, wq, wk, wv, wo)
    return u.reshape(8 * half, d_model), a, a_got


def solution(mesh):
    tok_spec = P(("dp", "ep"), None)
    cache_spec = P(None, ("dp", "ep"), "pool", None, None)
    up_spec = P(None, "ep", None, "pool")
    down_spec = P(None, "ep", "pool", None)
    in_specs = (tok_spec, cache_spec, cache_spec, P(("dp", "ep")), P(), P(), P(), P(), P(), P(None, ("dp", "ep"), None), up_spec, up_spec, down_spec)

    def body(hidden, kc, vc, lens, wq, wk, wv, wo, wr, ids, w1, w3, w2):
        layers, tokens, seq, heads, dim = kc.shape
        n_local = w1.shape[1]
        top_k = ids.shape[2]
        kc = kc.reshape(layers, tokens, seq * heads, dim)
        vc = vc.reshape(layers, tokens, seq * heads, dim)
        w1 = jnp.swapaxes(w1, 2, 3)
        w3 = jnp.swapaxes(w3, 2, 3)
        wr = jnp.swapaxes(wr, 1, 2)
        ids = jnp.pad(jnp.swapaxes(ids, 1, 2), ((0, 0), (0, 8 - top_k), (0, 0)))
        weights = (lens, kc, vc, wq, wk, wv, wo)
        u, a, a_got, pos, ids_all, off = attention(0, hidden, *weights, ids, n_local)
        for layer in range(layers):
            own, got = [], []
            for part in range(PARTS):
                kept, send = experts(layer, part, off, u, pos, w1, w3, w2, PART_ROWS[part])
                own.append(kept)
                if part < PARTS - 1:
                    got.append(lax.ppermute(send, "pool", [(0, 1), (1, 0)]))
            gm, t0 = gates(layer, own[0], got[0], u, wr, ids_all, pos)
            args = (own[1], got[1], own[2], send, gm, t0, a, a_got)
            if layer + 1 < layers:
                u, a, a_got = next_layer(layer + 1, args, *weights)
        return combine(args)

    return jax.shard_map(body, mesh=mesh, in_specs=in_specs, out_specs=tok_spec, check_vma=False)
```
